32 devices in a mesh: dp: 8 (over z, x), ctx: 2 (over core), tensor: 2 (over y).
Axes of the slice: x: 2, y: 2, z: 4, core: 2. Of those that a mesh axis runs over, the one named last changes fastest.
Arguments:
- tokens: bfloat16 [16, 736, 1152], P(('dp', 'tensor'), 'ctx'), may hold values from -6 to 6
- teacher: bfloat16 [16, 736, 1152], P(('dp', 'tensor'), 'ctx'), may hold values from -6 to 6
- valid_len: int32 [16], P(('dp', 'tensor')), may hold values from 0 to 729, as said below
- ln1_gain: bfloat16 [1152], P(('dp', 'ctx')), may hold values from 0.5 to 1.5
- ln1_bias: bfloat16 [1152], P(('dp', 'ctx')), may hold values from -4 to 4
- w_q: bfloat16 [1152, 1152], P(('dp', 'ctx'), 'tensor'), may hold values from -0.25 to 0.25
- b_q: bfloat16 [1152], P('tensor'), may hold values from -4 to 4
- w_k: bfloat16 [1152, 1152], P(('dp', 'ctx'), 'tensor'), may hold values from -0.25 to 0.25
- w_v: bfloat16 [1152, 1152], P(('dp', 'ctx'), 'tensor'), may hold values from -0.1875 to 0.1875
- b_v: bfloat16 [1152], P('tensor'), may hold values from -4 to 4
- w_o: bfloat16 [1152, 1152], P('tensor', ('dp', 'ctx')), may hold values from -1.5 to 1.5
- b_o: bfloat16 [1152], P(('dp', 'ctx')), may hold values from -6 to 6
- ln2_gain: bfloat16 [1152], P(('dp', 'ctx')), may hold values from 0.5 to 1.5
- ln2_bias: bfloat16 [1152], P(('dp', 'ctx')), may hold values from -4 to 4
- w_up: bfloat16 [1152, 4304], P(('dp', 'ctx'), 'tensor'), may hold values from -0.1875 to 0.1875
- b_up: bfloat16 [4304], P('tensor'), may hold values from -6 to 6
- w_down: bfloat16 [4304, 1152], P('tensor', ('dp', 'ctx')), may hold values from -0.09375 to 0.09375
- b_down: bfloat16 [1152], P(('dp', 'ctx')), may hold values from -6 to 6
Outputs:
- layer_out: bfloat16 [16, 736, 1152], P(('dp', 'tensor'), 'ctx')
- loss: float32 [], replicated
- tokens_grad: float32 [16, 736, 1152], P(('dp', 'tensor'), 'ctx')
- ln1_gain_grad: float32 [1152], P(('dp', 'ctx'))
- ln1_bias_grad: float32 [1152], P(('dp', 'ctx'))
- w_q_grad: float32 [1152, 1152], P(('dp', 'ctx'), 'tensor')
- b_q_grad: float32 [1152], P('tensor')
- w_k_grad: float32 [1152, 1152], P(('dp', 'ctx'), 'tensor')
- w_v_grad: float32 [1152, 1152], P(('dp', 'ctx'), 'tensor')
- b_v_grad: float32 [1152], P('tensor')
- w_o_grad: float32 [1152, 1152], P('tensor', ('dp', 'ctx'))
- b_o_grad: float32 [1152], P(('dp', 'ctx'))
- ln2_gain_grad: float32 [1152], P(('dp', 'ctx'))
- ln2_bias_grad: float32 [1152], P(('dp', 'ctx'))
- w_up_grad: float32 [1152, 4304], P(('dp', 'ctx'), 'tensor')
- b_up_grad: float32 [4304], P('tensor')
- w_down_grad: float32 [4304, 1152], P('tensor', ('dp', 'ctx'))
- b_down_grad: float32 [1152], P(('dp', 'ctx'))
The draws below stay inside these ranges and needn't reach their ends.
Inputs may be any that keep to these rules, and one draw needn't show every extreme that they name: The first valid_len[s] token positions of slot s are valid and the others are not; the last slot has exactly 729 valid tokens.
All inputs are finite; a program needn't handle non-finite values.
Results may differ from the reference program's by a relative error of at most 0.014.
Values may be sent and summed in bfloat16 or wider, within the bound.
A program may use at most 192 MiB of HBM per device.

```python
import jax
import jax.numpy as jnp
from jax import lax

D = 1152
H = 16
HD = 72
FF = 4304
SEQ = 736
REAL = 729
HH = 1152
IMG = 16
LOSS_SCALE = 13565952


def draw_valid_len(key, part):
    slot_index = jnp.arange(IMG)
    top_len = REAL // 9 + (REAL - REAL // 9) * slot_index // max(IMG - 1, 1)
    first_key, second_key = jax.random.split(jax.random.fold_in(key, 11))
    random_bits = jax.random.randint(first_key, (IMG,), 0, 1 << 20)
    bottom_len = top_len // 2
    lengths = bottom_len + random_bits % (top_len - bottom_len + 1)
    dropped = jax.random.randint(second_key, (IMG,), 0, 16) == 0
    lengths = jnp.where(dropped, 0, lengths)
    lengths = jnp.where(slot_index == IMG - 1, REAL, lengths)
    return lengths.astype(jnp.int32)


def block_levels(rng, extent, pieces, low, top_value):
    def one(position, parts):
        steps = jax.random.uniform(jax.random.fold_in(jax.random.fold_in(rng, 6), position), (parts,), jnp.float32, low / len(pieces), top_value / len(pieces))
        return jnp.repeat(jnp.exp(steps), extent[position] // parts).reshape((-1,) + (1,) * (len(extent) - position - 1))

    gain = one(*pieces[0])
    for cut in pieces[1:]:
        gain = gain * one(*cut)
    return gain


def scatter_about(stream_key, dims, scale, most, shards=(), held_as=jnp.bfloat16):
    level = block_levels(stream_key, dims, shards, -0.22, 0.18) if shards else 1.0
    values = jax.random.normal(stream_key, dims, jnp.float32) * scale * level
    return jnp.minimum(jnp.maximum(values, -most), most).astype(held_as)


def setup_inputs(seed: int = 0) -> dict:
    seeds = jax.random.split(jax.random.key(seed), 19)
    tokens = scatter_about(seeds[0], (IMG, SEQ, D), 1.0, 6.0, ((0, 16), (1, 2)))
    teacher = scatter_about(seeds[1], (IMG, SEQ, D), 1.0, 6.0, ((0, 16), (1, 2)))
    valid_len = draw_valid_len(jax.random.fold_in(seeds[18], 71), 0)
    ln1_gain = jnp.clip(1.0 + 0.1 * jax.random.normal(seeds[3], (D,), jnp.float32), 0.5, 1.5).astype(jnp.bfloat16)
    ln1_bias = scatter_about(seeds[4], (D,), 0.3, 4.0, ((0, 16),))
    w_q = scatter_about(seeds[5], (D, HH), (D // 2) ** -0.5, 0.25, ((0, 16), (1, 2)))
    b_q = scatter_about(seeds[6], (HH,), 0.3, 4.0, ((0, 2),))
    w_k = scatter_about(seeds[7], (D, HH), (D // 2) ** -0.5, 0.25, ((0, 16), (1, 2)))
    w_v = scatter_about(seeds[8], (D, HH), D ** -0.5, 0.1875, ((0, 16), (1, 2)))
    b_v = scatter_about(seeds[9], (HH,), 0.3, 4.0, ((0, 2),))
    w_o = scatter_about(seeds[10], (HH, D), (HH // 64) ** -0.5, 1.5, ((0, 2), (1, 16)))
    b_o = scatter_about(seeds[11], (D,), 0.5, 6.0, ((0, 16),))
    ln2_gain = jnp.clip(1.0 + 0.1 * jax.random.normal(seeds[12], (D,), jnp.float32), 0.5, 1.5).astype(jnp.bfloat16)
    ln2_bias = scatter_about(seeds[13], (D,), 0.3, 4.0, ((0, 16),))
    w_up = scatter_about(seeds[14], (D, FF), D ** -0.5, 0.1875, ((0, 16), (1, 2)))
    b_up = scatter_about(seeds[15], (FF,), 0.5, 6.0, ((0, 2),))
    w_down = scatter_about(seeds[16], (FF, D), FF ** -0.5, 0.09375, ((0, 2), (1, 16)))
    b_down = scatter_about(seeds[17], (D,), 0.5, 6.0, ((0, 16),))
    return {"tokens": tokens, "teacher": teacher, "valid_len": valid_len, "ln1_gain": ln1_gain, "ln1_bias": ln1_bias, "w_q": w_q, "b_q": b_q, "w_k": w_k, "w_v": w_v, "b_v": b_v, "w_o": w_o, "b_o": b_o, "ln2_gain": ln2_gain, "ln2_bias": ln2_bias, "w_up": w_up, "b_up": b_up, "w_down": w_down, "b_down": b_down}


EPSILON = 1e-06
GELU_C = 0.7978845608028654
GELU_K = 0.044715
HIGHEST = lax.Precision.HIGHEST
BLOCK_IMAGES = 4

@jax.custom_vjp
def low(v):
    return lax.optimization_barrier(v.astype(jnp.bfloat16)).astype(jnp.float32)

@jax.custom_vjp
def low_back(v):
    return v

def low_keep(v):
    return (low(v), None)

def low_pass(kept, grad):
    return (grad,)

def back_keep(v):
    return (v, None)

def back_low(kept, grad):
    return (low(grad),)
low.defvjp(low_keep, low_pass)
low_back.defvjp(back_keep, back_low)

def matmul(left, right):
    return jnp.dot(left, right, precision=HIGHEST, preferred_element_type=jnp.float32)

def layer_norm(row_values, gain_vec, shift_vec):
    average = lax.optimization_barrier(jnp.mean(row_values, axis=-1, keepdims=True))
    centred = row_values - average
    spread = lax.optimization_barrier(jnp.mean(centred * centred, axis=-1, keepdims=True))
    return centred * lax.rsqrt(spread + EPSILON) * gain_vec + shift_vec

def gelu_tanh(values):
    return 0.5 * values * (1.0 + jnp.tanh(GELU_C * (values + GELU_K * values * values * values)))

def block_forward(params, images, targets, lengths):
    gain_one, shift_one, query_w, query_b, key_w, value_w, value_b, out_w, out_b, gain_two, shift_two, up_w, up_b, down_w, down_b = params
    count_img = images.shape[0]
    row_values = images.reshape(count_img * SEQ, D)
    normed = low(layer_norm(row_values, gain_one, shift_one))
    queries = low(low_back(matmul(normed, query_w) + query_b)).reshape(count_img, SEQ, H, HD)
    key_rows = low(low_back(matmul(normed, key_w))).reshape(count_img, SEQ, H, HD)
    value_rows = low(low_back(matmul(normed, value_w) + value_b)).reshape(count_img, SEQ, H, HD)
    raw_scores = jnp.einsum('bqhd,bkhd->bhqk', queries, key_rows, precision=HIGHEST)
    scores = low_back(raw_scores * HD ** (-0.5))
    usable = jnp.arange(SEQ) < REAL
    scores = jnp.where(usable, scores, -1e+30)
    soft_weights = low(jax.nn.softmax(scores, axis=-1))
    mixed_rows = jnp.einsum('bhqk,bkhd->bqhd', soft_weights, value_rows, precision=HIGHEST)
    mixed_rows = low(low_back(mixed_rows)).reshape(count_img * SEQ, H * HD)
    hidden = row_values + low_back(matmul(mixed_rows, out_w)) + out_b
    normed_two = low(layer_norm(hidden, gain_two, shift_two))
    before = low_back(matmul(normed_two, up_w) + up_b)
    active = low(gelu_tanh(before))
    result = hidden + low_back(matmul(active, down_w)) + down_b
    valid_rows = (jnp.arange(SEQ)[None, :] < lengths[:, None]).astype(jnp.float32).reshape(-1)
    error_rows = result - targets.reshape(count_img * SEQ, D)
    partial_value = 0.5 * jnp.sum(valid_rows * lax.optimization_barrier(jnp.mean(error_rows * error_rows, axis=-1)))
    return (result.reshape(count_img, SEQ, D), partial_value)

def reference(tokens, teacher, valid_len, ln1_gain, ln1_bias, w_q, b_q, w_k, w_v, b_v, w_o, b_o, ln2_gain, ln2_bias, w_up, b_up, w_down, b_down):
    params = tuple((weight_arg.astype(jnp.float32) for weight_arg in (ln1_gain, ln1_bias, w_q, b_q, w_k, w_v, b_v, w_o, b_o, ln2_gain, ln2_bias, w_up, b_up, w_down, b_down)))
    inputs = tokens.astype(jnp.float32)
    block_count = IMG // BLOCK_IMAGES
    targets = teacher.astype(jnp.float32).reshape(block_count, BLOCK_IMAGES, SEQ, D)
    lengths = valid_len.reshape(block_count, BLOCK_IMAGES)
    valid_count = jnp.sum(valid_len.astype(jnp.float32))

    def whole_pass(images, weights):
        blocks = images.reshape(block_count, BLOCK_IMAGES, SEQ, D)

        def advance(running, block_item):
            out_block, partial_value = jax.checkpoint(block_forward)(weights, block_item[0], block_item[1], block_item[2])
            return (running + partial_value, out_block)
        running, outputs = lax.scan(advance, jnp.zeros((), jnp.float32), (blocks, targets, lengths))
        return (outputs.reshape(IMG, SEQ, D), running / valid_count)
    (layer_out, loss_value), pullback = jax.vjp(whole_pass, inputs, params)
    input_grad, grads = pullback((jnp.zeros_like(layer_out), jnp.asarray(LOSS_SCALE, dtype=jnp.float32)))
    return (layer_out.astype(jnp.bfloat16), loss_value, input_grad, grads[0], grads[1], grads[2], grads[3], grads[4], grads[5], grads[6], grads[7], grads[8], grads[9], grads[10], grads[11], grads[12], grads[13], grads[14])
```

```python
import jax
import jax.numpy as jnp
from jax import lax
from jax.sharding import PartitionSpec as P

HD = 72
REAL = 729


EPSILON = 1e-06
GELU_C = 0.7978845608028654
GELU_K = 0.044715
BF = jnp.bfloat16
F32 = jnp.float32


def norm_forward(row_values, gain_vec, shift_vec):
    average = jnp.mean(row_values, axis=-1, keepdims=True)
    centred = row_values - average
    spread = jnp.mean(centred * centred, axis=-1, keepdims=True)
    inverse = lax.rsqrt(spread + EPSILON)
    unit_rows = centred * inverse
    return (unit_rows * gain_vec + shift_vec, unit_rows, inverse)


def norm_backward(upstream, unit_rows, inverse, gain_vec):
    scaled = upstream * gain_vec
    inner_sum = (
        scaled
        - jnp.mean(scaled, axis=-1, keepdims=True)
        - unit_rows * jnp.mean(scaled * unit_rows, axis=-1, keepdims=True)
    )
    return (inner_sum * inverse, jnp.sum(upstream * unit_rows, axis=0), jnp.sum(upstream, axis=0))


def gelu_tanh(values):
    return 0.5 * values * (1.0 + jnp.tanh(GELU_C * (values + GELU_K * values * values * values)))


def gelu_slope(values):
    tanh_part = jnp.tanh(GELU_C * (values + GELU_K * values * values * values))
    return 0.5 * (1.0 + tanh_part) + 0.5 * values * (1.0 - tanh_part * tanh_part) * GELU_C * (
        1.0 + 3.0 * GELU_K * values * values
    )


def swap(values, axis):
    return lax.ppermute(values, axis, [(0, 1), (1, 0)])


def tensor_gather(values):
    if lax.axis_size("tensor") == 2:
        return jnp.stack([values, swap(values, "tensor")])
    return lax.all_gather(values, "tensor", axis=0)


def tensor_reduce(partials):
    if lax.axis_size("tensor") == 2:
        return partials[0] + swap(partials[1].astype(BF), "tensor").astype(F32)
    return lax.psum_scatter(partials.astype(BF), "tensor", scatter_dimension=0).astype(F32)


def ctx_gather(values):
    if lax.axis_size("ctx") == 2:
        return jnp.concatenate([values, swap(values, "ctx")], axis=2)
    return lax.all_gather(values, "ctx", axis=2, tiled=True)


def ctx_reduce(values, half_len):
    if lax.axis_size("ctx") == 2:
        other = swap(values[:, :, half_len:].astype(BF), "ctx")
        return values[:, :, :half_len] + other.astype(F32)
    return lax.psum_scatter(
        values.astype(BF), "ctx", scatter_dimension=2, tiled=True
    ).astype(F32)


def key_positions(half_len):
    n_ctx = lax.axis_size("ctx")
    local = jnp.arange(half_len * n_ctx)
    if n_ctx == 2:
        me = lax.axis_index("ctx")
        block = jnp.where(local < half_len, me, 1 - me)
        return block * half_len + local % half_len
    return local


def tree_sum(values, axes):
    for axis in axes:
        size = lax.axis_size(axis)
        if size & (size - 1):
            values = jax.tree.map(lambda v: lax.psum(v, axis), values)
            continue
        step = 1
        while step < size:
            perm = [(i, i ^ step) for i in range(size)]
            values = jax.tree.map(lambda v: v + lax.ppermute(v, axis, perm), values)
            step *= 2
    return values


def on_device(
    tokens,
    teacher,
    valid_len,
    ln1_gain,
    ln1_bias,
    w_q,
    b_q,
    w_k,
    w_v,
    b_v,
    w_o,
    b_o,
    ln2_gain,
    ln2_bias,
    w_up,
    b_up,
    w_down,
    b_down,
):
    own_images, half_len, width = tokens.shape
    n_t = lax.axis_size("tensor")
    piece, head_width = w_q.shape
    local_heads = head_width // HD
    hidden_width = w_up.shape[1]
    rows = own_images * half_len
    images = n_t * own_images

    valid_count = tree_sum(jnp.sum(valid_len.astype(jnp.int32)), ("tensor", "dp")).astype(F32)

    vector_rows = jnp.stack([ln1_gain, ln1_bias, b_o, ln2_gain, ln2_bias, b_down], axis=1)
    vector_slot = jnp.pad(vector_rows, ((0, 0), (0, head_width - vector_rows.shape[1])))
    attn_pack = jnp.stack([w_q, w_k, w_v, w_o.T, vector_slot])
    attn_full = lax.all_gather(attn_pack, ("dp", "ctx"), axis=1, tiled=True)
    mlp_pack = jnp.stack([w_up, w_down.T])
    mlp_full = lax.all_gather(mlp_pack, ("dp", "ctx"), axis=1, tiled=True)
    query_w, key_w, value_w, out_wt = attn_full[0], attn_full[1], attn_full[2], attn_full[3]
    vectors = attn_full[4][:, :6].astype(F32)
    gain_one, shift_one, out_bias, gain_two, shift_two, down_bias = [
        vectors[:, i] for i in range(6)
    ]
    up_w, down_wt = mlp_full[0], mlp_full[1]

    query_per_head = query_w.reshape(width, local_heads, HD)
    key_per_head = key_w.reshape(width, local_heads, HD)
    value_per_head = value_w.reshape(width, local_heads, HD)
    out_per_head = out_wt.reshape(width, local_heads, HD)
    query_bias = b_q.astype(F32).reshape(1, local_heads, 1, HD)
    value_bias = b_v.astype(F32).reshape(1, local_heads, 1, HD)

    inputs = tokens.astype(F32).reshape(rows, width)
    normed, unit_one, inverse_one = norm_forward(inputs, gain_one, shift_one)
    normed_every_row = tensor_gather(normed.astype(BF)).reshape(images, half_len, width)
    queries = (
        jnp.einsum("pro,ojx->pjrx", normed_every_row, query_per_head, preferred_element_type=F32)
        + query_bias
    ).astype(BF)
    key_rows = jnp.einsum(
        "pro,ojx->pjrx", normed_every_row, key_per_head, preferred_element_type=F32
    ).astype(BF)
    value_rows = (
        jnp.einsum("pro,ojx->pjrx", normed_every_row, value_per_head, preferred_element_type=F32)
        + value_bias
    ).astype(BF)
    key_all = ctx_gather(key_rows)
    value_all = ctx_gather(value_rows)
    usable = key_positions(half_len) < REAL
    score_scale = HD ** (-0.5)

    raw_scores = jnp.einsum("bhqe,bhke->bhqk", queries, key_all, preferred_element_type=F32)
    scores = jnp.where(usable, raw_scores * score_scale, -1e30)
    summit = jnp.max(scores, axis=-1, keepdims=True)
    exp_total = jnp.sum(jnp.exp(scores - summit), axis=-1, keepdims=True)
    log_totals = summit + jnp.log(exp_total)
    soft_weights = jnp.exp(scores - log_totals).astype(BF)
    mixed_per_head = jnp.einsum(
        "bhqk,bhke->bhqe", soft_weights, value_all, preferred_element_type=F32
    ).astype(BF)

    attn_terms = jnp.einsum(
        "lscm,dsm->lcd", mixed_per_head, out_per_head, preferred_element_type=F32
    )
    attn_sum = tensor_reduce(attn_terms.reshape(n_t, rows, width))
    hidden = inputs + attn_sum + out_bias
    normed_two, unit_two, inverse_two = norm_forward(hidden, gain_two, shift_two)
    normed_two_all = tensor_gather(normed_two.astype(BF)).reshape(images * half_len, width)
    before = jnp.dot(normed_two_all, up_w, preferred_element_type=F32) + b_up.astype(F32)
    active = gelu_tanh(before).astype(BF)
    mlp_terms = jnp.einsum("rf,df->rd", active, down_wt, preferred_element_type=F32)
    result = hidden + tensor_reduce(mlp_terms.reshape(n_t, rows, width)) + down_bias
    layer_out = result.astype(BF).reshape(own_images, half_len, width)

    position = lax.axis_index("ctx") * half_len + jnp.arange(half_len)
    valid_rows = (position[None, :] < valid_len[:, None]).astype(F32).reshape(rows)
    error_rows = result - teacher.astype(F32).reshape(rows, width)
    partial_value = 0.5 * jnp.sum(valid_rows * jnp.mean(error_rows * error_rows, axis=-1))
    slot_total = own_images * lax.axis_size("dp") * n_t
    factor = slot_total * (half_len * lax.axis_size("ctx")) / valid_count
    grad_out = error_rows * (valid_rows[:, None] * factor)

    grad_rows = tensor_gather(grad_out.astype(BF)).reshape(images * half_len, width)
    down_grad_t = jnp.einsum("rd,rf->df", grad_rows, active, preferred_element_type=F32)
    active_grad = jnp.einsum("rd,df->rf", grad_rows, down_wt, preferred_element_type=F32)
    before_grad = (active_grad * gelu_slope(before)).astype(BF)
    up_bias_grad = jnp.sum(before_grad, axis=0, dtype=F32)
    up_grad = jnp.einsum("rd,rf->df", normed_two_all, before_grad, preferred_element_type=F32)
    mlp_grads = lax.psum_scatter(
        jnp.concatenate([up_grad, down_grad_t], axis=1).astype(BF),
        ("dp", "ctx"),
        scatter_dimension=0,
        tiled=True,
    )
    norm_two_terms = jnp.einsum("rf,df->rd", before_grad, up_w, preferred_element_type=F32)
    norm_two_grad = tensor_reduce(norm_two_terms.reshape(n_t, rows, width))
    hidden_back, gain_two_grad, shift_two_grad = norm_backward(
        norm_two_grad, unit_two, inverse_two, gain_two
    )
    hidden_grad = grad_out + hidden_back
    down_bias_grad = jnp.sum(grad_out, axis=0)
    out_bias_grad = jnp.sum(hidden_grad, axis=0)
    hidden_token_rows = tensor_gather(hidden_grad.astype(BF)).reshape(images, half_len, width)
    out_grad_t = jnp.einsum(
        "lcd,lscm->dsm", hidden_token_rows, mixed_per_head, preferred_element_type=F32
    ).reshape(width, head_width)
    mixed_grad = jnp.einsum(
        "lcd,dsm->lscm", hidden_token_rows, out_per_head, preferred_element_type=F32
    ).astype(BF)

    soft_full = jnp.exp(scores - log_totals)
    soft_grad = jnp.einsum("bhqe,bhke->bhqk", mixed_grad, value_all, preferred_element_type=F32)
    value_grads = jnp.einsum(
        "bhqk,bhqe->bhke", soft_full.astype(BF), mixed_grad, preferred_element_type=F32
    )
    inner_sum = jnp.sum(soft_full * soft_grad, axis=-1, keepdims=True)
    score_grad = (soft_full * (soft_grad - inner_sum)).astype(BF)
    query_grads = (
        jnp.einsum("bhqk,bhke->bhqe", score_grad, key_all, preferred_element_type=F32)
        * score_scale
    )
    key_grads = (
        jnp.einsum("bhqk,bhqe->bhke", score_grad, queries, preferred_element_type=F32)
        * score_scale
    )
    key_reduced_precision = ctx_reduce(key_grads, half_len).astype(BF)
    value_reduced_precision = ctx_reduce(value_grads, half_len).astype(BF)
    query_reduced_precision = query_grads.astype(BF)
    query_bias_grad = jnp.sum(query_reduced_precision, axis=(0, 2), dtype=F32).reshape(head_width)
    value_bias_grad = jnp.sum(value_reduced_precision, axis=(0, 2), dtype=F32).reshape(head_width)
    query_weight_grad = jnp.einsum(
        "okz,oaks->zas", normed_every_row, query_reduced_precision, preferred_element_type=F32
    ).reshape(width, head_width)
    key_weight_grad = jnp.einsum(
        "okz,oaks->zas", normed_every_row, key_reduced_precision, preferred_element_type=F32
    ).reshape(width, head_width)
    value_weight_grad = jnp.einsum(
        "okz,oaks->zas", normed_every_row, value_reduced_precision, preferred_element_type=F32
    ).reshape(width, head_width)
    attn_grads = lax.psum_scatter(
        jnp.concatenate(
            [query_weight_grad, key_weight_grad, value_weight_grad, out_grad_t], axis=1
        ).astype(BF),
        ("dp", "ctx"),
        scatter_dimension=0,
        tiled=True,
    )
    norm_one_terms = jnp.einsum(
        "tivw,niw->tvn", query_reduced_precision, query_per_head, preferred_element_type=F32
    )
    norm_one_terms = norm_one_terms + jnp.einsum(
        "tivw,niw->tvn", key_reduced_precision, key_per_head, preferred_element_type=F32
    )
    norm_one_terms = norm_one_terms + jnp.einsum(
        "tivw,niw->tvn", value_reduced_precision, value_per_head, preferred_element_type=F32
    )
    norm_one_grad = tensor_reduce(norm_one_terms.reshape(n_t, rows, width))
    input_back, gain_one_grad, shift_one_grad = norm_backward(
        norm_one_grad, unit_one, inverse_one, gain_one
    )
    tokens_grad = (hidden_grad + input_back).reshape(own_images, half_len, width)

    row_sums = jnp.concatenate(
        [
            gain_one_grad,
            shift_one_grad,
            out_bias_grad,
            gain_two_grad,
            shift_two_grad,
            down_bias_grad,
            partial_value.reshape(1),
        ]
    )
    head_sums = jnp.concatenate([query_bias_grad, value_bias_grad, up_bias_grad])
    row_sums, head_sums = tree_sum((row_sums, head_sums), ("ctx", "dp"))
    row_sums = tree_sum(row_sums, ("tensor",))
    loss_value = row_sums[6 * width] / valid_count
    piece_start = lax.axis_index(("dp", "ctx")) * piece
    vector_shards = [
        lax.dynamic_slice_in_dim(row_sums, i * width + piece_start, piece) for i in range(6)
    ]
    query_bias_sum = head_sums[:head_width]
    value_bias_sum = head_sums[head_width : 2 * head_width]
    up_bias_sum = head_sums[2 * head_width :]
    attn_grads = attn_grads.astype(F32).reshape(piece, 4, head_width)
    mlp_grads = mlp_grads.astype(F32)
    attn_grads = [attn_grads[:, i] for i in range(4)]
    mlp_grads = [mlp_grads[:, :hidden_width], mlp_grads[:, hidden_width:]]
    return (
        layer_out,
        loss_value,
        tokens_grad,
        vector_shards[0],
        vector_shards[1],
        attn_grads[0],
        query_bias_sum,
        attn_grads[1],
        attn_grads[2],
        value_bias_sum,
        attn_grads[3].T,
        vector_shards[2],
        vector_shards[3],
        vector_shards[4],
        mlp_grads[0],
        up_bias_sum,
        mlp_grads[1].T,
        vector_shards[5],
    )


def solution(mesh):
    return jax.shard_map(
        on_device,
        mesh=mesh,
        in_specs=(
            P(("dp", "tensor"), "ctx", None),
            P(("dp", "tensor"), "ctx", None),
            P(("dp", "tensor")),
            P(("dp", "ctx")),
            P(("dp", "ctx")),
            P(("dp", "ctx"), "tensor"),
            P("tensor"),
            P(("dp", "ctx"), "tensor"),
            P(("dp", "ctx"), "tensor"),
            P("tensor"),
            P("tensor", ("dp", "ctx")),
            P(("dp", "ctx")),
            P(("dp", "ctx")),
            P(("dp", "ctx")),
            P(("dp", "ctx"), "tensor"),
            P("tensor"),
            P("tensor", ("dp", "ctx")),
            P(("dp", "ctx")),
        ),
        out_specs=(
            P(("dp", "tensor"), "ctx", None),
            P(),
            P(("dp", "tensor"), "ctx", None),
            P(("dp", "ctx")),
            P(("dp", "ctx")),
            P(("dp", "ctx"), "tensor"),
            P("tensor"),
            P(("dp", "ctx"), "tensor"),
            P(("dp", "ctx"), "tensor"),
            P("tensor"),
            P("tensor", ("dp", "ctx")),
            P(("dp", "ctx")),
            P(("dp", "ctx")),
            P(("dp", "ctx")),
            P(("dp", "ctx"), "tensor"),
            P("tensor"),
            P("tensor", ("dp", "ctx")),
            P(("dp", "ctx")),
        ),
        check_vma=False,
    )
```

```python
import jax
import jax.numpy as jnp
from jax import lax
from jax.sharding import PartitionSpec as P

HD = 72
REAL = 729


EPSILON = 1e-06
GELU_C = 0.7978845608028654
GELU_K = 0.044715
BF = jnp.bfloat16
F32 = jnp.float32


def norm_forward(row_values, gain_vec, shift_vec):
    average = jnp.mean(row_values, axis=-1, keepdims=True)
    centred = row_values - average
    spread = jnp.mean(centred * centred, axis=-1, keepdims=True)
    inverse = lax.rsqrt(spread + EPSILON)
    unit_rows = centred * inverse
    return (unit_rows * gain_vec + shift_vec, unit_rows, inverse)


def norm_backward(upstream, unit_rows, inverse, gain_vec):
    scaled = upstream * gain_vec
    inner_sum = (
        scaled
        - jnp.mean(scaled, axis=-1, keepdims=True)
        - unit_rows * jnp.mean(scaled * unit_rows, axis=-1, keepdims=True)
    )
    return (inner_sum * inverse, jnp.sum(upstream * unit_rows, axis=0), jnp.sum(upstream, axis=0))


def gelu_tanh(values):
    return 0.5 * values * (1.0 + jnp.tanh(GELU_C * (values + GELU_K * values * values * values)))


def gelu_slope(values):
    tanh_part = jnp.tanh(GELU_C * (values + GELU_K * values * values * values))
    return 0.5 * (1.0 + tanh_part) + 0.5 * values * (1.0 - tanh_part * tanh_part) * GELU_C * (
        1.0 + 3.0 * GELU_K * values * values
    )


def swap(values, axis):
    return lax.ppermute(values, axis, [(0, 1), (1, 0)])


def tensor_gather(values):
    if lax.axis_size("tensor") == 2:
        return jnp.stack([values, swap(values, "tensor")])
    return lax.all_gather(values, "tensor", axis=0)


def tensor_reduce(partials):
    if lax.axis_size("tensor") == 2:
        return partials[0] + swap(partials[1].astype(BF), "tensor").astype(F32)
    return lax.psum_scatter(partials.astype(BF), "tensor", scatter_dimension=0).astype(F32)


def ctx_gather(values):
    if lax.axis_size("ctx") == 2:
        return jnp.concatenate([values, swap(values, "ctx")], axis=2)
    return lax.all_gather(values, "ctx", axis=2, tiled=True)


def ctx_reduce(values, half_len):
    if lax.axis_size("ctx") == 2:
        other = swap(values[:, :, half_len:].astype(BF), "ctx")
        return values[:, :, :half_len] + other.astype(F32)
    return lax.psum_scatter(
        values.astype(BF), "ctx", scatter_dimension=2, tiled=True
    ).astype(F32)


def key_positions(half_len):
    n_ctx = lax.axis_size("ctx")
    local = jnp.arange(half_len * n_ctx)
    if n_ctx == 2:
        me = lax.axis_index("ctx")
        block = jnp.where(local < half_len, me, 1 - me)
        return block * half_len + local % half_len
    return local


def tree_sum(values, axes):
    for axis in axes:
        size = lax.axis_size(axis)
        if size & (size - 1):
            values = jax.tree.map(lambda v: lax.psum(v, axis), values)
            continue
        step = 1
        while step < size:
            perm = [(i, i ^ step) for i in range(size)]
            values = jax.tree.map(lambda v: v + lax.ppermute(v, axis, perm), values)
            step *= 2
    return values


def on_device(
    tokens,
    teacher,
    valid_len,
    ln1_gain,
    ln1_bias,
    w_q,
    b_q,
    w_k,
    w_v,
    b_v,
    w_o,
    b_o,
    ln2_gain,
    ln2_bias,
    w_up,
    b_up,
    w_down,
    b_down,
):
    own_images, half_len, width = tokens.shape
    n_t = lax.axis_size("tensor")
    piece, head_width = w_q.shape
    local_heads = head_width // HD
    hidden_width = w_up.shape[1]
    rows = own_images * half_len
    images = n_t * own_images

    valid_count = tree_sum(jnp.sum(valid_len.astype(jnp.int32)), ("tensor", "dp")).astype(F32)
    valid_count, tokens = lax.optimization_barrier((valid_count, tokens))

    pad_hidden = (-hidden_width) % 128
    pad_out = (-head_width) % 128
    vector_rows = jnp.stack([ln1_gain, ln1_bias, b_o, ln2_gain, ln2_bias, b_down], axis=1)
    vector_slot = jnp.pad(vector_rows, ((0, 0), (0, head_width - vector_rows.shape[1])))
    attn_pack = jnp.stack([w_q, w_k, w_v, w_o.T, vector_slot])
    attn_full = lax.all_gather(attn_pack, ("dp", "ctx"), axis=1, tiled=True)
    mlp_pack = jnp.pad(jnp.stack([w_up, w_down.T]), ((0, 0), (0, 0), (0, pad_hidden)))
    mlp_full = lax.all_gather(mlp_pack, ("dp", "ctx"), axis=1, tiled=True)
    qkv_w = attn_full[:3].reshape(3, width, local_heads, HD)
    out_wt = attn_full[3]
    vectors = attn_full[4][:, :6].astype(F32)
    gain_one, shift_one, out_bias, gain_two, shift_two, down_bias = [
        vectors[:, i] for i in range(6)
    ]
    up_w, down_wt = mlp_full[0], mlp_full[1]
    up_b = jnp.pad(b_up.astype(F32), (0, pad_hidden))

    out_per_head = out_wt.reshape(width, local_heads, HD)
    qkv_bias = jnp.stack(
        [b_q.astype(F32), jnp.zeros((head_width,), F32), b_v.astype(F32)]
    ).reshape(3, 1, local_heads, 1, HD)

    inputs = tokens.astype(F32).reshape(rows, width)
    normed, unit_one, inverse_one = norm_forward(inputs, gain_one, shift_one)
    normed_every_row = tensor_gather(normed.astype(BF)).reshape(images, half_len, width)
    qkv_rows = (
        jnp.einsum("pro,tojx->tpjrx", normed_every_row, qkv_w, preferred_element_type=F32)
        + qkv_bias
    ).astype(BF)
    queries, key_rows, value_rows = qkv_rows[0], qkv_rows[1], qkv_rows[2]
    key_all = ctx_gather(key_rows)
    value_all = ctx_gather(value_rows)
    usable = key_positions(half_len) < REAL
    score_scale = HD ** (-0.5)

    raw_scores = jnp.einsum("bhqe,bhke->bhqk", queries, key_all, preferred_element_type=F32)
    scores = jnp.where(usable, raw_scores * score_scale, -1e30)
    summit = jnp.max(scores, axis=-1, keepdims=True)
    exp_total = jnp.sum(jnp.exp(scores - summit), axis=-1, keepdims=True)
    log_totals = summit + jnp.log(exp_total)
    soft_weights = jnp.exp(scores - log_totals).astype(BF)
    mixed_per_head = jnp.einsum(
        "bhqk,bhke->bhqe", soft_weights, value_all, preferred_element_type=F32
    ).astype(BF)

    attn_terms = jnp.einsum(
        "lscm,dsm->lcd", mixed_per_head, out_per_head, preferred_element_type=F32
    )
    attn_sum = tensor_reduce(attn_terms.reshape(n_t, rows, width))
    hidden = inputs + attn_sum + out_bias
    normed_two, unit_two, inverse_two = norm_forward(hidden, gain_two, shift_two)
    normed_two_all = tensor_gather(normed_two.astype(BF)).reshape(images * half_len, width)
    before = jnp.dot(normed_two_all, up_w, preferred_element_type=F32) + up_b
    active = gelu_tanh(before).astype(BF)
    mlp_terms = jnp.einsum("rf,df->rd", active, down_wt, preferred_element_type=F32)
    result = hidden + tensor_reduce(mlp_terms.reshape(n_t, rows, width)) + down_bias
    layer_out = result.astype(BF).reshape(own_images, half_len, width)

    position = lax.axis_index("ctx") * half_len + jnp.arange(half_len)
    valid_rows = (position[None, :] < valid_len[:, None]).astype(F32).reshape(rows)
    error_rows = result - teacher.astype(F32).reshape(rows, width)
    partial_value = 0.5 * jnp.sum(valid_rows * jnp.mean(error_rows * error_rows, axis=-1))
    slot_total = own_images * lax.axis_size("dp") * n_t
    factor = slot_total * (half_len * lax.axis_size("ctx")) / valid_count
    grad_out = error_rows * (valid_rows[:, None] * factor)

    grad_rows = tensor_gather(grad_out.astype(BF)).reshape(images * half_len, width)
    down_grad_t = jnp.einsum("rd,rf->df", grad_rows, active, preferred_element_type=F32)
    active_grad = jnp.einsum("rd,df->rf", grad_rows, down_wt, preferred_element_type=F32)
    before_grad = (active_grad * gelu_slope(before)).astype(BF)
    up_bias_grad = jnp.sum(before_grad[:, :hidden_width], axis=0, dtype=F32)
    up_grad = jnp.einsum("rd,rf->df", normed_two_all, before_grad, preferred_element_type=F32)
    mlp_grad_pack = jnp.concatenate([up_grad.astype(BF), down_grad_t.astype(BF)], axis=1)
    norm_two_terms = jnp.einsum("rf,df->rd", before_grad, up_w, preferred_element_type=F32)
    norm_two_grad = tensor_reduce(norm_two_terms.reshape(n_t, rows, width))
    hidden_back, gain_two_grad, shift_two_grad = norm_backward(
        norm_two_grad, unit_two, inverse_two, gain_two
    )
    hidden_grad = grad_out + hidden_back
    mlp_grad_pack, hidden_grad = lax.optimization_barrier((mlp_grad_pack, hidden_grad))
    mlp_grads = lax.psum_scatter(mlp_grad_pack, ("dp", "ctx"), scatter_dimension=0, tiled=True)
    down_bias_grad = jnp.sum(grad_out, axis=0)
    out_bias_grad = jnp.sum(hidden_grad, axis=0)
    hidden_token_rows = tensor_gather(hidden_grad.astype(BF)).reshape(images, half_len, width)
    out_grad_t = jnp.einsum(
        "lcd,lscm->dsm", hidden_token_rows, mixed_per_head, preferred_element_type=F32
    ).reshape(width, head_width)
    mixed_grad = jnp.einsum(
        "lcd,dsm->lscm", hidden_token_rows, out_per_head, preferred_element_type=F32
    ).astype(BF)

    soft_full = jnp.exp(scores - log_totals)
    soft_grad = jnp.einsum("bhqe,bhke->bhqk", mixed_grad, value_all, preferred_element_type=F32)
    value_grads = jnp.einsum(
        "bhqk,bhqe->bhke", soft_full.astype(BF), mixed_grad, preferred_element_type=F32
    )
    inner_sum = jnp.sum(soft_full * soft_grad, axis=-1, keepdims=True)
    score_grad = (soft_full * (soft_grad - inner_sum)).astype(BF)
    query_grads = (
        jnp.einsum("bhqk,bhke->bhqe", score_grad, key_all, preferred_element_type=F32)
        * score_scale
    )
    key_grads = (
        jnp.einsum("bhqk,bhqe->bhke", score_grad, queries, preferred_element_type=F32)
        * score_scale
    )
    key_reduced_precision = ctx_reduce(key_grads, half_len).astype(BF)
    value_reduced_precision = ctx_reduce(value_grads, half_len).astype(BF)
    query_reduced_precision = query_grads.astype(BF)
    query_bias_grad = jnp.sum(query_reduced_precision, axis=(0, 2), dtype=F32).reshape(head_width)
    value_bias_grad = jnp.sum(value_reduced_precision, axis=(0, 2), dtype=F32).reshape(head_width)
    qkv_grads = jnp.stack(
        [query_reduced_precision, key_reduced_precision, value_reduced_precision]
    )
    qkv_weight_grad = jnp.einsum(
        "okz,toaks->ztas", normed_every_row, qkv_grads, preferred_element_type=F32
    ).reshape(width, 3 * head_width)
    attn_grads = lax.psum_scatter(
        jnp.concatenate(
            [jnp.pad(out_grad_t.astype(BF), ((0, 0), (0, pad_out))), qkv_weight_grad.astype(BF)],
            axis=1,
        ),
        ("dp", "ctx"),
        scatter_dimension=0,
        tiled=True,
    )
    norm_one_terms = jnp.einsum(
        "toaks,tzas->okz", qkv_grads, qkv_w, preferred_element_type=F32
    )
    norm_one_grad = tensor_reduce(norm_one_terms.reshape(n_t, rows, width))
    input_back, gain_one_grad, shift_one_grad = norm_backward(
        norm_one_grad, unit_one, inverse_one, gain_one
    )
    tokens_grad = (hidden_grad + input_back).reshape(own_images, half_len, width)

    row_sums = jnp.concatenate(
        [
            gain_one_grad,
            shift_one_grad,
            out_bias_grad,
            gain_two_grad,
            shift_two_grad,
            down_bias_grad,
            partial_value.reshape(1),
        ]
    )
    head_sums = jnp.concatenate([query_bias_grad, value_bias_grad, up_bias_grad])
    row_sums, head_sums = tree_sum((row_sums, head_sums), ("ctx", "dp"))
    row_sums = tree_sum(row_sums, ("tensor",))
    loss_value = row_sums[6 * width] / valid_count
    piece_start = lax.axis_index(("dp", "ctx")) * piece
    vector_shards = [
        lax.dynamic_slice_in_dim(row_sums, i * width + piece_start, piece) for i in range(6)
    ]
    query_bias_sum = head_sums[:head_width]
    value_bias_sum = head_sums[head_width : 2 * head_width]
    up_bias_sum = head_sums[2 * head_width :]
    attn_grads = attn_grads.astype(F32)
    mlp_grads = mlp_grads.astype(F32)
    out_cols = head_width + pad_out
    attn_grads = [
        attn_grads[:, out_cols + i * head_width : out_cols + (i + 1) * head_width]
        for i in range(3)
    ] + [attn_grads[:, :head_width]]
    hidden_cols = hidden_width + pad_hidden
    mlp_grads = [
        mlp_grads[:, :hidden_width],
        mlp_grads[:, hidden_cols : hidden_cols + hidden_width],
    ]
    return (
        layer_out,
        loss_value,
        tokens_grad,
        vector_shards[0],
        vector_shards[1],
        attn_grads[0],
        query_bias_sum,
        attn_grads[1],
        attn_grads[2],
        value_bias_sum,
        attn_grads[3].T,
        vector_shards[2],
        vector_shards[3],
        vector_shards[4],
        mlp_grads[0],
        up_bias_sum,
        mlp_grads[1].T,
        vector_shards[5],
    )


def solution(mesh):
    return jax.shard_map(
        on_device,
        mesh=mesh,
        in_specs=(
            P(("dp", "tensor"), "ctx", None),
            P(("dp", "tensor"), "ctx", None),
            P(("dp", "tensor")),
            P(("dp", "ctx")),
            P(("dp", "ctx")),
            P(("dp", "ctx"), "tensor"),
            P("tensor"),
            P(("dp", "ctx"), "tensor"),
            P(("dp", "ctx"), "tensor"),
            P("tensor"),
            P("tensor", ("dp", "ctx")),
            P(("dp", "ctx")),
            P(("dp", "ctx")),
            P(("dp", "ctx")),
            P(("dp", "ctx"), "tensor"),
            P("tensor"),
            P("tensor", ("dp", "ctx")),
            P(("dp", "ctx")),
        ),
        out_specs=(
            P(("dp", "tensor"), "ctx", None),
            P(),
            P(("dp", "tensor"), "ctx", None),
            P(("dp", "ctx")),
            P(("dp", "ctx")),
            P(("dp", "ctx"), "tensor"),
            P("tensor"),
            P(("dp", "ctx"), "tensor"),
            P(("dp", "ctx"), "tensor"),
            P("tensor"),
            P("tensor", ("dp", "ctx")),
            P(("dp", "ctx")),
            P(("dp", "ctx")),
            P(("dp", "ctx")),
            P(("dp", "ctx"), "tensor"),
            P("tensor"),
            P("tensor", ("dp", "ctx")),
            P(("dp", "ctx")),
        ),
        check_vma=False,
    )
```

```python
import jax
import jax.numpy as jnp
from jax import lax
from jax.sharding import PartitionSpec as P


HD = 72
REAL = 729


EPSILON = 1e-06
GELU_C = 0.7978845608028654
GELU_K = 0.044715
BF = jnp.bfloat16
F32 = jnp.float32


def norm_forward(row_values, gain_vec, shift_vec):
    average = jnp.mean(row_values, axis=-1, keepdims=True)
    centred = row_values - average
    spread = jnp.mean(centred * centred, axis=-1, keepdims=True)
    inverse = lax.rsqrt(spread + EPSILON)
    unit_rows = centred * inverse
    return (unit_rows * gain_vec + shift_vec, unit_rows, inverse)


def norm_backward(upstream, unit_rows, inverse, gain_vec):
    scaled = upstream * gain_vec
    inner_sum = (
        scaled
        - jnp.mean(scaled, axis=-1, keepdims=True)
        - unit_rows * jnp.mean(scaled * unit_rows, axis=-1, keepdims=True)
    )
    return (inner_sum * inverse, jnp.sum(upstream * unit_rows, axis=0), jnp.sum(upstream, axis=0))


def gelu_tanh(values):
    return 0.5 * values * (1.0 + jnp.tanh(GELU_C * (values + GELU_K * values * values * values)))


def gelu_slope(values):
    tanh_part = jnp.tanh(GELU_C * (values + GELU_K * values * values * values))
    return 0.5 * (1.0 + tanh_part) + 0.5 * values * (1.0 - tanh_part * tanh_part) * GELU_C * (
        1.0 + 3.0 * GELU_K * values * values
    )


def swap(values, axis):
    return lax.ppermute(values, axis, [(0, 1), (1, 0)])


def tensor_gather(values):
    if lax.axis_size("tensor") == 2:
        return jnp.stack([values, swap(values, "tensor")])
    return lax.all_gather(values, "tensor", axis=0)


def tensor_reduce(partials):
    if lax.axis_size("tensor") == 2:
        return partials[0] + swap(partials[1].astype(BF), "tensor").astype(F32)
    return lax.psum_scatter(partials.astype(BF), "tensor", scatter_dimension=0).astype(F32)


def ctx_gather(values):
    if lax.axis_size("ctx") == 2:
        return jnp.concatenate([values, swap(values, "ctx")], axis=2)
    return lax.all_gather(values, "ctx", axis=2, tiled=True)


def ctx_reduce(values, half_len):
    if lax.axis_size("ctx") == 2:
        other = swap(values[:, :, half_len:].astype(BF), "ctx")
        return values[:, :, :half_len] + other.astype(F32)
    return lax.psum_scatter(
        values.astype(BF), "ctx", scatter_dimension=2, tiled=True
    ).astype(F32)


def key_positions(half_len):
    n_ctx = lax.axis_size("ctx")
    local = jnp.arange(half_len * n_ctx)
    if n_ctx == 2:
        me = lax.axis_index("ctx")
        block = jnp.where(local < half_len, me, 1 - me)
        return block * half_len + local % half_len
    return local


def tree_sum(values, axes):
    for axis in axes:
        size = lax.axis_size(axis)
        if size & (size - 1):
            values = jax.tree.map(lambda v: lax.psum(v, axis), values)
            continue
        step = 1
        while step < size:
            perm = [(i, i ^ step) for i in range(size)]
            values = jax.tree.map(lambda v: v + lax.ppermute(v, axis, perm), values)
            step *= 2
    return values


def on_device_body(
    tokens,
    teacher,
    valid_len,
    ln1_gain,
    ln1_bias,
    w_q,
    b_q,
    w_k,
    w_v,
    b_v,
    w_o,
    b_o,
    ln2_gain,
    ln2_bias,
    w_up,
    b_up,
    w_down,
    b_down,
):
    own_images, half_len, width = tokens.shape
    n_t = lax.axis_size("tensor")
    piece, head_width = w_q.shape
    local_heads = head_width // HD
    hidden_width = w_up.shape[1]
    rows = own_images * half_len
    images = n_t * own_images

    valid_count = tree_sum(jnp.sum(valid_len.astype(jnp.int32)), ("tensor", "dp")).astype(F32)
    valid_count, tokens = lax.optimization_barrier((valid_count, tokens))

    pad_hidden = (-hidden_width) % 128
    pad_out = (-head_width) % 128
    vector_rows = jnp.stack([ln1_gain, ln1_bias, b_o, ln2_gain, ln2_bias, b_down], axis=1)
    vector_slot = jnp.pad(vector_rows, ((0, 0), (0, head_width - vector_rows.shape[1])))
    attn_pack = jnp.stack([w_q, w_k, w_v, w_o.T, vector_slot])
    attn_full = lax.all_gather(attn_pack, ("dp", "ctx"), axis=1, tiled=True)
    mlp_pack = jnp.pad(jnp.stack([w_up, w_down.T]), ((0, 0), (0, 0), (0, pad_hidden)))
    mlp_full = lax.all_gather(mlp_pack, ("dp", "ctx"), axis=1, tiled=True)
    qkv_w = attn_full[:3].reshape(3, width, local_heads, HD)
    out_wt = attn_full[3]
    vectors = attn_full[4][:, :6].astype(F32)
    gain_one, shift_one, out_bias, gain_two, shift_two, down_bias = [
        vectors[:, i] for i in range(6)
    ]
    up_w, down_wt = mlp_full[0], mlp_full[1]
    up_b = jnp.pad(b_up.astype(F32), (0, pad_hidden))

    out_per_head = out_wt.reshape(width, local_heads, HD)
    qkv_bias = jnp.stack(
        [b_q.astype(F32), jnp.zeros((head_width,), F32), b_v.astype(F32)]
    ).reshape(3, 1, local_heads, 1, HD)

    inputs = tokens.astype(F32).reshape(rows, width)
    normed, unit_one, inverse_one = norm_forward(inputs, gain_one, shift_one)
    normed_every_row = tensor_gather(normed.astype(BF)).reshape(images, half_len, width)
    qkv_rows = (
        jnp.einsum("pro,tojx->tpjrx", normed_every_row, qkv_w, preferred_element_type=F32)
        + qkv_bias
    ).astype(BF)
    queries, key_rows, value_rows = qkv_rows[0], qkv_rows[1], qkv_rows[2]
    key_all = ctx_gather(key_rows)
    value_all = ctx_gather(value_rows)
    usable = key_positions(half_len) < REAL
    score_scale = HD ** (-0.5)

    raw_scores = jnp.einsum("bhqe,bhke->bhqk", queries, key_all, preferred_element_type=F32)
    scores = jnp.where(usable, raw_scores * score_scale, -1e30)
    summit = jnp.max(scores, axis=-1, keepdims=True)
    exp_total = jnp.sum(jnp.exp(scores - summit), axis=-1, keepdims=True)
    log_totals = summit + jnp.log(exp_total)
    soft_weights = jnp.exp(scores - log_totals).astype(BF)
    mixed_per_head = jnp.einsum(
        "bhqk,bhke->bhqe", soft_weights, value_all, preferred_element_type=F32
    ).astype(BF)

    attn_terms = jnp.einsum(
        "lscm,dsm->lcd", mixed_per_head, out_per_head, preferred_element_type=F32
    )
    attn_sum = tensor_reduce(attn_terms.reshape(n_t, rows, width))
    hidden = inputs + attn_sum + out_bias
    normed_two, unit_two, inverse_two = norm_forward(hidden, gain_two, shift_two)
    normed_two_all = tensor_gather(normed_two.astype(BF)).reshape(images * half_len, width)
    before = jnp.dot(normed_two_all, up_w, preferred_element_type=F32) + up_b
    active = gelu_tanh(before).astype(BF)
    mlp_terms = jnp.einsum("rf,df->rd", active, down_wt, preferred_element_type=F32)
    result = hidden + tensor_reduce(mlp_terms.reshape(n_t, rows, width)) + down_bias
    layer_out = result.astype(BF).reshape(own_images, half_len, width)

    position = lax.axis_index("ctx") * half_len + jnp.arange(half_len)
    valid_rows = (position[None, :] < valid_len[:, None]).astype(F32).reshape(rows)
    error_rows = result - teacher.astype(F32).reshape(rows, width)
    partial_value = 0.5 * jnp.sum(valid_rows * jnp.mean(error_rows * error_rows, axis=-1))
    slot_total = own_images * lax.axis_size("dp") * n_t
    factor = slot_total * (half_len * lax.axis_size("ctx")) / valid_count
    grad_out = error_rows * (valid_rows[:, None] * factor)

    grad_rows = tensor_gather(grad_out.astype(BF)).reshape(images * half_len, width)
    down_grad_t = jnp.einsum("rd,rf->df", grad_rows, active, preferred_element_type=F32)
    active_grad = jnp.einsum("rd,df->rf", grad_rows, down_wt, preferred_element_type=F32)
    before_grad = (active_grad * gelu_slope(before)).astype(BF)
    up_bias_grad = jnp.sum(before_grad[:, :hidden_width], axis=0, dtype=F32)
    up_grad = jnp.einsum("rd,rf->df", normed_two_all, before_grad, preferred_element_type=F32)
    mlp_grad_pack = jnp.concatenate([up_grad.astype(BF), down_grad_t.astype(BF)], axis=1)
    norm_two_terms = jnp.einsum("rf,df->rd", before_grad, up_w, preferred_element_type=F32)
    norm_two_grad = tensor_reduce(norm_two_terms.reshape(n_t, rows, width))
    hidden_back, gain_two_grad, shift_two_grad = norm_backward(
        norm_two_grad, unit_two, inverse_two, gain_two
    )
    hidden_grad = grad_out + hidden_back
    mlp_grad_pack, hidden_grad = lax.optimization_barrier((mlp_grad_pack, hidden_grad))
    mlp_grads = lax.psum_scatter(
        mlp_grad_pack, ("dp", "ctx"), scatter_dimension=0, tiled=True
    )
    down_bias_grad = jnp.sum(grad_out, axis=0)
    out_bias_grad = jnp.sum(hidden_grad, axis=0)
    hidden_token_rows = tensor_gather(hidden_grad.astype(BF)).reshape(images, half_len, width)
    out_grad_t = jnp.einsum(
        "lcd,lscm->dsm", hidden_token_rows, mixed_per_head, preferred_element_type=F32
    ).reshape(width, head_width)
    mixed_grad = jnp.einsum(
        "lcd,dsm->lscm", hidden_token_rows, out_per_head, preferred_element_type=F32
    ).astype(BF)

    soft_full = jnp.exp(scores - log_totals)
    soft_grad = jnp.einsum("bhqe,bhke->bhqk", mixed_grad, value_all, preferred_element_type=F32)
    value_grads = jnp.einsum(
        "bhqk,bhqe->bhke", soft_full.astype(BF), mixed_grad, preferred_element_type=F32
    )
    inner_sum = jnp.sum(soft_full * soft_grad, axis=-1, keepdims=True)
    score_grad = (soft_full * (soft_grad - inner_sum)).astype(BF)
    query_grads = (
        jnp.einsum("bhqk,bhke->bhqe", score_grad, key_all, preferred_element_type=F32)
        * score_scale
    )
    key_grads = (
        jnp.einsum("bhqk,bhqe->bhke", score_grad, queries, preferred_element_type=F32)
        * score_scale
    )
    key_reduced_precision = ctx_reduce(key_grads, half_len).astype(BF)
    value_reduced_precision = ctx_reduce(value_grads, half_len).astype(BF)
    query_reduced_precision = query_grads.astype(BF)
    query_bias_grad = jnp.sum(query_reduced_precision, axis=(0, 2), dtype=F32).reshape(head_width)
    value_bias_grad = jnp.sum(value_reduced_precision, axis=(0, 2), dtype=F32).reshape(head_width)
    qkv_grads = jnp.stack(
        [query_reduced_precision, key_reduced_precision, value_reduced_precision]
    )
    qkv_weight_grad = jnp.einsum(
        "okz,toaks->ztas", normed_every_row, qkv_grads, preferred_element_type=F32
    ).reshape(width, 3 * head_width)
    attn_grads = lax.psum_scatter(
        jnp.concatenate(
            [jnp.pad(out_grad_t.astype(BF), ((0, 0), (0, pad_out))), qkv_weight_grad.astype(BF)],
            axis=1,
        ),
        ("dp", "ctx"),
        scatter_dimension=0,
        tiled=True,
    )
    norm_one_terms = jnp.einsum(
        "toaks,tzas->okz", qkv_grads, qkv_w, preferred_element_type=F32
    )
    norm_one_grad = tensor_reduce(norm_one_terms.reshape(n_t, rows, width))
    input_back, gain_one_grad, shift_one_grad = norm_backward(
        norm_one_grad, unit_one, inverse_one, gain_one
    )
    tokens_grad = (hidden_grad + input_back).reshape(own_images, half_len, width)

    row_sums = jnp.concatenate(
        [
            gain_one_grad,
            shift_one_grad,
            out_bias_grad,
            gain_two_grad,
            shift_two_grad,
            down_bias_grad,
            partial_value.reshape(1),
        ]
    )
    head_sums = jnp.concatenate([query_bias_grad, value_bias_grad, up_bias_grad])
    row_sums, head_sums = tree_sum((row_sums, head_sums), ("ctx", "dp"))
    row_sums = tree_sum(row_sums, ("tensor",))
    loss_value = row_sums[6 * width] / valid_count
    piece_start = lax.axis_index(("dp", "ctx")) * piece
    vector_shards = [
        lax.dynamic_slice_in_dim(row_sums, i * width + piece_start, piece) for i in range(6)
    ]
    query_bias_sum = head_sums[:head_width]
    value_bias_sum = head_sums[head_width : 2 * head_width]
    up_bias_sum = head_sums[2 * head_width :]
    attn_grads = attn_grads.astype(F32)
    mlp_grads = mlp_grads.astype(F32)
    out_cols = head_width + pad_out
    attn_grads = [
        attn_grads[:, out_cols + i * head_width : out_cols + (i + 1) * head_width]
        for i in range(3)
    ] + [attn_grads[:, :head_width]]
    hidden_cols = hidden_width + pad_hidden
    mlp_grads = [
        mlp_grads[:, :hidden_width],
        mlp_grads[:, hidden_cols : hidden_cols + hidden_width],
    ]
    return (
        layer_out,
        loss_value,
        tokens_grad,
        vector_shards[0],
        vector_shards[1],
        attn_grads[0],
        query_bias_sum,
        attn_grads[1],
        attn_grads[2],
        value_bias_sum,
        attn_grads[3].T,
        vector_shards[2],
        vector_shards[3],
        vector_shards[4],
        mlp_grads[0],
        up_bias_sum,
        mlp_grads[1].T,
        vector_shards[5],
    )


def solution(mesh):
    return jax.shard_map(
        on_device_body,
        mesh=mesh,
        in_specs=(
            P(("dp", "tensor"), "ctx", None),
            P(("dp", "tensor"), "ctx", None),
            P(("dp", "tensor")),
            P(("dp", "ctx")),
            P(("dp", "ctx")),
            P(("dp", "ctx"), "tensor"),
            P("tensor"),
            P(("dp", "ctx"), "tensor"),
            P(("dp", "ctx"), "tensor"),
            P("tensor"),
            P("tensor", ("dp", "ctx")),
            P(("dp", "ctx")),
            P(("dp", "ctx")),
            P(("dp", "ctx")),
            P(("dp", "ctx"), "tensor"),
            P("tensor"),
            P("tensor", ("dp", "ctx")),
            P(("dp", "ctx")),
        ),
        out_specs=(
            P(("dp", "tensor"), "ctx", None),
            P(),
            P(("dp", "tensor"), "ctx", None),
            P(("dp", "ctx")),
            P(("dp", "ctx")),
            P(("dp", "ctx"), "tensor"),
            P("tensor"),
            P(("dp", "ctx"), "tensor"),
            P(("dp", "ctx"), "tensor"),
            P("tensor"),
            P("tensor", ("dp", "ctx")),
            P(("dp", "ctx")),
            P(("dp", "ctx")),
            P(("dp", "ctx")),
            P(("dp", "ctx"), "tensor"),
            P("tensor"),
            P("tensor", ("dp", "ctx")),
            P(("dp", "ctx")),
        ),
        check_vma=False,
    )
```

```python
import jax
import jax.numpy as jnp
from jax import lax
from jax.sharding import PartitionSpec as P


HD = 72
REAL = 729


EPSILON = 1e-06
GELU_C = 0.7978845608028654
GELU_K = 0.044715
BF = jnp.bfloat16
F32 = jnp.float32


def norm_forward(row_values, gain_vec, shift_vec):
    average = jnp.mean(row_values, axis=-1, keepdims=True)
    centred = row_values - average
    spread = jnp.mean(centred * centred, axis=-1, keepdims=True)
    inverse = lax.rsqrt(spread + EPSILON)
    unit_rows = centred * inverse
    return (unit_rows * gain_vec + shift_vec, unit_rows, inverse)


def norm_backward(upstream, unit_rows, inverse, gain_vec):
    scaled = upstream * gain_vec
    inner_sum = (
        scaled
        - jnp.mean(scaled, axis=-1, keepdims=True)
        - unit_rows * jnp.mean(scaled * unit_rows, axis=-1, keepdims=True)
    )
    return (inner_sum * inverse, jnp.sum(upstream * unit_rows, axis=0), jnp.sum(upstream, axis=0))


def gelu_tanh(values):
    return 0.5 * values * (1.0 + jnp.tanh(GELU_C * (values + GELU_K * values * values * values)))


def gelu_slope(values):
    tanh_part = jnp.tanh(GELU_C * (values + GELU_K * values * values * values))
    return 0.5 * (1.0 + tanh_part) + 0.5 * values * (1.0 - tanh_part * tanh_part) * GELU_C * (
        1.0 + 3.0 * GELU_K * values * values
    )


def swap(values, axis):
    return lax.ppermute(values, axis, [(0, 1), (1, 0)])


def tensor_gather(values):
    if lax.axis_size("tensor") == 2:
        return jnp.stack([values, swap(values, "tensor")])
    return lax.all_gather(values, "tensor", axis=0)


def tensor_reduce(partials):
    if lax.axis_size("tensor") == 2:
        return partials[0] + swap(partials[1].astype(BF), "tensor").astype(F32)
    return lax.psum_scatter(partials.astype(BF), "tensor", scatter_dimension=0).astype(F32)


def tensor_gather_parts(values):
    if lax.axis_size("tensor") == 2:
        return [values, swap(values, "tensor")]
    gathered = lax.all_gather(values, "tensor", axis=0)
    return [gathered[i] for i in range(gathered.shape[0])]


def tensor_reduce_parts(parts):
    if lax.axis_size("tensor") == 2:
        return parts[0] + swap(parts[1].astype(BF), "tensor").astype(F32)
    return lax.psum_scatter(
        jnp.stack(parts).astype(BF), "tensor", scatter_dimension=0
    ).astype(F32)


def split_rows(values, count):
    size = values.shape[0] // count
    return [values[i * size : (i + 1) * size] for i in range(count)]


def ctx_gather(values):
    if lax.axis_size("ctx") == 2:
        return jnp.concatenate([values, swap(values, "ctx")], axis=2)
    return lax.all_gather(values, "ctx", axis=2, tiled=True)


def ctx_reduce(values, half_len):
    if lax.axis_size("ctx") == 2:
        other = swap(values[:, :, half_len:].astype(BF), "ctx")
        return values[:, :, :half_len] + other.astype(F32)
    return lax.psum_scatter(
        values.astype(BF), "ctx", scatter_dimension=2, tiled=True
    ).astype(F32)


def key_positions(half_len):
    n_ctx = lax.axis_size("ctx")
    local = jnp.arange(half_len * n_ctx)
    if n_ctx == 2:
        me = lax.axis_index("ctx")
        block = jnp.where(local < half_len, me, 1 - me)
        return block * half_len + local % half_len
    return local


def tree_sum(values, axes):
    for axis in axes:
        size = lax.axis_size(axis)
        if size & (size - 1):
            values = jax.tree.map(lambda v: lax.psum(v, axis), values)
            continue
        step = 1
        while step < size:
            perm = [(i, i ^ step) for i in range(size)]
            values = jax.tree.map(lambda v: v + lax.ppermute(v, axis, perm), values)
            step *= 2
    return values


def on_device_body(
    tokens,
    teacher,
    valid_len,
    ln1_gain,
    ln1_bias,
    w_q,
    b_q,
    w_k,
    w_v,
    b_v,
    w_o,
    b_o,
    ln2_gain,
    ln2_bias,
    w_up,
    b_up,
    w_down,
    b_down,
):
    own_images, half_len, width = tokens.shape
    n_t = lax.axis_size("tensor")
    piece, head_width = w_q.shape
    local_heads = head_width // HD
    hidden_width = w_up.shape[1]
    rows = own_images * half_len
    images = n_t * own_images

    valid_count = tree_sum(jnp.sum(valid_len.astype(jnp.int32)), ("tensor", "dp")).astype(F32)
    valid_count, tokens = lax.optimization_barrier((valid_count, tokens))

    pad_hidden = (-hidden_width) % 128
    pad_out = (-head_width) % 128
    vector_rows = jnp.stack([ln1_gain, ln1_bias, b_o, ln2_gain, ln2_bias, b_down], axis=1)
    vector_slot = jnp.pad(vector_rows, ((0, 0), (0, head_width - vector_rows.shape[1])))
    attn_pack = jnp.stack([w_q, w_k, w_v, w_o.T, vector_slot])
    attn_full = lax.all_gather(attn_pack, ("dp", "ctx"), axis=1, tiled=True)
    mlp_pack = jnp.pad(jnp.stack([w_up, w_down.T]), ((0, 0), (0, 0), (0, pad_hidden)))
    mlp_full = lax.all_gather(mlp_pack, ("dp", "ctx"), axis=1, tiled=True)
    qkv_w = attn_full[:3].reshape(3, width, local_heads, HD)
    out_wt = attn_full[3]
    vectors = attn_full[4][:, :6].astype(F32)
    gain_one, shift_one, out_bias, gain_two, shift_two, down_bias = [
        vectors[:, i] for i in range(6)
    ]
    up_w, down_wt = mlp_full[0], mlp_full[1]
    up_b = jnp.pad(b_up.astype(F32), (0, pad_hidden))

    out_per_head = out_wt.reshape(width, local_heads, HD)
    qkv_bias = jnp.stack(
        [b_q.astype(F32), jnp.zeros((head_width,), F32), b_v.astype(F32)]
    ).reshape(3, 1, local_heads, 1, HD)

    inputs = tokens.astype(F32).reshape(rows, width)
    normed, unit_one, inverse_one = norm_forward(inputs, gain_one, shift_one)
    normed_every_row = tensor_gather(normed.astype(BF)).reshape(images, half_len, width)
    qkv_rows = (
        jnp.einsum("pro,tojx->tpjrx", normed_every_row, qkv_w, preferred_element_type=F32)
        + qkv_bias
    ).astype(BF)
    queries, key_rows, value_rows = qkv_rows[0], qkv_rows[1], qkv_rows[2]
    key_all = ctx_gather(key_rows)
    value_all = ctx_gather(value_rows)
    usable = key_positions(half_len) < REAL
    score_scale = HD ** (-0.5)

    raw_scores = jnp.einsum("bhqe,bhke->bhqk", queries, key_all, preferred_element_type=F32)
    scores = jnp.where(usable, raw_scores * score_scale, -1e30)
    summit = jnp.max(scores, axis=-1, keepdims=True)
    exp_total = jnp.sum(jnp.exp(scores - summit), axis=-1, keepdims=True)
    log_totals = summit + jnp.log(exp_total)
    soft_weights = jnp.exp(scores - log_totals).astype(BF)
    mixed_per_head = jnp.einsum(
        "bhqk,bhke->bhqe", soft_weights, value_all, preferred_element_type=F32
    ).astype(BF)

    attn_terms = jnp.einsum(
        "lscm,dsm->lcd", mixed_per_head, out_per_head, preferred_element_type=F32
    )
    attn_sum = tensor_reduce(attn_terms.reshape(n_t, rows, width))
    hidden = inputs + attn_sum + out_bias
    normed_two, unit_two, inverse_two = norm_forward(hidden, gain_two, shift_two)
    normed_two_parts = tensor_gather_parts(normed_two.astype(BF))
    normed_two_all = jnp.concatenate(normed_two_parts)
    before = jnp.dot(normed_two_all, up_w, preferred_element_type=F32) + up_b
    active = gelu_tanh(before).astype(BF)
    before_parts = split_rows(before, n_t)
    active_parts = split_rows(active, n_t)
    mlp_terms = [
        jnp.einsum("rf,df->rd", part, down_wt, preferred_element_type=F32)
        for part in active_parts
    ]
    result = hidden + tensor_reduce_parts(mlp_terms) + down_bias
    layer_out = result.astype(BF).reshape(own_images, half_len, width)

    position = lax.axis_index("ctx") * half_len + jnp.arange(half_len)
    valid_rows = (position[None, :] < valid_len[:, None]).astype(F32).reshape(rows)
    error_rows = result - teacher.astype(F32).reshape(rows, width)
    partial_value = 0.5 * jnp.sum(valid_rows * jnp.mean(error_rows * error_rows, axis=-1))
    slot_total = own_images * lax.axis_size("dp") * n_t
    factor = slot_total * (half_len * lax.axis_size("ctx")) / valid_count
    grad_out = error_rows * (valid_rows[:, None] * factor)

    grad_parts = tensor_gather_parts(grad_out.astype(BF))
    before_grad_parts = [
        (
            jnp.einsum("rd,df->rf", g, down_wt, preferred_element_type=F32)
            * gelu_slope(p)
        ).astype(BF)
        for g, p in zip(grad_parts, before_parts)
    ]
    norm_two_terms = [
        jnp.einsum("rf,df->rd", g, up_w, preferred_element_type=F32)
        for g in before_grad_parts
    ]
    down_grad_t = None
    up_grad = None
    for g, a_part, n_part, p_grad in zip(
        grad_parts, active_parts, normed_two_parts, before_grad_parts
    ):
        down_term = jnp.einsum("rd,rf->df", g, a_part, preferred_element_type=F32)
        up_term = jnp.einsum("rd,rf->df", n_part, p_grad, preferred_element_type=F32)
        down_grad_t = down_term if down_grad_t is None else down_grad_t + down_term
        up_grad = up_term if up_grad is None else up_grad + up_term
    before_grad = jnp.concatenate(before_grad_parts)
    up_bias_grad = jnp.sum(before_grad[:, :hidden_width], axis=0, dtype=F32)
    mlp_grad_pack = jnp.concatenate([up_grad.astype(BF), down_grad_t.astype(BF)], axis=1)
    mlp_grads = lax.psum_scatter(
        mlp_grad_pack, ("dp", "ctx"), scatter_dimension=0, tiled=True
    )
    norm_two_grad = tensor_reduce_parts(norm_two_terms)
    hidden_back, gain_two_grad, shift_two_grad = norm_backward(
        norm_two_grad, unit_two, inverse_two, gain_two
    )
    hidden_grad = grad_out + hidden_back
    down_bias_grad = jnp.sum(grad_out, axis=0)
    out_bias_grad = jnp.sum(hidden_grad, axis=0)
    hidden_token_rows = tensor_gather(hidden_grad.astype(BF)).reshape(images, half_len, width)
    out_grad_t = jnp.einsum(
        "lcd,lscm->dsm", hidden_token_rows, mixed_per_head, preferred_element_type=F32
    ).reshape(width, head_width)
    mixed_grad = jnp.einsum(
        "lcd,dsm->lscm", hidden_token_rows, out_per_head, preferred_element_type=F32
    ).astype(BF)

    soft_full = jnp.exp(scores - log_totals)
    soft_grad = jnp.einsum("bhqe,bhke->bhqk", mixed_grad, value_all, preferred_element_type=F32)
    value_grads = jnp.einsum(
        "bhqk,bhqe->bhke", soft_full.astype(BF), mixed_grad, preferred_element_type=F32
    )
    inner_sum = jnp.sum(soft_full * soft_grad, axis=-1, keepdims=True)
    score_grad = (soft_full * (soft_grad - inner_sum)).astype(BF)
    query_grads = (
        jnp.einsum("bhqk,bhke->bhqe", score_grad, key_all, preferred_element_type=F32)
        * score_scale
    )
    key_grads = (
        jnp.einsum("bhqk,bhqe->bhke", score_grad, queries, preferred_element_type=F32)
        * score_scale
    )
    key_reduced_precision = ctx_reduce(key_grads, half_len).astype(BF)
    value_reduced_precision = ctx_reduce(value_grads, half_len).astype(BF)
    query_reduced_precision = query_grads.astype(BF)
    query_bias_grad = jnp.sum(query_reduced_precision, axis=(0, 2), dtype=F32).reshape(head_width)
    value_bias_grad = jnp.sum(value_reduced_precision, axis=(0, 2), dtype=F32).reshape(head_width)
    qkv_grads = jnp.stack(
        [query_reduced_precision, key_reduced_precision, value_reduced_precision]
    )
    qkv_weight_grad = jnp.einsum(
        "okz,toaks->ztas", normed_every_row, qkv_grads, preferred_element_type=F32
    ).reshape(width, 3 * head_width)
    attn_grads = lax.psum_scatter(
        jnp.concatenate(
            [jnp.pad(out_grad_t.astype(BF), ((0, 0), (0, pad_out))), qkv_weight_grad.astype(BF)],
            axis=1,
        ),
        ("dp", "ctx"),
        scatter_dimension=0,
        tiled=True,
    )
    norm_one_terms = jnp.einsum(
        "toaks,tzas->okz", qkv_grads, qkv_w, preferred_element_type=F32
    )
    norm_one_grad = tensor_reduce(norm_one_terms.reshape(n_t, rows, width))
    input_back, gain_one_grad, shift_one_grad = norm_backward(
        norm_one_grad, unit_one, inverse_one, gain_one
    )
    tokens_grad = (hidden_grad + input_back).reshape(own_images, half_len, width)

    row_sums = jnp.concatenate(
        [
            gain_one_grad,
            shift_one_grad,
            out_bias_grad,
            gain_two_grad,
            shift_two_grad,
            down_bias_grad,
            partial_value.reshape(1),
        ]
    )
    head_sums = jnp.concatenate([query_bias_grad, value_bias_grad, up_bias_grad])
    row_sums, head_sums = tree_sum((row_sums, head_sums), ("ctx", "dp"))
    row_sums = tree_sum(row_sums, ("tensor",))
    loss_value = row_sums[6 * width] / valid_count
    piece_start = lax.axis_index(("dp", "ctx")) * piece
    vector_shards = [
        lax.dynamic_slice_in_dim(row_sums, i * width + piece_start, piece) for i in range(6)
    ]
    query_bias_sum = head_sums[:head_width]
    value_bias_sum = head_sums[head_width : 2 * head_width]
    up_bias_sum = head_sums[2 * head_width :]
    attn_grads = attn_grads.astype(F32)
    mlp_grads = mlp_grads.astype(F32)
    out_cols = head_width + pad_out
    attn_grads = [
        attn_grads[:, out_cols + i * head_width : out_cols + (i + 1) * head_width]
        for i in range(3)
    ] + [attn_grads[:, :head_width]]
    hidden_cols = hidden_width + pad_hidden
    mlp_grads = [
        mlp_grads[:, :hidden_width],
        mlp_grads[:, hidden_cols : hidden_cols + hidden_width],
    ]
    return (
        layer_out,
        loss_value,
        tokens_grad,
        vector_shards[0],
        vector_shards[1],
        attn_grads[0],
        query_bias_sum,
        attn_grads[1],
        attn_grads[2],
        value_bias_sum,
        attn_grads[3].T,
        vector_shards[2],
        vector_shards[3],
        vector_shards[4],
        mlp_grads[0],
        up_bias_sum,
        mlp_grads[1].T,
        vector_shards[5],
    )


def solution(mesh):
    return jax.shard_map(
        on_device_body,
        mesh=mesh,
        in_specs=(
            P(("dp", "tensor"), "ctx", None),
            P(("dp", "tensor"), "ctx", None),
            P(("dp", "tensor")),
            P(("dp", "ctx")),
            P(("dp", "ctx")),
            P(("dp", "ctx"), "tensor"),
            P("tensor"),
            P(("dp", "ctx"), "tensor"),
            P(("dp", "ctx"), "tensor"),
            P("tensor"),
            P("tensor", ("dp", "ctx")),
            P(("dp", "ctx")),
            P(("dp", "ctx")),
            P(("dp", "ctx")),
            P(("dp", "ctx"), "tensor"),
            P("tensor"),
            P("tensor", ("dp", "ctx")),
            P(("dp", "ctx")),
        ),
        out_specs=(
            P(("dp", "tensor"), "ctx", None),
            P(),
            P(("dp", "tensor"), "ctx", None),
            P(("dp", "ctx")),
            P(("dp", "ctx")),
            P(("dp", "ctx"), "tensor"),
            P("tensor"),
            P(("dp", "ctx"), "tensor"),
            P(("dp", "ctx"), "tensor"),
            P("tensor"),
            P("tensor", ("dp", "ctx")),
            P(("dp", "ctx")),
            P(("dp", "ctx")),
            P(("dp", "ctx")),
            P(("dp", "ctx"), "tensor"),
            P("tensor"),
            P("tensor", ("dp", "ctx")),
            P(("dp", "ctx")),
        ),
        check_vma=False,
    )
```

```python
import jax
import jax.numpy as jnp
from jax import lax
from jax.sharding import PartitionSpec as P


HD = 72
REAL = 729


EPSILON = 1e-06
GELU_C = 0.7978845608028654
GELU_K = 0.044715
BF = jnp.bfloat16
F32 = jnp.float32


def norm_forward(row_values, gain_vec, shift_vec):
    average = jnp.mean(row_values, axis=-1, keepdims=True)
    centred = row_values - average
    spread = jnp.mean(centred * centred, axis=-1, keepdims=True)
    inverse = lax.rsqrt(spread + EPSILON)
    unit_rows = centred * inverse
    return (unit_rows * gain_vec + shift_vec, unit_rows, inverse)


def norm_backward(upstream, unit_rows, inverse, gain_vec):
    scaled = upstream * gain_vec
    inner_sum = (
        scaled
        - jnp.mean(scaled, axis=-1, keepdims=True)
        - unit_rows * jnp.mean(scaled * unit_rows, axis=-1, keepdims=True)
    )
    return (inner_sum * inverse, jnp.sum(upstream * unit_rows, axis=0), jnp.sum(upstream, axis=0))


def gelu_tanh(values):
    return 0.5 * values * (1.0 + jnp.tanh(GELU_C * (values + GELU_K * values * values * values)))


def gelu_slope(values):
    tanh_part = jnp.tanh(GELU_C * (values + GELU_K * values * values * values))
    return 0.5 * (1.0 + tanh_part) + 0.5 * values * (1.0 - tanh_part * tanh_part) * GELU_C * (
        1.0 + 3.0 * GELU_K * values * values
    )


def swap(values, axis):
    return lax.ppermute(values, axis, [(0, 1), (1, 0)])


def tensor_gather(values):
    if lax.axis_size("tensor") == 2:
        return jnp.stack([values, swap(values, "tensor")])
    return lax.all_gather(values, "tensor", axis=0)


def tensor_reduce(partials):
    if lax.axis_size("tensor") == 2:
        return partials[0] + swap(partials[1].astype(BF), "tensor").astype(F32)
    return lax.psum_scatter(partials.astype(BF), "tensor", scatter_dimension=0).astype(F32)


def tensor_gather_parts(values):
    if lax.axis_size("tensor") == 2:
        return [values, swap(values, "tensor")]
    gathered = lax.all_gather(values, "tensor", axis=0)
    return [gathered[i] for i in range(gathered.shape[0])]


def tensor_reduce_parts(parts):
    if lax.axis_size("tensor") == 2:
        return parts[0] + swap(parts[1].astype(BF), "tensor").astype(F32)
    return lax.psum_scatter(
        jnp.stack(parts).astype(BF), "tensor", scatter_dimension=0
    ).astype(F32)


def split_rows(values, count):
    size = values.shape[0] // count
    return [values[i * size : (i + 1) * size] for i in range(count)]


def ctx_gather(values):
    if lax.axis_size("ctx") == 2:
        return jnp.concatenate([values, swap(values, "ctx")], axis=2)
    return lax.all_gather(values, "ctx", axis=2, tiled=True)


def ctx_reduce(values, half_len):
    if lax.axis_size("ctx") == 2:
        other = swap(values[:, :, half_len:].astype(BF), "ctx")
        return values[:, :, :half_len] + other.astype(F32)
    return lax.psum_scatter(
        values.astype(BF), "ctx", scatter_dimension=2, tiled=True
    ).astype(F32)


def key_positions(half_len):
    n_ctx = lax.axis_size("ctx")
    local = jnp.arange(half_len * n_ctx)
    if n_ctx == 2:
        me = lax.axis_index("ctx")
        block = jnp.where(local < half_len, me, 1 - me)
        return block * half_len + local % half_len
    return local


def tree_sum(values, axes):
    for axis in axes:
        size = lax.axis_size(axis)
        if size & (size - 1):
            values = jax.tree.map(lambda v: lax.psum(v, axis), values)
            continue
        step = 1
        while step < size:
            perm = [(i, i ^ step) for i in range(size)]
            values = jax.tree.map(lambda v: v + lax.ppermute(v, axis, perm), values)
            step *= 2
    return values


def gather_vectors(block, count):
    n_ctx = lax.axis_size("ctx")
    n_dp = lax.axis_size("dp")
    if n_ctx != 2 or n_dp & (n_dp - 1):
        gathered = lax.all_gather(block, ("dp", "ctx"), axis=0, tiled=True)
        return gathered, tree_sum(count, ("tensor", "dp"))
    count = tree_sum(count, ("tensor",))
    other = swap(block, "ctx")
    first = lax.axis_index("ctx") == 0
    blocks = jnp.where(first, jnp.stack([block, other]), jnp.stack([other, block]))
    dp_index = lax.axis_index("dp")
    step = 1
    while step < n_dp:
        perm = [(i, i ^ step) for i in range(n_dp)]
        their_blocks, their_count = lax.ppermute((blocks, count), "dp", perm)
        low = (dp_index // step) % 2 == 0
        blocks = jnp.where(
            low,
            jnp.concatenate([blocks, their_blocks]),
            jnp.concatenate([their_blocks, blocks]),
        )
        count = count + their_count
        step *= 2
    return blocks.reshape(-1, block.shape[1]), count


def on_device_body(
    tokens,
    teacher,
    valid_len,
    ln1_gain,
    ln1_bias,
    w_q,
    b_q,
    w_k,
    w_v,
    b_v,
    w_o,
    b_o,
    ln2_gain,
    ln2_bias,
    w_up,
    b_up,
    w_down,
    b_down,
):
    own_images, half_len, width = tokens.shape
    n_t = lax.axis_size("tensor")
    piece, head_width = w_q.shape
    local_heads = head_width // HD
    hidden_width = w_up.shape[1]
    rows = own_images * half_len
    images = n_t * own_images

    pad_hidden = (-hidden_width) % 128
    pad_out = (-head_width) % 128
    vector_rows = jnp.stack([ln1_gain, ln1_bias, b_o, ln2_gain, ln2_bias, b_down], axis=1)
    vectors, valid_count = gather_vectors(vector_rows, jnp.sum(valid_len.astype(jnp.int32)))
    valid_count = valid_count.astype(F32)
    valid_count, tokens = lax.optimization_barrier((valid_count, tokens))
    attn_pack = jnp.stack([w_q, w_k, w_v, w_o.T])
    attn_full = lax.all_gather(attn_pack, ("dp", "ctx"), axis=1, tiled=True)
    mlp_pack = jnp.pad(jnp.stack([w_up, w_down.T]), ((0, 0), (0, 0), (0, pad_hidden)))
    mlp_full = lax.all_gather(mlp_pack, ("dp", "ctx"), axis=1, tiled=True)
    qkv_w = attn_full[:3].reshape(3, width, local_heads, HD)
    out_wt = attn_full[3]
    vectors = vectors.astype(F32)
    gain_one, shift_one, out_bias, gain_two, shift_two, down_bias = [
        vectors[:, i] for i in range(6)
    ]
    up_w, down_wt = mlp_full[0], mlp_full[1]
    up_b = jnp.pad(b_up.astype(F32), (0, pad_hidden))

    out_per_head = out_wt.reshape(width, local_heads, HD)
    qkv_bias = jnp.stack(
        [b_q.astype(F32), jnp.zeros((head_width,), F32), b_v.astype(F32)]
    ).reshape(3, 1, local_heads, 1, HD)

    inputs = tokens.astype(F32).reshape(rows, width)
    normed, unit_one, inverse_one = norm_forward(inputs, gain_one, shift_one)
    normed_every_row = tensor_gather(normed.astype(BF)).reshape(images, half_len, width)
    qkv_rows = (
        jnp.einsum("pro,tojx->tpjrx", normed_every_row, qkv_w, preferred_element_type=F32)
        + qkv_bias
    ).astype(BF)
    queries, key_rows, value_rows = qkv_rows[0], qkv_rows[1], qkv_rows[2]
    key_all = ctx_gather(key_rows)
    value_all = ctx_gather(value_rows)
    usable = key_positions(half_len) < REAL
    score_scale = HD ** (-0.5)

    raw_scores = jnp.einsum("bhqe,bhke->bhqk", queries, key_all, preferred_element_type=F32)
    scores = jnp.where(usable, raw_scores * score_scale, -1e30)
    summit = jnp.max(scores, axis=-1, keepdims=True)
    exp_total = jnp.sum(jnp.exp(scores - summit), axis=-1, keepdims=True)
    log_totals = summit + jnp.log(exp_total)
    soft_weights = jnp.exp(scores - log_totals).astype(BF)
    mixed_per_head = jnp.einsum(
        "bhqk,bhke->bhqe", soft_weights, value_all, preferred_element_type=F32
    ).astype(BF)

    attn_terms = jnp.einsum(
        "lscm,dsm->lcd", mixed_per_head, out_per_head, preferred_element_type=F32
    )
    attn_sum = tensor_reduce(attn_terms.reshape(n_t, rows, width))
    hidden = inputs + attn_sum + out_bias
    normed_two, unit_two, inverse_two = norm_forward(hidden, gain_two, shift_two)
    normed_two_parts = tensor_gather_parts(normed_two.astype(BF))
    normed_two_all = jnp.concatenate(normed_two_parts)
    before = jnp.dot(normed_two_all, up_w, preferred_element_type=F32) + up_b
    active = gelu_tanh(before).astype(BF)
    before_parts = split_rows(before, n_t)
    active_parts = split_rows(active, n_t)
    mlp_terms = [
        jnp.einsum("rf,df->rd", part, down_wt, preferred_element_type=F32)
        for part in active_parts
    ]
    result = hidden + tensor_reduce_parts(mlp_terms) + down_bias
    layer_out = result.astype(BF).reshape(own_images, half_len, width)

    position = lax.axis_index("ctx") * half_len + jnp.arange(half_len)
    valid_rows = (position[None, :] < valid_len[:, None]).astype(F32).reshape(rows)
    error_rows = result - teacher.astype(F32).reshape(rows, width)
    partial_value = 0.5 * jnp.sum(valid_rows * jnp.mean(error_rows * error_rows, axis=-1))
    slot_total = own_images * lax.axis_size("dp") * n_t
    factor = slot_total * (half_len * lax.axis_size("ctx")) / valid_count
    grad_out = error_rows * (valid_rows[:, None] * factor)

    grad_parts = tensor_gather_parts(grad_out.astype(BF))
    before_grad_parts = [
        (
            jnp.einsum("rd,df->rf", g, down_wt, preferred_element_type=F32)
            * gelu_slope(p)
        ).astype(BF)
        for g, p in zip(grad_parts, before_parts)
    ]
    norm_two_terms = [
        jnp.einsum("rf,df->rd", g, up_w, preferred_element_type=F32)
        for g in before_grad_parts
    ]
    down_grad_t = None
    up_grad = None
    for g, a_part, n_part, p_grad in zip(
        grad_parts, active_parts, normed_two_parts, before_grad_parts
    ):
        down_term = jnp.einsum("rd,rf->df", g, a_part, preferred_element_type=F32)
        up_term = jnp.einsum("rd,rf->df", n_part, p_grad, preferred_element_type=F32)
        down_grad_t = down_term if down_grad_t is None else down_grad_t + down_term
        up_grad = up_term if up_grad is None else up_grad + up_term
    before_grad = jnp.concatenate(before_grad_parts)
    up_bias_grad = jnp.sum(before_grad[:, :hidden_width], axis=0, dtype=F32)
    mlp_grad_pack = jnp.concatenate([up_grad.astype(BF), down_grad_t.astype(BF)], axis=1)
    mlp_grads = lax.psum_scatter(
        mlp_grad_pack, ("dp", "ctx"), scatter_dimension=0, tiled=True
    )
    norm_two_grad = tensor_reduce_parts(norm_two_terms)
    hidden_back, gain_two_grad, shift_two_grad = norm_backward(
        norm_two_grad, unit_two, inverse_two, gain_two
    )
    hidden_grad = grad_out + hidden_back
    down_bias_grad = jnp.sum(grad_out, axis=0)
    out_bias_grad = jnp.sum(hidden_grad, axis=0)
    hidden_token_rows = tensor_gather(hidden_grad.astype(BF)).reshape(images, half_len, width)
    out_grad_t = jnp.einsum(
        "lcd,lscm->dsm", hidden_token_rows, mixed_per_head, preferred_element_type=F32
    ).reshape(width, head_width)
    mixed_grad = jnp.einsum(
        "lcd,dsm->lscm", hidden_token_rows, out_per_head, preferred_element_type=F32
    ).astype(BF)

    soft_full = jnp.exp(scores - log_totals)
    soft_grad = jnp.einsum("bhqe,bhke->bhqk", mixed_grad, value_all, preferred_element_type=F32)
    value_grads = jnp.einsum(
        "bhqk,bhqe->bhke", soft_full.astype(BF), mixed_grad, preferred_element_type=F32
    )
    inner_sum = jnp.sum(soft_full * soft_grad, axis=-1, keepdims=True)
    score_grad = (soft_full * (soft_grad - inner_sum)).astype(BF)
    query_grads = (
        jnp.einsum("bhqk,bhke->bhqe", score_grad, key_all, preferred_element_type=F32)
        * score_scale
    )
    key_grads = (
        jnp.einsum("bhqk,bhqe->bhke", score_grad, queries, preferred_element_type=F32)
        * score_scale
    )
    key_reduced_precision = ctx_reduce(key_grads, half_len).astype(BF)
    value_reduced_precision = ctx_reduce(value_grads, half_len).astype(BF)
    query_reduced_precision = query_grads.astype(BF)
    query_bias_grad = jnp.sum(query_reduced_precision, axis=(0, 2), dtype=F32).reshape(head_width)
    value_bias_grad = jnp.sum(value_reduced_precision, axis=(0, 2), dtype=F32).reshape(head_width)
    qkv_grads = jnp.stack(
        [query_reduced_precision, key_reduced_precision, value_reduced_precision]
    )
    qkv_weight_grad = jnp.einsum(
        "okz,toaks->ztas", normed_every_row, qkv_grads, preferred_element_type=F32
    ).reshape(width, 3 * head_width)
    attn_grads = lax.psum_scatter(
        jnp.concatenate(
            [jnp.pad(out_grad_t.astype(BF), ((0, 0), (0, pad_out))), qkv_weight_grad.astype(BF)],
            axis=1,
        ),
        ("dp", "ctx"),
        scatter_dimension=0,
        tiled=True,
    )
    norm_one_terms = jnp.einsum(
        "toaks,tzas->okz", qkv_grads, qkv_w, preferred_element_type=F32
    )
    norm_one_grad = tensor_reduce(norm_one_terms.reshape(n_t, rows, width))
    input_back, gain_one_grad, shift_one_grad = norm_backward(
        norm_one_grad, unit_one, inverse_one, gain_one
    )
    tokens_grad = (hidden_grad + input_back).reshape(own_images, half_len, width)

    row_sums = jnp.concatenate(
        [
            gain_one_grad,
            shift_one_grad,
            out_bias_grad,
            gain_two_grad,
            shift_two_grad,
            down_bias_grad,
            partial_value.reshape(1),
        ]
    )
    head_sums = jnp.concatenate([query_bias_grad, value_bias_grad, up_bias_grad])
    row_sums, head_sums = tree_sum((row_sums, head_sums), ("ctx", "dp"))
    row_sums = tree_sum(row_sums, ("tensor",))
    loss_value = row_sums[6 * width] / valid_count
    piece_start = lax.axis_index(("dp", "ctx")) * piece
    vector_shards = [
        lax.dynamic_slice_in_dim(row_sums, i * width + piece_start, piece) for i in range(6)
    ]
    query_bias_sum = head_sums[:head_width]
    value_bias_sum = head_sums[head_width : 2 * head_width]
    up_bias_sum = head_sums[2 * head_width :]
    attn_grads = attn_grads.astype(F32)
    mlp_grads = mlp_grads.astype(F32)
    out_cols = head_width + pad_out
    attn_grads = [
        attn_grads[:, out_cols + i * head_width : out_cols + (i + 1) * head_width]
        for i in range(3)
    ] + [attn_grads[:, :head_width]]
    hidden_cols = hidden_width + pad_hidden
    mlp_grads = [
        mlp_grads[:, :hidden_width],
        mlp_grads[:, hidden_cols : hidden_cols + hidden_width],
    ]
    return (
        layer_out,
        loss_value,
        tokens_grad,
        vector_shards[0],
        vector_shards[1],
        attn_grads[0],
        query_bias_sum,
        attn_grads[1],
        attn_grads[2],
        value_bias_sum,
        attn_grads[3].T,
        vector_shards[2],
        vector_shards[3],
        vector_shards[4],
        mlp_grads[0],
        up_bias_sum,
        mlp_grads[1].T,
        vector_shards[5],
    )


def solution(mesh):
    return jax.shard_map(
        on_device_body,
        mesh=mesh,
        in_specs=(
            P(("dp", "tensor"), "ctx", None),
            P(("dp", "tensor"), "ctx", None),
            P(("dp", "tensor")),
            P(("dp", "ctx")),
            P(("dp", "ctx")),
            P(("dp", "ctx"), "tensor"),
            P("tensor"),
            P(("dp", "ctx"), "tensor"),
            P(("dp", "ctx"), "tensor"),
            P("tensor"),
            P("tensor", ("dp", "ctx")),
            P(("dp", "ctx")),
            P(("dp", "ctx")),
            P(("dp", "ctx")),
            P(("dp", "ctx"), "tensor"),
            P("tensor"),
            P("tensor", ("dp", "ctx")),
            P(("dp", "ctx")),
        ),
        out_specs=(
            P(("dp", "tensor"), "ctx", None),
            P(),
            P(("dp", "tensor"), "ctx", None),
            P(("dp", "ctx")),
            P(("dp", "ctx")),
            P(("dp", "ctx"), "tensor"),
            P("tensor"),
            P(("dp", "ctx"), "tensor"),
            P(("dp", "ctx"), "tensor"),
            P("tensor"),
            P("tensor", ("dp", "ctx")),
            P(("dp", "ctx")),
            P(("dp", "ctx")),
            P(("dp", "ctx")),
            P(("dp", "ctx"), "tensor"),
            P("tensor"),
            P("tensor", ("dp", "ctx")),
            P(("dp", "ctx")),
        ),
        check_vma=False,
    )
```

```python
import jax
import jax.numpy as jnp
from jax import lax
from jax.sharding import PartitionSpec as P


HD = 72
REAL = 729


EPSILON = 1e-06
GELU_C = 0.7978845608028654
GELU_K = 0.044715
BF = jnp.bfloat16
F32 = jnp.float32


def norm_forward(row_values, gain_vec, shift_vec):
    average = jnp.mean(row_values, axis=-1, keepdims=True)
    centred = row_values - average
    spread = jnp.mean(centred * centred, axis=-1, keepdims=True)
    inverse = lax.rsqrt(spread + EPSILON)
    unit_rows = centred * inverse
    return (unit_rows * gain_vec + shift_vec, unit_rows, inverse)


def norm_backward(upstream, unit_rows, inverse, gain_vec):
    scaled = upstream * gain_vec
    inner_sum = (
        scaled
        - jnp.mean(scaled, axis=-1, keepdims=True)
        - unit_rows * jnp.mean(scaled * unit_rows, axis=-1, keepdims=True)
    )
    return (inner_sum * inverse, jnp.sum(upstream * unit_rows, axis=0), jnp.sum(upstream, axis=0))


def gelu_tanh(values):
    return 0.5 * values * (1.0 + jnp.tanh(GELU_C * (values + GELU_K * values * values * values)))


def gelu_slope(values):
    tanh_part = jnp.tanh(GELU_C * (values + GELU_K * values * values * values))
    return 0.5 * (1.0 + tanh_part) + 0.5 * values * (1.0 - tanh_part * tanh_part) * GELU_C * (
        1.0 + 3.0 * GELU_K * values * values
    )


def swap(values, axis):
    return lax.ppermute(values, axis, [(0, 1), (1, 0)])


def tensor_gather(values):
    if lax.axis_size("tensor") == 2:
        return jnp.stack([values, swap(values, "tensor")])
    return lax.all_gather(values, "tensor", axis=0)


def tensor_reduce(partials):
    if lax.axis_size("tensor") == 2:
        return partials[0] + swap(partials[1].astype(BF), "tensor").astype(F32)
    return lax.psum_scatter(partials.astype(BF), "tensor", scatter_dimension=0).astype(F32)


def tensor_gather_parts(values):
    if lax.axis_size("tensor") == 2:
        return [values, swap(values, "tensor")]
    gathered = lax.all_gather(values, "tensor", axis=0)
    return [gathered[i] for i in range(gathered.shape[0])]


def tensor_reduce_parts(parts):
    if lax.axis_size("tensor") == 2:
        return parts[0] + swap(parts[1].astype(BF), "tensor").astype(F32)
    return lax.psum_scatter(
        jnp.stack(parts).astype(BF), "tensor", scatter_dimension=0
    ).astype(F32)


def ctx_gather(values):
    if lax.axis_size("ctx") == 2:
        return jnp.concatenate([values, swap(values, "ctx")], axis=2)
    return lax.all_gather(values, "ctx", axis=2, tiled=True)


def ctx_reduce(values, half_len):
    if lax.axis_size("ctx") == 2:
        other = swap(values[:, :, half_len:].astype(BF), "ctx")
        return values[:, :, :half_len] + other.astype(F32)
    return lax.psum_scatter(
        values.astype(BF), "ctx", scatter_dimension=2, tiled=True
    ).astype(F32)


def key_positions(half_len):
    n_ctx = lax.axis_size("ctx")
    local = jnp.arange(half_len * n_ctx)
    if n_ctx == 2:
        me = lax.axis_index("ctx")
        block = jnp.where(local < half_len, me, 1 - me)
        return block * half_len + local % half_len
    return local


def tree_sum(values, axes):
    for axis in axes:
        size = lax.axis_size(axis)
        if size & (size - 1):
            values = jax.tree.map(lambda v: lax.psum(v, axis), values)
            continue
        step = 1
        while step < size:
            perm = [(i, i ^ step) for i in range(size)]
            values = jax.tree.map(lambda v: v + lax.ppermute(v, axis, perm), values)
            step *= 2
    return values


def gather_vectors(block, count):
    n_ctx = lax.axis_size("ctx")
    n_dp = lax.axis_size("dp")
    if n_ctx != 2 or n_dp & (n_dp - 1):
        gathered = lax.all_gather(block, ("dp", "ctx"), axis=0, tiled=True)
        return gathered, tree_sum(count, ("tensor", "dp"))
    count = tree_sum(count, ("tensor",))
    other = swap(block, "ctx")
    first = lax.axis_index("ctx") == 0
    blocks = jnp.where(first, jnp.stack([block, other]), jnp.stack([other, block]))
    dp_index = lax.axis_index("dp")
    step = 1
    while step < n_dp:
        perm = [(i, i ^ step) for i in range(n_dp)]
        their_blocks, their_count = lax.ppermute((blocks, count), "dp", perm)
        low = (dp_index // step) % 2 == 0
        blocks = jnp.where(
            low,
            jnp.concatenate([blocks, their_blocks]),
            jnp.concatenate([their_blocks, blocks]),
        )
        count = count + their_count
        step *= 2
    return blocks.reshape(-1, block.shape[1]), count


def halving_reduce_scatter(values):
    n_ctx = lax.axis_size("ctx")
    n_dp = lax.axis_size("dp")
    if n_ctx != 2 or n_dp & (n_dp - 1):
        return lax.psum_scatter(
            values.astype(BF), ("dp", "ctx"), scatter_dimension=0, tiled=True
        ).astype(F32)
    total, cols = values.shape
    piece = total // (n_dp * n_ctx)
    acc = values.reshape(n_dp, 2, piece, cols)
    me = lax.axis_index("ctx")
    keep = lax.dynamic_index_in_dim(acc, me, axis=1, keepdims=False)
    send = lax.dynamic_index_in_dim(acc, 1 - me, axis=1, keepdims=False).astype(BF)
    acc = keep + swap(send, "ctx").astype(F32)
    dp_index = lax.axis_index("dp")
    groups = n_dp
    step = 1
    while step < n_dp:
        acc = acc.reshape(groups // 2, 2, piece, cols)
        bit = (dp_index // step) % 2
        keep = lax.dynamic_index_in_dim(acc, bit, axis=1, keepdims=False)
        send = lax.dynamic_index_in_dim(acc, 1 - bit, axis=1, keepdims=False).astype(BF)
        perm = [(i, i ^ step) for i in range(n_dp)]
        acc = keep + lax.ppermute(send, "dp", perm).astype(F32)
        groups //= 2
        step *= 2
    return acc.reshape(piece, cols)


def on_device_body(
    tokens,
    teacher,
    valid_len,
    ln1_gain,
    ln1_bias,
    w_q,
    b_q,
    w_k,
    w_v,
    b_v,
    w_o,
    b_o,
    ln2_gain,
    ln2_bias,
    w_up,
    b_up,
    w_down,
    b_down,
):
    own_images, half_len, width = tokens.shape
    n_t = lax.axis_size("tensor")
    piece, head_width = w_q.shape
    local_heads = head_width // HD
    hidden_width = w_up.shape[1]
    rows = own_images * half_len
    images = n_t * own_images

    pad_hidden = (-hidden_width) % 128
    pad_out = (-head_width) % 128
    vector_rows = jnp.stack([ln1_gain, ln1_bias, b_o, ln2_gain, ln2_bias, b_down], axis=1)
    vectors, valid_count = gather_vectors(vector_rows, jnp.sum(valid_len.astype(jnp.int32)))
    valid_count = valid_count.astype(F32)
    valid_count, tokens = lax.optimization_barrier((valid_count, tokens))
    attn_pack = jnp.stack([w_q, w_k, w_v, w_o.T])
    attn_full = lax.all_gather(attn_pack, ("dp", "ctx"), axis=1, tiled=True)
    mlp_pack = jnp.pad(jnp.stack([w_up, w_down.T]), ((0, 0), (0, 0), (0, pad_hidden)))
    mlp_full = lax.all_gather(mlp_pack, ("dp", "ctx"), axis=1, tiled=True)
    qkv_w = attn_full[:3].reshape(3, width, local_heads, HD)
    out_wt = attn_full[3]
    vectors = vectors.astype(F32)
    gain_one, shift_one, out_bias, gain_two, shift_two, down_bias = [
        vectors[:, i] for i in range(6)
    ]
    up_w, down_wt = mlp_full[0], mlp_full[1]
    up_b = jnp.pad(b_up.astype(F32), (0, pad_hidden))

    out_per_head = out_wt.reshape(width, local_heads, HD)
    qkv_bias = jnp.stack(
        [b_q.astype(F32), jnp.zeros((head_width,), F32), b_v.astype(F32)]
    ).reshape(3, 1, local_heads, 1, HD)

    inputs = tokens.astype(F32).reshape(rows, width)
    normed, unit_one, inverse_one = norm_forward(inputs, gain_one, shift_one)
    normed_every_row = tensor_gather(normed.astype(BF)).reshape(images, half_len, width)
    qkv_rows = (
        jnp.einsum("pro,tojx->tpjrx", normed_every_row, qkv_w, preferred_element_type=F32)
        + qkv_bias
    ).astype(BF)
    queries, key_rows, value_rows = qkv_rows[0], qkv_rows[1], qkv_rows[2]
    key_all = ctx_gather(key_rows)
    value_all = ctx_gather(value_rows)
    usable = key_positions(half_len) < REAL
    score_scale = HD ** (-0.5)

    raw_scores = jnp.einsum("bhqe,bhke->bhqk", queries, key_all, preferred_element_type=F32)
    scores = jnp.where(usable, raw_scores * score_scale, -1e30)
    summit = jnp.max(scores, axis=-1, keepdims=True)
    exp_total = jnp.sum(jnp.exp(scores - summit), axis=-1, keepdims=True)
    log_totals = summit + jnp.log(exp_total)
    soft_weights = jnp.exp(scores - log_totals).astype(BF)
    mixed_per_head = jnp.einsum(
        "bhqk,bhke->bhqe", soft_weights, value_all, preferred_element_type=F32
    ).astype(BF)

    attn_terms = jnp.einsum(
        "lscm,dsm->lcd", mixed_per_head, out_per_head, preferred_element_type=F32
    )
    attn_sum = tensor_reduce(attn_terms.reshape(n_t, rows, width))
    hidden = inputs + attn_sum + out_bias
    normed_two, unit_two, inverse_two = norm_forward(hidden, gain_two, shift_two)
    normed_two_parts = tensor_gather_parts(normed_two.astype(BF))
    before_parts = [
        jnp.dot(part, up_w, preferred_element_type=F32) + up_b for part in normed_two_parts
    ]
    active_parts = [gelu_tanh(part).astype(BF) for part in before_parts]
    mlp_terms = [
        jnp.einsum("rf,df->rd", part, down_wt, preferred_element_type=F32)
        for part in active_parts
    ]
    result = hidden + tensor_reduce_parts(mlp_terms) + down_bias
    layer_out = result.astype(BF).reshape(own_images, half_len, width)

    position = lax.axis_index("ctx") * half_len + jnp.arange(half_len)
    valid_rows = (position[None, :] < valid_len[:, None]).astype(F32).reshape(rows)
    error_rows = result - teacher.astype(F32).reshape(rows, width)
    partial_value = 0.5 * jnp.sum(valid_rows * jnp.mean(error_rows * error_rows, axis=-1))
    slot_total = own_images * lax.axis_size("dp") * n_t
    factor = slot_total * (half_len * lax.axis_size("ctx")) / valid_count
    grad_out = error_rows * (valid_rows[:, None] * factor)

    grad_parts = tensor_gather_parts(grad_out.astype(BF))
    before_grad_parts = [
        (
            jnp.einsum("rd,df->rf", g, down_wt, preferred_element_type=F32)
            * gelu_slope(p)
        ).astype(BF)
        for g, p in zip(grad_parts, before_parts)
    ]
    norm_two_terms = [
        jnp.einsum("rf,df->rd", g, up_w, preferred_element_type=F32)
        for g in before_grad_parts
    ]
    down_grad_t = None
    up_grad = None
    for g, a_part, n_part, p_grad in zip(
        grad_parts, active_parts, normed_two_parts, before_grad_parts
    ):
        down_term = jnp.einsum("rd,rf->df", g, a_part, preferred_element_type=F32)
        up_term = jnp.einsum("rd,rf->df", n_part, p_grad, preferred_element_type=F32)
        down_grad_t = down_term if down_grad_t is None else down_grad_t + down_term
        up_grad = up_term if up_grad is None else up_grad + up_term
    before_grad = jnp.concatenate(before_grad_parts)
    up_bias_grad = jnp.sum(before_grad[:, :hidden_width], axis=0, dtype=F32)
    mlp_grad_pack = jnp.concatenate([up_grad.astype(BF), down_grad_t.astype(BF)], axis=1)
    mlp_grads = lax.psum_scatter(
        mlp_grad_pack, ("dp", "ctx"), scatter_dimension=0, tiled=True
    )
    norm_two_grad = tensor_reduce_parts(norm_two_terms)
    hidden_back, gain_two_grad, shift_two_grad = norm_backward(
        norm_two_grad, unit_two, inverse_two, gain_two
    )
    hidden_grad = grad_out + hidden_back
    down_bias_grad = jnp.sum(grad_out, axis=0)
    out_bias_grad = jnp.sum(hidden_grad, axis=0)
    hidden_token_rows = tensor_gather(hidden_grad.astype(BF)).reshape(images, half_len, width)
    out_grad_t = jnp.einsum(
        "lcd,lscm->dsm", hidden_token_rows, mixed_per_head, preferred_element_type=F32
    ).reshape(width, head_width)
    mixed_grad = jnp.einsum(
        "lcd,dsm->lscm", hidden_token_rows, out_per_head, preferred_element_type=F32
    ).astype(BF)

    soft_full = jnp.exp(scores - log_totals)
    soft_grad = jnp.einsum("bhqe,bhke->bhqk", mixed_grad, value_all, preferred_element_type=F32)
    value_grads = jnp.einsum(
        "bhqk,bhqe->bhke", soft_full.astype(BF), mixed_grad, preferred_element_type=F32
    )
    inner_sum = jnp.sum(soft_full * soft_grad, axis=-1, keepdims=True)
    score_grad = (soft_full * (soft_grad - inner_sum)).astype(BF)
    query_grads = (
        jnp.einsum("bhqk,bhke->bhqe", score_grad, key_all, preferred_element_type=F32)
        * score_scale
    )
    key_grads = (
        jnp.einsum("bhqk,bhqe->bhke", score_grad, queries, preferred_element_type=F32)
        * score_scale
    )
    key_reduced_precision = ctx_reduce(key_grads, half_len).astype(BF)
    value_reduced_precision = ctx_reduce(value_grads, half_len).astype(BF)
    query_reduced_precision = query_grads.astype(BF)
    query_bias_grad = jnp.sum(query_reduced_precision, axis=(0, 2), dtype=F32).reshape(head_width)
    value_bias_grad = jnp.sum(value_reduced_precision, axis=(0, 2), dtype=F32).reshape(head_width)
    qkv_grads = jnp.stack(
        [query_reduced_precision, key_reduced_precision, value_reduced_precision]
    )
    qkv_weight_grad = jnp.einsum(
        "okz,toaks->ztas", normed_every_row, qkv_grads, preferred_element_type=F32
    ).reshape(width, 3 * head_width)
    attn_grads = halving_reduce_scatter(
        jnp.concatenate([jnp.pad(out_grad_t, ((0, 0), (0, pad_out))), qkv_weight_grad], axis=1)
    )
    norm_one_terms = jnp.einsum(
        "toaks,tzas->okz", qkv_grads, qkv_w, preferred_element_type=F32
    )
    norm_one_grad = tensor_reduce(norm_one_terms.reshape(n_t, rows, width))
    input_back, gain_one_grad, shift_one_grad = norm_backward(
        norm_one_grad, unit_one, inverse_one, gain_one
    )
    tokens_grad = (hidden_grad + input_back).reshape(own_images, half_len, width)

    row_sums = jnp.concatenate(
        [
            gain_one_grad,
            shift_one_grad,
            out_bias_grad,
            gain_two_grad,
            shift_two_grad,
            down_bias_grad,
            partial_value.reshape(1),
        ]
    )
    head_sums = jnp.concatenate([query_bias_grad, value_bias_grad, up_bias_grad])
    row_sums, head_sums = tree_sum((row_sums, head_sums), ("ctx", "dp"))
    row_sums = tree_sum(row_sums, ("tensor",))
    loss_value = row_sums[6 * width] / valid_count
    piece_start = lax.axis_index(("dp", "ctx")) * piece
    vector_shards = [
        lax.dynamic_slice_in_dim(row_sums, i * width + piece_start, piece) for i in range(6)
    ]
    query_bias_sum = head_sums[:head_width]
    value_bias_sum = head_sums[head_width : 2 * head_width]
    up_bias_sum = head_sums[2 * head_width :]
    mlp_grads = mlp_grads.astype(F32)
    out_cols = head_width + pad_out
    attn_grads = [
        attn_grads[:, out_cols + i * head_width : out_cols + (i + 1) * head_width]
        for i in range(3)
    ] + [attn_grads[:, :head_width]]
    hidden_cols = hidden_width + pad_hidden
    mlp_grads = [
        mlp_grads[:, :hidden_width],
        mlp_grads[:, hidden_cols : hidden_cols + hidden_width],
    ]
    return (
        layer_out,
        loss_value,
        tokens_grad,
        vector_shards[0],
        vector_shards[1],
        attn_grads[0],
        query_bias_sum,
        attn_grads[1],
        attn_grads[2],
        value_bias_sum,
        attn_grads[3].T,
        vector_shards[2],
        vector_shards[3],
        vector_shards[4],
        mlp_grads[0],
        up_bias_sum,
        mlp_grads[1].T,
        vector_shards[5],
    )


def solution(mesh):
    return jax.shard_map(
        on_device_body,
        mesh=mesh,
        in_specs=(
            P(("dp", "tensor"), "ctx", None),
            P(("dp", "tensor"), "ctx", None),
            P(("dp", "tensor")),
            P(("dp", "ctx")),
            P(("dp", "ctx")),
            P(("dp", "ctx"), "tensor"),
            P("tensor"),
            P(("dp", "ctx"), "tensor"),
            P(("dp", "ctx"), "tensor"),
            P("tensor"),
            P("tensor", ("dp", "ctx")),
            P(("dp", "ctx")),
            P(("dp", "ctx")),
            P(("dp", "ctx")),
            P(("dp", "ctx"), "tensor"),
            P("tensor"),
            P("tensor", ("dp", "ctx")),
            P(("dp", "ctx")),
        ),
        out_specs=(
            P(("dp", "tensor"), "ctx", None),
            P(),
            P(("dp", "tensor"), "ctx", None),
            P(("dp", "ctx")),
            P(("dp", "ctx")),
            P(("dp", "ctx"), "tensor"),
            P("tensor"),
            P(("dp", "ctx"), "tensor"),
            P(("dp", "ctx"), "tensor"),
            P("tensor"),
            P("tensor", ("dp", "ctx")),
            P(("dp", "ctx")),
            P(("dp", "ctx")),
            P(("dp", "ctx")),
            P(("dp", "ctx"), "tensor"),
            P("tensor"),
            P("tensor", ("dp", "ctx")),
            P(("dp", "ctx")),
        ),
        check_vma=False,
    )
```

```python
import jax
import jax.numpy as jnp
from jax import lax
from jax.sharding import PartitionSpec as P


HD = 72
REAL = 729


EPSILON = 1e-06
GELU_C = 0.7978845608028654
GELU_K = 0.044715
BF = jnp.bfloat16
F32 = jnp.float32


def norm_forward(row_values, gain_vec, shift_vec):
    average = jnp.mean(row_values, axis=-1, keepdims=True)
    centred = row_values - average
    spread = jnp.mean(centred * centred, axis=-1, keepdims=True)
    inverse = lax.rsqrt(spread + EPSILON)
    unit_rows = centred * inverse
    return (unit_rows * gain_vec + shift_vec, unit_rows, inverse)


def norm_backward(upstream, unit_rows, inverse, gain_vec):
    scaled = upstream * gain_vec
    inner_sum = (
        scaled
        - jnp.mean(scaled, axis=-1, keepdims=True)
        - unit_rows * jnp.mean(scaled * unit_rows, axis=-1, keepdims=True)
    )
    return (inner_sum * inverse, jnp.sum(upstream * unit_rows, axis=0), jnp.sum(upstream, axis=0))


def gelu_tanh(values):
    return 0.5 * values * (1.0 + jnp.tanh(GELU_C * (values + GELU_K * values * values * values)))


def gelu_slope(values):
    tanh_part = jnp.tanh(GELU_C * (values + GELU_K * values * values * values))
    return 0.5 * (1.0 + tanh_part) + 0.5 * values * (1.0 - tanh_part * tanh_part) * GELU_C * (
        1.0 + 3.0 * GELU_K * values * values
    )


def swap(values, axis):
    return lax.ppermute(values, axis, [(0, 1), (1, 0)])


def tensor_gather(values):
    if lax.axis_size("tensor") == 2:
        return jnp.stack([values, swap(values, "tensor")])
    return lax.all_gather(values, "tensor", axis=0)


def tensor_reduce(partials):
    if lax.axis_size("tensor") == 2:
        return partials[0] + swap(partials[1].astype(BF), "tensor").astype(F32)
    return lax.psum_scatter(partials.astype(BF), "tensor", scatter_dimension=0).astype(F32)


def tensor_gather_parts(values):
    if lax.axis_size("tensor") == 2:
        return [values, swap(values, "tensor")]
    gathered = lax.all_gather(values, "tensor", axis=0)
    return [gathered[i] for i in range(gathered.shape[0])]


def tensor_reduce_parts(parts):
    if lax.axis_size("tensor") == 2:
        other = swap(parts[1].astype(BF), "tensor")
        return lax.optimization_barrier(parts[0]) + other.astype(F32)
    return lax.psum_scatter(
        jnp.stack(parts).astype(BF), "tensor", scatter_dimension=0
    ).astype(F32)


def ctx_gather(values):
    if lax.axis_size("ctx") == 2:
        return jnp.concatenate([values, swap(values, "ctx")], axis=2)
    return lax.all_gather(values, "ctx", axis=2, tiled=True)


def ctx_reduce(values, half_len):
    if lax.axis_size("ctx") == 2:
        other = swap(values[:, :, half_len:].astype(BF), "ctx")
        return values[:, :, :half_len] + other.astype(F32)
    return lax.psum_scatter(
        values.astype(BF), "ctx", scatter_dimension=2, tiled=True
    ).astype(F32)


def key_positions(half_len):
    n_ctx = lax.axis_size("ctx")
    local = jnp.arange(half_len * n_ctx)
    if n_ctx == 2:
        me = lax.axis_index("ctx")
        block = jnp.where(local < half_len, me, 1 - me)
        return block * half_len + local % half_len
    return local


def tree_sum(values, axes):
    for axis in axes:
        size = lax.axis_size(axis)
        if size & (size - 1):
            values = jax.tree.map(lambda v: lax.psum(v, axis), values)
            continue
        step = 1
        while step < size:
            perm = [(i, i ^ step) for i in range(size)]
            values = jax.tree.map(lambda v: v + lax.ppermute(v, axis, perm), values)
            step *= 2
    return values


def gather_vectors(block, count):
    n_ctx = lax.axis_size("ctx")
    n_dp = lax.axis_size("dp")
    if n_ctx != 2 or n_dp & (n_dp - 1):
        gathered = lax.all_gather(block, ("dp", "ctx"), axis=0, tiled=True)
        return gathered, tree_sum(count, ("tensor", "dp"))
    count = tree_sum(count, ("tensor",))
    other = swap(block, "ctx")
    first = lax.axis_index("ctx") == 0
    blocks = jnp.where(first, jnp.stack([block, other]), jnp.stack([other, block]))
    dp_index = lax.axis_index("dp")
    step = 1
    while step < n_dp:
        perm = [(i, i ^ step) for i in range(n_dp)]
        their_blocks, their_count = lax.ppermute((blocks, count), "dp", perm)
        low = (dp_index // step) % 2 == 0
        blocks = jnp.where(
            low,
            jnp.concatenate([blocks, their_blocks]),
            jnp.concatenate([their_blocks, blocks]),
        )
        count = count + their_count
        step *= 2
    return blocks.reshape(-1, block.shape[1]), count


def on_device_body(
    tokens,
    teacher,
    valid_len,
    ln1_gain,
    ln1_bias,
    w_q,
    b_q,
    w_k,
    w_v,
    b_v,
    w_o,
    b_o,
    ln2_gain,
    ln2_bias,
    w_up,
    b_up,
    w_down,
    b_down,
):
    own_images, half_len, width = tokens.shape
    n_t = lax.axis_size("tensor")
    piece, head_width = w_q.shape
    local_heads = head_width // HD
    hidden_width = w_up.shape[1]
    rows = own_images * half_len
    images = n_t * own_images

    pad_hidden = (-hidden_width) % 128
    pad_out = (-head_width) % 128
    vector_rows = jnp.stack([ln1_gain, ln1_bias, b_o, ln2_gain, ln2_bias, b_down], axis=1)
    vectors, valid_count = gather_vectors(vector_rows, jnp.sum(valid_len.astype(jnp.int32)))
    valid_count = valid_count.astype(F32)
    valid_count, tokens = lax.optimization_barrier((valid_count, tokens))
    attn_pack = jnp.stack([w_q, w_k, w_v, w_o.T])
    attn_full = lax.all_gather(attn_pack, ("dp", "ctx"), axis=1, tiled=True)
    mlp_pack = jnp.pad(jnp.stack([w_up, w_down.T]), ((0, 0), (0, 0), (0, pad_hidden)))
    mlp_full = lax.all_gather(mlp_pack, ("dp", "ctx"), axis=1, tiled=True)
    qkv_w = attn_full[:3].reshape(3, width, local_heads, HD)
    out_wt = attn_full[3]
    vectors = vectors.astype(F32)
    gain_one, shift_one, out_bias, gain_two, shift_two, down_bias = [
        vectors[:, i] for i in range(6)
    ]
    up_w, down_wt = mlp_full[0], mlp_full[1]
    up_b = jnp.pad(b_up.astype(F32), (0, pad_hidden))

    out_per_head = out_wt.reshape(width, local_heads, HD)
    qkv_bias = jnp.stack(
        [b_q.astype(F32), jnp.zeros((head_width,), F32), b_v.astype(F32)]
    ).reshape(3, 1, local_heads, 1, HD)

    inputs = tokens.astype(F32).reshape(rows, width)
    normed, unit_one, inverse_one = norm_forward(inputs, gain_one, shift_one)
    normed_every_row = tensor_gather(normed.astype(BF)).reshape(images, half_len, width)
    qkv_rows = (
        jnp.einsum("pro,tojx->tpjrx", normed_every_row, qkv_w, preferred_element_type=F32)
        + qkv_bias
    ).astype(BF)
    queries, key_rows, value_rows = qkv_rows[0], qkv_rows[1], qkv_rows[2]
    key_all = ctx_gather(key_rows)
    value_all = ctx_gather(value_rows)
    usable = key_positions(half_len) < REAL
    score_scale = HD ** (-0.5)

    raw_scores = jnp.einsum("bhqe,bhke->bhqk", queries, key_all, preferred_element_type=F32)
    scores = jnp.where(usable, raw_scores * score_scale, -1e30)
    summit = jnp.max(scores, axis=-1, keepdims=True)
    exp_total = jnp.sum(jnp.exp(scores - summit), axis=-1, keepdims=True)
    log_totals = summit + jnp.log(exp_total)
    soft_weights = jnp.exp(scores - log_totals).astype(BF)
    mixed_per_head = jnp.einsum(
        "bhqk,bhke->bhqe", soft_weights, value_all, preferred_element_type=F32
    ).astype(BF)

    attn_terms = jnp.einsum(
        "lscm,dsm->lcd", mixed_per_head, out_per_head, preferred_element_type=F32
    )
    attn_sum = tensor_reduce(attn_terms.reshape(n_t, rows, width))
    hidden = inputs + attn_sum + out_bias
    normed_two, unit_two, inverse_two = norm_forward(hidden, gain_two, shift_two)
    normed_two_parts = tensor_gather_parts(normed_two.astype(BF))
    before_parts = [
        jnp.dot(part, up_w, preferred_element_type=F32) + up_b for part in normed_two_parts
    ]
    active_parts = [gelu_tanh(part).astype(BF) for part in before_parts]
    mlp_terms = [
        jnp.einsum("rf,df->rd", part, down_wt, preferred_element_type=F32)
        for part in active_parts
    ]
    result = hidden + tensor_reduce_parts(mlp_terms) + down_bias
    layer_out = result.astype(BF).reshape(own_images, half_len, width)

    position = lax.axis_index("ctx") * half_len + jnp.arange(half_len)
    valid_rows = (position[None, :] < valid_len[:, None]).astype(F32).reshape(rows)
    error_rows = result - teacher.astype(F32).reshape(rows, width)
    partial_value = 0.5 * jnp.sum(valid_rows * jnp.mean(error_rows * error_rows, axis=-1))
    slot_total = own_images * lax.axis_size("dp") * n_t
    factor = slot_total * (half_len * lax.axis_size("ctx")) / valid_count
    grad_out = error_rows * (valid_rows[:, None] * factor)

    grad_parts = tensor_gather_parts(grad_out.astype(BF))
    before_grad_parts = [
        (
            jnp.einsum("rd,df->rf", g, down_wt, preferred_element_type=F32)
            * gelu_slope(p)
        ).astype(BF)
        for g, p in zip(grad_parts, before_parts)
    ]
    norm_two_terms = [
        jnp.einsum("rf,df->rd", g, up_w, preferred_element_type=F32)
        for g in before_grad_parts
    ]
    down_grad_t = None
    up_grad = None
    for g, a_part, n_part, p_grad in zip(
        grad_parts, active_parts, normed_two_parts, before_grad_parts
    ):
        down_term = jnp.einsum("rd,rf->df", g, a_part, preferred_element_type=F32)
        up_term = jnp.einsum("rd,rf->df", n_part, p_grad, preferred_element_type=F32)
        down_grad_t = down_term if down_grad_t is None else down_grad_t + down_term
        up_grad = up_term if up_grad is None else up_grad + up_term
    before_grad = jnp.concatenate(before_grad_parts)
    up_bias_grad = jnp.sum(before_grad[:, :hidden_width], axis=0, dtype=F32)
    mlp_grad_pack = jnp.concatenate([up_grad.astype(BF), down_grad_t.astype(BF)], axis=1)
    mlp_grads = lax.psum_scatter(
        mlp_grad_pack, ("dp", "ctx"), scatter_dimension=0, tiled=True
    )
    norm_two_grad = tensor_reduce_parts(norm_two_terms)
    hidden_back, gain_two_grad, shift_two_grad = norm_backward(
        norm_two_grad, unit_two, inverse_two, gain_two
    )
    hidden_grad = grad_out + hidden_back
    down_bias_grad = jnp.sum(grad_out, axis=0)
    out_bias_grad = jnp.sum(hidden_grad, axis=0)
    hidden_token_rows = tensor_gather(hidden_grad.astype(BF)).reshape(images, half_len, width)
    out_grad_t = jnp.einsum(
        "lcd,lscm->dsm", hidden_token_rows, mixed_per_head, preferred_element_type=F32
    ).reshape(width, head_width)
    mixed_grad = jnp.einsum(
        "lcd,dsm->lscm", hidden_token_rows, out_per_head, preferred_element_type=F32
    ).astype(BF)

    soft_full = jnp.exp(scores - log_totals)
    soft_grad = jnp.einsum("bhqe,bhke->bhqk", mixed_grad, value_all, preferred_element_type=F32)
    value_grads = jnp.einsum(
        "bhqk,bhqe->bhke", soft_full.astype(BF), mixed_grad, preferred_element_type=F32
    )
    inner_sum = jnp.sum(soft_full * soft_grad, axis=-1, keepdims=True)
    score_grad = (soft_full * (soft_grad - inner_sum)).astype(BF)
    query_grads = (
        jnp.einsum("bhqk,bhke->bhqe", score_grad, key_all, preferred_element_type=F32)
        * score_scale
    )
    key_grads = (
        jnp.einsum("bhqk,bhqe->bhke", score_grad, queries, preferred_element_type=F32)
        * score_scale
    )
    key_reduced_precision = ctx_reduce(key_grads, half_len).astype(BF)
    value_reduced_precision = ctx_reduce(value_grads, half_len).astype(BF)
    query_reduced_precision = query_grads.astype(BF)
    query_bias_grad = jnp.sum(query_reduced_precision, axis=(0, 2), dtype=F32).reshape(head_width)
    value_bias_grad = jnp.sum(value_reduced_precision, axis=(0, 2), dtype=F32).reshape(head_width)
    qkv_grads = jnp.stack(
        [query_reduced_precision, key_reduced_precision, value_reduced_precision]
    )
    qkv_weight_grad = jnp.einsum(
        "okz,toaks->ztas", normed_every_row, qkv_grads, preferred_element_type=F32
    ).reshape(width, 3 * head_width)
    attn_grads = lax.psum_scatter(
        jnp.concatenate(
            [jnp.pad(out_grad_t.astype(BF), ((0, 0), (0, pad_out))), qkv_weight_grad.astype(BF)],
            axis=1,
        ),
        ("dp", "ctx"),
        scatter_dimension=0,
        tiled=True,
    )
    norm_one_terms = jnp.einsum(
        "toaks,tzas->okz", qkv_grads, qkv_w, preferred_element_type=F32
    )
    norm_one_grad = tensor_reduce(norm_one_terms.reshape(n_t, rows, width))
    input_back, gain_one_grad, shift_one_grad = norm_backward(
        norm_one_grad, unit_one, inverse_one, gain_one
    )
    tokens_grad = (hidden_grad + input_back).reshape(own_images, half_len, width)

    row_sums = jnp.concatenate(
        [
            gain_one_grad,
            shift_one_grad,
            out_bias_grad,
            gain_two_grad,
            shift_two_grad,
            down_bias_grad,
            partial_value.reshape(1),
        ]
    )
    head_sums = jnp.concatenate([query_bias_grad, value_bias_grad, up_bias_grad])
    row_sums, head_sums = tree_sum((row_sums, head_sums), ("ctx", "dp"))
    row_sums = tree_sum(row_sums, ("tensor",))
    loss_value = row_sums[6 * width] / valid_count
    piece_start = lax.axis_index(("dp", "ctx")) * piece
    vector_shards = [
        lax.dynamic_slice_in_dim(row_sums, i * width + piece_start, piece) for i in range(6)
    ]
    query_bias_sum = head_sums[:head_width]
    value_bias_sum = head_sums[head_width : 2 * head_width]
    up_bias_sum = head_sums[2 * head_width :]
    attn_grads = attn_grads.astype(F32)
    mlp_grads = mlp_grads.astype(F32)
    out_cols = head_width + pad_out
    attn_grads = [
        attn_grads[:, out_cols + i * head_width : out_cols + (i + 1) * head_width]
        for i in range(3)
    ] + [attn_grads[:, :head_width]]
    hidden_cols = hidden_width + pad_hidden
    mlp_grads = [
        mlp_grads[:, :hidden_width],
        mlp_grads[:, hidden_cols : hidden_cols + hidden_width],
    ]
    return (
        layer_out,
        loss_value,
        tokens_grad,
        vector_shards[0],
        vector_shards[1],
        attn_grads[0],
        query_bias_sum,
        attn_grads[1],
        attn_grads[2],
        value_bias_sum,
        attn_grads[3].T,
        vector_shards[2],
        vector_shards[3],
        vector_shards[4],
        mlp_grads[0],
        up_bias_sum,
        mlp_grads[1].T,
        vector_shards[5],
    )


def solution(mesh):
    return jax.shard_map(
        on_device_body,
        mesh=mesh,
        in_specs=(
            P(("dp", "tensor"), "ctx", None),
            P(("dp", "tensor"), "ctx", None),
            P(("dp", "tensor")),
            P(("dp", "ctx")),
            P(("dp", "ctx")),
            P(("dp", "ctx"), "tensor"),
            P("tensor"),
            P(("dp", "ctx"), "tensor"),
            P(("dp", "ctx"), "tensor"),
            P("tensor"),
            P("tensor", ("dp", "ctx")),
            P(("dp", "ctx")),
            P(("dp", "ctx")),
            P(("dp", "ctx")),
            P(("dp", "ctx"), "tensor"),
            P("tensor"),
            P("tensor", ("dp", "ctx")),
            P(("dp", "ctx")),
        ),
        out_specs=(
            P(("dp", "tensor"), "ctx", None),
            P(),
            P(("dp", "tensor"), "ctx", None),
            P(("dp", "ctx")),
            P(("dp", "ctx")),
            P(("dp", "ctx"), "tensor"),
            P("tensor"),
            P(("dp", "ctx"), "tensor"),
            P(("dp", "ctx"), "tensor"),
            P("tensor"),
            P("tensor", ("dp", "ctx")),
            P(("dp", "ctx")),
            P(("dp", "ctx")),
            P(("dp", "ctx")),
            P(("dp", "ctx"), "tensor"),
            P("tensor"),
            P("tensor", ("dp", "ctx")),
            P(("dp", "ctx")),
        ),
        check_vma=False,
    )
```

```python
import jax
import jax.numpy as jnp
from jax import lax
from jax.sharding import PartitionSpec as P


HD = 72
REAL = 729


EPSILON = 1e-06
GELU_C = 0.7978845608028654
GELU_K = 0.044715
BF = jnp.bfloat16
F32 = jnp.float32


def norm_forward(row_values, gain_vec, shift_vec):
    average = jnp.mean(row_values, axis=-1, keepdims=True)
    centred = row_values - average
    spread = jnp.mean(centred * centred, axis=-1, keepdims=True)
    inverse = lax.rsqrt(spread + EPSILON)
    unit_rows = centred * inverse
    return (unit_rows * gain_vec + shift_vec, unit_rows, inverse)


def norm_backward(upstream, unit_rows, inverse, gain_vec):
    scaled = upstream * gain_vec
    inner_sum = (
        scaled
        - jnp.mean(scaled, axis=-1, keepdims=True)
        - unit_rows * jnp.mean(scaled * unit_rows, axis=-1, keepdims=True)
    )
    return (inner_sum * inverse, jnp.sum(upstream * unit_rows, axis=0), jnp.sum(upstream, axis=0))


def gelu_tanh(values):
    return 0.5 * values * (1.0 + jnp.tanh(GELU_C * (values + GELU_K * values * values * values)))


def gelu_slope(values):
    tanh_part = jnp.tanh(GELU_C * (values + GELU_K * values * values * values))
    return 0.5 * (1.0 + tanh_part) + 0.5 * values * (1.0 - tanh_part * tanh_part) * GELU_C * (
        1.0 + 3.0 * GELU_K * values * values
    )


def swap(values, axis):
    return lax.ppermute(values, axis, [(0, 1), (1, 0)])


def tensor_gather(values):
    if lax.axis_size("tensor") == 2:
        return jnp.stack([values, swap(values, "tensor")])
    return lax.all_gather(values, "tensor", axis=0)


def tensor_reduce(partials):
    if lax.axis_size("tensor") == 2:
        return partials[0] + swap(partials[1].astype(BF), "tensor").astype(F32)
    return lax.psum_scatter(partials.astype(BF), "tensor", scatter_dimension=0).astype(F32)


def tensor_gather_parts(values):
    if lax.axis_size("tensor") == 2:
        return [values, swap(values, "tensor")]
    gathered = lax.all_gather(values, "tensor", axis=0)
    return [gathered[i] for i in range(gathered.shape[0])]


def tensor_reduce_parts(parts):
    if lax.axis_size("tensor") == 2:
        other = swap(parts[1].astype(BF), "tensor")
        return lax.optimization_barrier(parts[0]) + other.astype(F32)
    return lax.psum_scatter(
        jnp.stack(parts).astype(BF), "tensor", scatter_dimension=0
    ).astype(F32)


def ctx_gather(values):
    if lax.axis_size("ctx") == 2:
        return jnp.concatenate([values, swap(values, "ctx")], axis=2)
    return lax.all_gather(values, "ctx", axis=2, tiled=True)


def ctx_reduce(values, half_len):
    if lax.axis_size("ctx") == 2:
        other = swap(values[:, :, half_len:].astype(BF), "ctx")
        return values[:, :, :half_len] + other.astype(F32)
    return lax.psum_scatter(
        values.astype(BF), "ctx", scatter_dimension=2, tiled=True
    ).astype(F32)


def key_positions(half_len):
    n_ctx = lax.axis_size("ctx")
    local = jnp.arange(half_len * n_ctx)
    if n_ctx == 2:
        me = lax.axis_index("ctx")
        block = jnp.where(local < half_len, me, 1 - me)
        return block * half_len + local % half_len
    return local


def tree_sum(values, axes):
    for axis in axes:
        size = lax.axis_size(axis)
        if size & (size - 1):
            values = jax.tree.map(lambda v: lax.psum(v, axis), values)
            continue
        step = 1
        while step < size:
            perm = [(i, i ^ step) for i in range(size)]
            values = jax.tree.map(lambda v: v + lax.ppermute(v, axis, perm), values)
            step *= 2
    return values


def gather_vectors(block, count):
    n_ctx = lax.axis_size("ctx")
    n_dp = lax.axis_size("dp")
    if n_ctx != 2 or n_dp & (n_dp - 1):
        gathered = lax.all_gather(block, ("dp", "ctx"), axis=0, tiled=True)
        return gathered, tree_sum(count, ("tensor", "dp"))
    count = tree_sum(count, ("tensor",))
    other = swap(block, "ctx")
    first = lax.axis_index("ctx") == 0
    blocks = jnp.where(first, jnp.stack([block, other]), jnp.stack([other, block]))
    dp_index = lax.axis_index("dp")
    step = 1
    while step < n_dp:
        perm = [(i, i ^ step) for i in range(n_dp)]
        their_blocks, their_count = lax.ppermute((blocks, count), "dp", perm)
        low = (dp_index // step) % 2 == 0
        blocks = jnp.where(
            low,
            jnp.concatenate([blocks, their_blocks]),
            jnp.concatenate([their_blocks, blocks]),
        )
        count = count + their_count
        step *= 2
    return blocks.reshape(-1, block.shape[1]), count


def on_device_body(
    tokens,
    teacher,
    valid_len,
    ln1_gain,
    ln1_bias,
    w_q,
    b_q,
    w_k,
    w_v,
    b_v,
    w_o,
    b_o,
    ln2_gain,
    ln2_bias,
    w_up,
    b_up,
    w_down,
    b_down,
):
    own_images, half_len, width = tokens.shape
    n_t = lax.axis_size("tensor")
    piece, head_width = w_q.shape
    local_heads = head_width // HD
    hidden_width = w_up.shape[1]
    rows = own_images * half_len
    images = n_t * own_images

    pad_hidden = (-hidden_width) % 128
    pad_out = (-head_width) % 128
    vector_rows = jnp.stack([ln1_gain, ln1_bias, b_o, ln2_gain, ln2_bias, b_down], axis=1)
    vectors, valid_count = gather_vectors(vector_rows, jnp.sum(valid_len.astype(jnp.int32)))
    valid_count = valid_count.astype(F32)
    valid_count, tokens = lax.optimization_barrier((valid_count, tokens))
    attn_pack = jnp.stack([w_q, w_k, w_v, w_o.T])
    attn_full = lax.all_gather(attn_pack, ("dp", "ctx"), axis=1, tiled=True)
    mlp_pack = jnp.pad(jnp.stack([w_up, w_down.T]), ((0, 0), (0, 0), (0, pad_hidden)))
    mlp_full = lax.all_gather(mlp_pack, ("dp", "ctx"), axis=1, tiled=True)
    qkv_w = attn_full[:3].reshape(3, width, local_heads, HD)
    out_wt = attn_full[3]
    vectors = vectors.astype(F32)
    gain_one, shift_one, out_bias, gain_two, shift_two, down_bias = [
        vectors[:, i] for i in range(6)
    ]
    up_w, down_wt = mlp_full[0], mlp_full[1]
    up_b = jnp.pad(b_up.astype(F32), (0, pad_hidden))

    out_per_head = out_wt.reshape(width, local_heads, HD)
    qkv_bias = jnp.stack(
        [b_q.astype(F32), jnp.zeros((head_width,), F32), b_v.astype(F32)]
    ).reshape(3, 1, local_heads, 1, HD)

    inputs = tokens.astype(F32).reshape(rows, width)
    normed, unit_one, inverse_one = norm_forward(inputs, gain_one, shift_one)
    normed_every_row = tensor_gather(normed.astype(BF)).reshape(images, half_len, width)
    qkv_rows = (
        jnp.einsum("pro,tojx->tpjrx", normed_every_row, qkv_w, preferred_element_type=F32)
        + qkv_bias
    ).astype(BF)
    queries, key_rows, value_rows = qkv_rows[0], qkv_rows[1], qkv_rows[2]
    key_all = ctx_gather(key_rows)
    value_all = ctx_gather(value_rows)
    usable = key_positions(half_len) < REAL
    score_scale = HD ** (-0.5)

    raw_scores = jnp.einsum("bhqe,bhke->bhqk", queries, key_all, preferred_element_type=F32)
    scores = jnp.where(usable, raw_scores * score_scale, -1e30)
    summit = jnp.max(scores, axis=-1, keepdims=True)
    exp_total = jnp.sum(jnp.exp(scores - summit), axis=-1, keepdims=True)
    log_totals = summit + jnp.log(exp_total)
    soft_weights = jnp.exp(scores - log_totals).astype(BF)
    mixed_per_head = jnp.einsum(
        "bhqk,bhke->bhqe", soft_weights, value_all, preferred_element_type=F32
    ).astype(BF)

    attn_terms = jnp.einsum(
        "lscm,dsm->lcd", mixed_per_head, out_per_head, preferred_element_type=F32
    )
    attn_sum = tensor_reduce(attn_terms.reshape(n_t, rows, width))
    hidden = inputs + attn_sum + out_bias
    normed_two, unit_two, inverse_two = norm_forward(hidden, gain_two, shift_two)
    normed_two_parts = tensor_gather_parts(normed_two.astype(BF))
    before_parts = [
        jnp.dot(part, up_w, preferred_element_type=F32) + up_b for part in normed_two_parts
    ]
    active_parts = [gelu_tanh(part).astype(BF) for part in before_parts]
    mlp_terms = [
        jnp.einsum("rf,df->rd", part, down_wt, preferred_element_type=F32)
        for part in active_parts
    ]
    result = hidden + tensor_reduce_parts(mlp_terms) + down_bias
    layer_out = result.astype(BF).reshape(own_images, half_len, width)

    position = lax.axis_index("ctx") * half_len + jnp.arange(half_len)
    valid_rows = (position[None, :] < valid_len[:, None]).astype(F32).reshape(rows)
    error_rows = result - teacher.astype(F32).reshape(rows, width)
    partial_value = 0.5 * jnp.sum(valid_rows * jnp.mean(error_rows * error_rows, axis=-1))
    slot_total = own_images * lax.axis_size("dp") * n_t
    factor = slot_total * (half_len * lax.axis_size("ctx")) / valid_count
    grad_out = error_rows * (valid_rows[:, None] * factor)

    grad_parts = tensor_gather_parts(grad_out.astype(BF))
    before_grad_parts = [
        (
            jnp.einsum("rd,df->rf", g, down_wt, preferred_element_type=F32)
            * gelu_slope(p)
        ).astype(BF)
        for g, p in zip(grad_parts, before_parts)
    ]
    norm_two_terms = [
        jnp.einsum("rf,df->rd", g, up_w, preferred_element_type=F32)
        for g in before_grad_parts
    ]
    down_grad_t = None
    up_grad = None
    for g, a_part, n_part, p_grad in zip(
        grad_parts, active_parts, normed_two_parts, before_grad_parts
    ):
        down_term = jnp.einsum("rd,rf->df", g, a_part, preferred_element_type=F32)
        up_term = jnp.einsum("rd,rf->df", n_part, p_grad, preferred_element_type=F32)
        down_grad_t = down_term if down_grad_t is None else down_grad_t + down_term
        up_grad = up_term if up_grad is None else up_grad + up_term
    before_grad = jnp.concatenate(before_grad_parts)
    up_bias_grad = jnp.sum(before_grad[:, :hidden_width], axis=0, dtype=F32)
    mlp_grad_pack = jnp.concatenate([up_grad.astype(BF), down_grad_t.astype(BF)], axis=1)
    mlp_grads = lax.psum_scatter(
        mlp_grad_pack, ("dp", "ctx"), scatter_dimension=0, tiled=True
    )
    norm_two_grad = tensor_reduce_parts(norm_two_terms)
    hidden_back, gain_two_grad, shift_two_grad = norm_backward(
        norm_two_grad, unit_two, inverse_two, gain_two
    )
    hidden_grad = grad_out + hidden_back
    down_bias_grad = jnp.sum(grad_out, axis=0)
    out_bias_grad = jnp.sum(hidden_grad, axis=0)
    hidden_token_parts = tensor_gather_parts(hidden_grad.astype(BF))
    out_grad_t = None
    query_parts, key_parts, value_parts = [], [], []
    for i, token_grad in enumerate(hidden_token_parts):
        sl = slice(i * own_images, (i + 1) * own_images)
        token_grad = token_grad.reshape(own_images, half_len, width)
        mixed_i = mixed_per_head[sl]
        out_term = jnp.einsum(
            "lcd,lscm->dsm", token_grad, mixed_i, preferred_element_type=F32
        ).reshape(width, head_width)
        out_grad_t = out_term if out_grad_t is None else out_grad_t + out_term
        mixed_grad = jnp.einsum(
            "lcd,dsm->lscm", token_grad, out_per_head, preferred_element_type=F32
        ).astype(BF)
        value_i = value_all[sl]
        key_i = key_all[sl]
        soft_full = jnp.exp(scores[sl] - log_totals[sl])
        soft_grad = jnp.einsum("bhqe,bhke->bhqk", mixed_grad, value_i, preferred_element_type=F32)
        value_parts.append(
            jnp.einsum(
                "bhqk,bhqe->bhke", soft_full.astype(BF), mixed_grad, preferred_element_type=F32
            )
        )
        inner_sum = jnp.sum(soft_full * soft_grad, axis=-1, keepdims=True)
        score_grad = (soft_full * (soft_grad - inner_sum)).astype(BF)
        query_parts.append(
            jnp.einsum("bhqk,bhke->bhqe", score_grad, key_i, preferred_element_type=F32)
            * score_scale
        )
        key_parts.append(
            jnp.einsum(
                "bhqk,bhqe->bhke", score_grad, queries[sl], preferred_element_type=F32
            )
            * score_scale
        )
    query_grads = jnp.concatenate(query_parts)
    key_grads = jnp.concatenate(key_parts)
    value_grads = jnp.concatenate(value_parts)
    key_reduced_precision = ctx_reduce(key_grads, half_len).astype(BF)
    value_reduced_precision = ctx_reduce(value_grads, half_len).astype(BF)
    query_reduced_precision = query_grads.astype(BF)
    query_bias_grad = jnp.sum(query_reduced_precision, axis=(0, 2), dtype=F32).reshape(head_width)
    value_bias_grad = jnp.sum(value_reduced_precision, axis=(0, 2), dtype=F32).reshape(head_width)
    qkv_grads = jnp.stack(
        [query_reduced_precision, key_reduced_precision, value_reduced_precision]
    )
    qkv_weight_grad = jnp.einsum(
        "okz,toaks->ztas", normed_every_row, qkv_grads, preferred_element_type=F32
    ).reshape(width, 3 * head_width)
    attn_grads = lax.psum_scatter(
        jnp.concatenate(
            [jnp.pad(out_grad_t.astype(BF), ((0, 0), (0, pad_out))), qkv_weight_grad.astype(BF)],
            axis=1,
        ),
        ("dp", "ctx"),
        scatter_dimension=0,
        tiled=True,
    )
    norm_one_terms = jnp.einsum(
        "toaks,tzas->okz", qkv_grads, qkv_w, preferred_element_type=F32
    )
    norm_one_grad = tensor_reduce(norm_one_terms.reshape(n_t, rows, width))
    input_back, gain_one_grad, shift_one_grad = norm_backward(
        norm_one_grad, unit_one, inverse_one, gain_one
    )
    tokens_grad = (hidden_grad + input_back).reshape(own_images, half_len, width)

    row_sums = jnp.concatenate(
        [
            gain_one_grad,
            shift_one_grad,
            out_bias_grad,
            gain_two_grad,
            shift_two_grad,
            down_bias_grad,
            partial_value.reshape(1),
        ]
    )
    head_sums = jnp.concatenate([query_bias_grad, value_bias_grad, up_bias_grad])
    row_sums, head_sums = tree_sum((row_sums, head_sums), ("ctx", "dp"))
    row_sums = tree_sum(row_sums, ("tensor",))
    loss_value = row_sums[6 * width] / valid_count
    piece_start = lax.axis_index(("dp", "ctx")) * piece
    vector_shards = [
        lax.dynamic_slice_in_dim(row_sums, i * width + piece_start, piece) for i in range(6)
    ]
    query_bias_sum = head_sums[:head_width]
    value_bias_sum = head_sums[head_width : 2 * head_width]
    up_bias_sum = head_sums[2 * head_width :]
    attn_grads = attn_grads.astype(F32)
    mlp_grads = mlp_grads.astype(F32)
    out_cols = head_width + pad_out
    attn_grads = [
        attn_grads[:, out_cols + i * head_width : out_cols + (i + 1) * head_width]
        for i in range(3)
    ] + [attn_grads[:, :head_width]]
    hidden_cols = hidden_width + pad_hidden
    mlp_grads = [
        mlp_grads[:, :hidden_width],
        mlp_grads[:, hidden_cols : hidden_cols + hidden_width],
    ]
    return (
        layer_out,
        loss_value,
        tokens_grad,
        vector_shards[0],
        vector_shards[1],
        attn_grads[0],
        query_bias_sum,
        attn_grads[1],
        attn_grads[2],
        value_bias_sum,
        attn_grads[3].T,
        vector_shards[2],
        vector_shards[3],
        vector_shards[4],
        mlp_grads[0],
        up_bias_sum,
        mlp_grads[1].T,
        vector_shards[5],
    )


def solution(mesh):
    return jax.shard_map(
        on_device_body,
        mesh=mesh,
        in_specs=(
            P(("dp", "tensor"), "ctx", None),
            P(("dp", "tensor"), "ctx", None),
            P(("dp", "tensor")),
            P(("dp", "ctx")),
            P(("dp", "ctx")),
            P(("dp", "ctx"), "tensor"),
            P("tensor"),
            P(("dp", "ctx"), "tensor"),
            P(("dp", "ctx"), "tensor"),
            P("tensor"),
            P("tensor", ("dp", "ctx")),
            P(("dp", "ctx")),
            P(("dp", "ctx")),
            P(("dp", "ctx")),
            P(("dp", "ctx"), "tensor"),
            P("tensor"),
            P("tensor", ("dp", "ctx")),
            P(("dp", "ctx")),
        ),
        out_specs=(
            P(("dp", "tensor"), "ctx", None),
            P(),
            P(("dp", "tensor"), "ctx", None),
            P(("dp", "ctx")),
            P(("dp", "ctx")),
            P(("dp", "ctx"), "tensor"),
            P("tensor"),
            P(("dp", "ctx"), "tensor"),
            P(("dp", "ctx"), "tensor"),
            P("tensor"),
            P("tensor", ("dp", "ctx")),
            P(("dp", "ctx")),
            P(("dp", "ctx")),
            P(("dp", "ctx")),
            P(("dp", "ctx"), "tensor"),
            P("tensor"),
            P("tensor", ("dp", "ctx")),
            P(("dp", "ctx")),
        ),
        check_vma=False,
    )
```

```python
import jax
import jax.numpy as jnp
from jax import lax
from jax.sharding import PartitionSpec as P


HD = 72
REAL = 729


EPSILON = 1e-06
GELU_C = 0.7978845608028654
GELU_K = 0.044715
BF = jnp.bfloat16
F32 = jnp.float32


def norm_forward(row_values, gain_vec, shift_vec):
    average = jnp.mean(row_values, axis=-1, keepdims=True)
    centred = row_values - average
    spread = jnp.mean(centred * centred, axis=-1, keepdims=True)
    inverse = lax.rsqrt(spread + EPSILON)
    unit_rows = centred * inverse
    return (unit_rows * gain_vec + shift_vec, unit_rows, inverse)


def norm_backward(upstream, unit_rows, inverse, gain_vec):
    scaled = upstream * gain_vec
    inner_sum = (
        scaled
        - jnp.mean(scaled, axis=-1, keepdims=True)
        - unit_rows * jnp.mean(scaled * unit_rows, axis=-1, keepdims=True)
    )
    return (inner_sum * inverse, jnp.sum(upstream * unit_rows, axis=0), jnp.sum(upstream, axis=0))


def gelu_tanh(values):
    return 0.5 * values * (1.0 + jnp.tanh(GELU_C * (values + GELU_K * values * values * values)))


def gelu_slope(values):
    tanh_part = jnp.tanh(GELU_C * (values + GELU_K * values * values * values))
    return 0.5 * (1.0 + tanh_part) + 0.5 * values * (1.0 - tanh_part * tanh_part) * GELU_C * (
        1.0 + 3.0 * GELU_K * values * values
    )


def swap(values, axis):
    return lax.ppermute(values, axis, [(0, 1), (1, 0)])


def tensor_gather(values):
    if lax.axis_size("tensor") == 2:
        return jnp.stack([values, swap(values, "tensor")])
    return lax.all_gather(values, "tensor", axis=0)


def tensor_reduce(partials):
    if lax.axis_size("tensor") == 2:
        return partials[0] + swap(partials[1].astype(BF), "tensor").astype(F32)
    return lax.psum_scatter(partials.astype(BF), "tensor", scatter_dimension=0).astype(F32)


def tensor_gather_parts(values):
    if lax.axis_size("tensor") == 2:
        return [values, swap(values, "tensor")]
    gathered = lax.all_gather(values, "tensor", axis=0)
    return [gathered[i] for i in range(gathered.shape[0])]


def tensor_reduce_parts(parts):
    if lax.axis_size("tensor") == 2:
        other = swap(parts[1].astype(BF), "tensor")
        return lax.optimization_barrier(parts[0]) + other.astype(F32)
    return lax.psum_scatter(
        jnp.stack(parts).astype(BF), "tensor", scatter_dimension=0
    ).astype(F32)


def ctx_gather(values):
    if lax.axis_size("ctx") == 2:
        return jnp.concatenate([values, swap(values, "ctx")], axis=2)
    return lax.all_gather(values, "ctx", axis=2, tiled=True)


def ctx_reduce(values, half_len):
    if lax.axis_size("ctx") == 2:
        other = swap(values[:, :, half_len:].astype(BF), "ctx")
        return values[:, :, :half_len] + other.astype(F32)
    return lax.psum_scatter(
        values.astype(BF), "ctx", scatter_dimension=2, tiled=True
    ).astype(F32)


def key_positions(half_len):
    n_ctx = lax.axis_size("ctx")
    local = jnp.arange(half_len * n_ctx)
    if n_ctx == 2:
        me = lax.axis_index("ctx")
        block = jnp.where(local < half_len, me, 1 - me)
        return block * half_len + local % half_len
    return local


def tree_sum(values, axes):
    for axis in axes:
        size = lax.axis_size(axis)
        if size & (size - 1):
            values = jax.tree.map(lambda v: lax.psum(v, axis), values)
            continue
        step = 1
        while step < size:
            perm = [(i, i ^ step) for i in range(size)]
            values = jax.tree.map(lambda v: v + lax.ppermute(v, axis, perm), values)
            step *= 2
    return values


def gather_vectors(block, count):
    n_ctx = lax.axis_size("ctx")
    n_dp = lax.axis_size("dp")
    if n_ctx != 2 or n_dp & (n_dp - 1):
        gathered = lax.all_gather(block, ("dp", "ctx"), axis=0, tiled=True)
        return gathered, tree_sum(count, ("tensor", "dp"))
    count = tree_sum(count, ("tensor",))
    other = swap(block, "ctx")
    first = lax.axis_index("ctx") == 0
    blocks = jnp.where(first, jnp.stack([block, other]), jnp.stack([other, block]))
    dp_index = lax.axis_index("dp")
    step = 1
    while step < n_dp:
        perm = [(i, i ^ step) for i in range(n_dp)]
        their_blocks, their_count = lax.ppermute((blocks, count), "dp", perm)
        low = (dp_index // step) % 2 == 0
        blocks = jnp.where(
            low,
            jnp.concatenate([blocks, their_blocks]),
            jnp.concatenate([their_blocks, blocks]),
        )
        count = count + their_count
        step *= 2
    return blocks.reshape(-1, block.shape[1]), count


def on_device_body(
    tokens,
    teacher,
    valid_len,
    ln1_gain,
    ln1_bias,
    w_q,
    b_q,
    w_k,
    w_v,
    b_v,
    w_o,
    b_o,
    ln2_gain,
    ln2_bias,
    w_up,
    b_up,
    w_down,
    b_down,
):
    own_images, half_len, width = tokens.shape
    n_t = lax.axis_size("tensor")
    piece, head_width = w_q.shape
    local_heads = head_width // HD
    hidden_width = w_up.shape[1]
    rows = own_images * half_len
    images = n_t * own_images

    pad_hidden = (-hidden_width) % 128
    pad_out = (-head_width) % 128
    vector_rows = jnp.stack([ln1_gain, ln1_bias, b_o, ln2_gain, ln2_bias, b_down], axis=1)
    vectors, valid_count = gather_vectors(vector_rows, jnp.sum(valid_len.astype(jnp.int32)))
    valid_count = valid_count.astype(F32)
    valid_count, tokens = lax.optimization_barrier((valid_count, tokens))
    attn_pack = jnp.stack([w_q, w_k, w_v, w_o.T])
    attn_full = lax.all_gather(attn_pack, ("dp", "ctx"), axis=1, tiled=True)
    mlp_pack = jnp.pad(jnp.stack([w_up, w_down.T]), ((0, 0), (0, 0), (0, pad_hidden)))
    mlp_full = lax.all_gather(mlp_pack, ("dp", "ctx"), axis=1, tiled=True)
    qkv_w = attn_full[:3].reshape(3, width, local_heads, HD)
    out_wt = attn_full[3]
    vectors = vectors.astype(F32)
    gain_one, shift_one, out_bias, gain_two, shift_two, down_bias = [
        vectors[:, i] for i in range(6)
    ]
    up_w, down_wt = mlp_full[0], mlp_full[1]
    up_b = jnp.pad(b_up.astype(F32), (0, pad_hidden))

    out_per_head = out_wt.reshape(width, local_heads, HD)
    qkv_bias = jnp.stack(
        [b_q.astype(F32), jnp.zeros((head_width,), F32), b_v.astype(F32)]
    ).reshape(3, 1, local_heads, 1, HD)

    inputs = tokens.astype(F32).reshape(rows, width)
    normed, unit_one, inverse_one = norm_forward(inputs, gain_one, shift_one)
    normed_every_row = tensor_gather(normed.astype(BF)).reshape(images, half_len, width)
    qkv_rows = (
        jnp.einsum("pro,tojx->tpjrx", normed_every_row, qkv_w, preferred_element_type=F32)
        + qkv_bias
    ).astype(BF)
    queries, key_rows, value_rows = qkv_rows[0], qkv_rows[1], qkv_rows[2]
    key_all = ctx_gather(key_rows)
    value_all = ctx_gather(value_rows)
    usable = key_positions(half_len) < REAL
    score_scale = HD ** (-0.5)

    raw_scores = jnp.einsum("bhqe,bhke->bhqk", queries, key_all, preferred_element_type=F32)
    scores = jnp.where(usable, raw_scores * score_scale, -1e30)
    summit = jnp.max(scores, axis=-1, keepdims=True)
    exp_total = jnp.sum(jnp.exp(scores - summit), axis=-1, keepdims=True)
    log_totals = summit + jnp.log(exp_total)
    soft_weights = jnp.exp(scores - log_totals).astype(BF)
    mixed_per_head = jnp.einsum(
        "bhqk,bhke->bhqe", soft_weights, value_all, preferred_element_type=F32
    ).astype(BF)

    attn_terms = jnp.einsum(
        "lscm,dsm->lcd", mixed_per_head, out_per_head, preferred_element_type=F32
    )
    attn_sum = tensor_reduce(attn_terms.reshape(n_t, rows, width))
    hidden = inputs + attn_sum + out_bias
    normed_two, unit_two, inverse_two = norm_forward(hidden, gain_two, shift_two)
    normed_two_parts = tensor_gather_parts(normed_two.astype(BF))
    before_parts = [
        jnp.dot(part, up_w, preferred_element_type=F32) + up_b for part in normed_two_parts
    ]
    active_parts = [gelu_tanh(part).astype(BF) for part in before_parts]
    slope_parts = [gelu_slope(part) for part in before_parts]
    if len(slope_parts) == 2:
        slope_parts[0], slope_parts[1], active_parts[0] = lax.optimization_barrier(
            (slope_parts[0], slope_parts[1], active_parts[0])
        )
    mlp_terms = [
        jnp.einsum("rf,df->rd", part, down_wt, preferred_element_type=F32)
        for part in active_parts
    ]
    result = hidden + tensor_reduce_parts(mlp_terms) + down_bias
    layer_out = result.astype(BF).reshape(own_images, half_len, width)

    position = lax.axis_index("ctx") * half_len + jnp.arange(half_len)
    valid_rows = (position[None, :] < valid_len[:, None]).astype(F32).reshape(rows)
    error_rows = result - teacher.astype(F32).reshape(rows, width)
    partial_value = 0.5 * jnp.sum(valid_rows * jnp.mean(error_rows * error_rows, axis=-1))
    slot_total = own_images * lax.axis_size("dp") * n_t
    factor = slot_total * (half_len * lax.axis_size("ctx")) / valid_count
    grad_out = error_rows * (valid_rows[:, None] * factor)

    grad_parts = tensor_gather_parts(grad_out.astype(BF))
    before_grad_parts = [
        (
            jnp.einsum("rd,df->rf", g, down_wt, preferred_element_type=F32)
            * p
        ).astype(BF)
        for g, p in zip(grad_parts, slope_parts)
    ]
    norm_two_terms = [
        jnp.einsum("rf,df->rd", g, up_w, preferred_element_type=F32)
        for g in before_grad_parts
    ]
    down_grad_t = None
    up_grad = None
    for g, a_part, n_part, p_grad in zip(
        grad_parts, active_parts, normed_two_parts, before_grad_parts
    ):
        down_term = jnp.einsum("rd,rf->df", g, a_part, preferred_element_type=F32)
        up_term = jnp.einsum("rd,rf->df", n_part, p_grad, preferred_element_type=F32)
        down_grad_t = down_term if down_grad_t is None else down_grad_t + down_term
        up_grad = up_term if up_grad is None else up_grad + up_term
    before_grad = jnp.concatenate(before_grad_parts)
    up_bias_grad = jnp.sum(before_grad[:, :hidden_width], axis=0, dtype=F32)
    mlp_grad_pack = jnp.concatenate([up_grad.astype(BF), down_grad_t.astype(BF)], axis=1)
    mlp_grads = lax.psum_scatter(
        mlp_grad_pack, ("dp", "ctx"), scatter_dimension=0, tiled=True
    )
    norm_two_grad = tensor_reduce_parts(norm_two_terms)
    hidden_back, gain_two_grad, shift_two_grad = norm_backward(
        norm_two_grad, unit_two, inverse_two, gain_two
    )
    hidden_grad = grad_out + hidden_back
    down_bias_grad = jnp.sum(grad_out, axis=0)
    out_bias_grad = jnp.sum(hidden_grad, axis=0)
    hidden_token_parts = tensor_gather_parts(hidden_grad.astype(BF))
    out_grad_t = None
    query_parts, key_parts, value_parts = [], [], []
    for i, token_grad in enumerate(hidden_token_parts):
        sl = slice(i * own_images, (i + 1) * own_images)
        token_grad = token_grad.reshape(own_images, half_len, width)
        mixed_i = mixed_per_head[sl]
        out_term = jnp.einsum(
            "lcd,lscm->dsm", token_grad, mixed_i, preferred_element_type=F32
        ).reshape(width, head_width)
        out_grad_t = out_term if out_grad_t is None else out_grad_t + out_term
        mixed_grad = jnp.einsum(
            "lcd,dsm->lscm", token_grad, out_per_head, preferred_element_type=F32
        ).astype(BF)
        value_i = value_all[sl]
        key_i = key_all[sl]
        soft_full = jnp.exp(scores[sl] - log_totals[sl])
        soft_grad = jnp.einsum("bhqe,bhke->bhqk", mixed_grad, value_i, preferred_element_type=F32)
        value_parts.append(
            jnp.einsum(
                "bhqk,bhqe->bhke", soft_full.astype(BF), mixed_grad, preferred_element_type=F32
            )
        )
        inner_sum = jnp.sum(soft_full * soft_grad, axis=-1, keepdims=True)
        score_grad = (soft_full * (soft_grad - inner_sum)).astype(BF)
        query_parts.append(
            jnp.einsum("bhqk,bhke->bhqe", score_grad, key_i, preferred_element_type=F32)
            * score_scale
        )
        key_parts.append(
            jnp.einsum(
                "bhqk,bhqe->bhke", score_grad, queries[sl], preferred_element_type=F32
            )
            * score_scale
        )
    query_grads = jnp.concatenate(query_parts)
    key_grads = jnp.concatenate(key_parts)
    value_grads = jnp.concatenate(value_parts)
    key_reduced_precision = ctx_reduce(key_grads, half_len).astype(BF)
    value_reduced_precision = ctx_reduce(value_grads, half_len).astype(BF)
    query_reduced_precision = query_grads.astype(BF)
    query_bias_grad = jnp.sum(query_reduced_precision, axis=(0, 2), dtype=F32).reshape(head_width)
    value_bias_grad = jnp.sum(value_reduced_precision, axis=(0, 2), dtype=F32).reshape(head_width)
    qkv_grads = jnp.stack(
        [query_reduced_precision, key_reduced_precision, value_reduced_precision]
    )
    qkv_weight_grad = jnp.einsum(
        "okz,toaks->ztas", normed_every_row, qkv_grads, preferred_element_type=F32
    ).reshape(width, 3 * head_width)
    attn_grads = lax.psum_scatter(
        jnp.concatenate(
            [jnp.pad(out_grad_t.astype(BF), ((0, 0), (0, pad_out))), qkv_weight_grad.astype(BF)],
            axis=1,
        ),
        ("dp", "ctx"),
        scatter_dimension=0,
        tiled=True,
    )
    norm_one_terms = jnp.einsum(
        "toaks,tzas->okz", qkv_grads, qkv_w, preferred_element_type=F32
    )
    norm_one_grad = tensor_reduce(norm_one_terms.reshape(n_t, rows, width))
    input_back, gain_one_grad, shift_one_grad = norm_backward(
        norm_one_grad, unit_one, inverse_one, gain_one
    )
    tokens_grad = (hidden_grad + input_back).reshape(own_images, half_len, width)

    row_sums = jnp.concatenate(
        [
            gain_one_grad,
            shift_one_grad,
            out_bias_grad,
            gain_two_grad,
            shift_two_grad,
            down_bias_grad,
            partial_value.reshape(1),
        ]
    )
    head_sums = jnp.concatenate([query_bias_grad, value_bias_grad, up_bias_grad])
    row_sums, head_sums = tree_sum((row_sums, head_sums), ("ctx", "dp"))
    row_sums = tree_sum(row_sums, ("tensor",))
    loss_value = row_sums[6 * width] / valid_count
    piece_start = lax.axis_index(("dp", "ctx")) * piece
    vector_shards = [
        lax.dynamic_slice_in_dim(row_sums, i * width + piece_start, piece) for i in range(6)
    ]
    query_bias_sum = head_sums[:head_width]
    value_bias_sum = head_sums[head_width : 2 * head_width]
    up_bias_sum = head_sums[2 * head_width :]
    attn_grads = attn_grads.astype(F32)
    mlp_grads = mlp_grads.astype(F32)
    out_cols = head_width + pad_out
    attn_grads = [
        attn_grads[:, out_cols + i * head_width : out_cols + (i + 1) * head_width]
        for i in range(3)
    ] + [attn_grads[:, :head_width]]
    hidden_cols = hidden_width + pad_hidden
    mlp_grads = [
        mlp_grads[:, :hidden_width],
        mlp_grads[:, hidden_cols : hidden_cols + hidden_width],
    ]
    return (
        layer_out,
        loss_value,
        tokens_grad,
        vector_shards[0],
        vector_shards[1],
        attn_grads[0],
        query_bias_sum,
        attn_grads[1],
        attn_grads[2],
        value_bias_sum,
        attn_grads[3].T,
        vector_shards[2],
        vector_shards[3],
        vector_shards[4],
        mlp_grads[0],
        up_bias_sum,
        mlp_grads[1].T,
        vector_shards[5],
    )


def solution(mesh):
    return jax.shard_map(
        on_device_body,
        mesh=mesh,
        in_specs=(
            P(("dp", "tensor"), "ctx", None),
            P(("dp", "tensor"), "ctx", None),
            P(("dp", "tensor")),
            P(("dp", "ctx")),
            P(("dp", "ctx")),
            P(("dp", "ctx"), "tensor"),
            P("tensor"),
            P(("dp", "ctx"), "tensor"),
            P(("dp", "ctx"), "tensor"),
            P("tensor"),
            P("tensor", ("dp", "ctx")),
            P(("dp", "ctx")),
            P(("dp", "ctx")),
            P(("dp", "ctx")),
            P(("dp", "ctx"), "tensor"),
            P("tensor"),
            P("tensor", ("dp", "ctx")),
            P(("dp", "ctx")),
        ),
        out_specs=(
            P(("dp", "tensor"), "ctx", None),
            P(),
            P(("dp", "tensor"), "ctx", None),
            P(("dp", "ctx")),
            P(("dp", "ctx")),
            P(("dp", "ctx"), "tensor"),
            P("tensor"),
            P(("dp", "ctx"), "tensor"),
            P(("dp", "ctx"), "tensor"),
            P("tensor"),
            P("tensor", ("dp", "ctx")),
            P(("dp", "ctx")),
            P(("dp", "ctx")),
            P(("dp", "ctx")),
            P(("dp", "ctx"), "tensor"),
            P("tensor"),
            P("tensor", ("dp", "ctx")),
            P(("dp", "ctx")),
        ),
        check_vma=False,
    )
```

```python
import jax
import jax.numpy as jnp
from jax import lax
from jax.sharding import PartitionSpec as P


HD = 72
REAL = 729


EPSILON = 1e-06
GELU_C = 0.7978845608028654
GELU_K = 0.044715
BF = jnp.bfloat16
F32 = jnp.float32


def norm_forward(row_values, gain_vec, shift_vec):
    average = jnp.mean(row_values, axis=-1, keepdims=True)
    centred = row_values - average
    spread = jnp.mean(centred * centred, axis=-1, keepdims=True)
    inverse = lax.rsqrt(spread + EPSILON)
    unit_rows = centred * inverse
    return (unit_rows * gain_vec + shift_vec, unit_rows, inverse)


def norm_backward(upstream, unit_rows, inverse, gain_vec):
    scaled = upstream * gain_vec
    inner_sum = (
        scaled
        - jnp.mean(scaled, axis=-1, keepdims=True)
        - unit_rows * jnp.mean(scaled * unit_rows, axis=-1, keepdims=True)
    )
    return (inner_sum * inverse, jnp.sum(upstream * unit_rows, axis=0), jnp.sum(upstream, axis=0))


def gelu_tanh(values):
    return 0.5 * values * (1.0 + jnp.tanh(GELU_C * (values + GELU_K * values * values * values)))


def gelu_slope(values):
    tanh_part = jnp.tanh(GELU_C * (values + GELU_K * values * values * values))
    return 0.5 * (1.0 + tanh_part) + 0.5 * values * (1.0 - tanh_part * tanh_part) * GELU_C * (
        1.0 + 3.0 * GELU_K * values * values
    )


def swap(values, axis):
    return lax.ppermute(values, axis, [(0, 1), (1, 0)])


def tensor_gather(values):
    if lax.axis_size("tensor") == 2:
        return jnp.stack([values, swap(values, "tensor")])
    return lax.all_gather(values, "tensor", axis=0)


def tensor_reduce(partials):
    if lax.axis_size("tensor") == 2:
        return partials[0] + swap(partials[1].astype(BF), "tensor").astype(F32)
    return lax.psum_scatter(partials.astype(BF), "tensor", scatter_dimension=0).astype(F32)


def tensor_gather_parts(values):
    if lax.axis_size("tensor") == 2:
        return [values, swap(values, "tensor")]
    gathered = lax.all_gather(values, "tensor", axis=0)
    return [gathered[i] for i in range(gathered.shape[0])]


def tensor_reduce_parts(parts):
    if lax.axis_size("tensor") == 2:
        other = swap(parts[1].astype(BF), "tensor")
        return lax.optimization_barrier(parts[0]) + other.astype(F32)
    return lax.psum_scatter(
        jnp.stack(parts).astype(BF), "tensor", scatter_dimension=0
    ).astype(F32)


def ctx_gather(values):
    if lax.axis_size("ctx") == 2:
        return jnp.concatenate([values, swap(values, "ctx")], axis=2)
    return lax.all_gather(values, "ctx", axis=2, tiled=True)


def ctx_reduce(values, half_len):
    if lax.axis_size("ctx") == 2:
        other = swap(values[:, :, half_len:].astype(BF), "ctx")
        return values[:, :, :half_len] + other.astype(F32)
    return lax.psum_scatter(
        values.astype(BF), "ctx", scatter_dimension=2, tiled=True
    ).astype(F32)


def key_positions(half_len):
    n_ctx = lax.axis_size("ctx")
    local = jnp.arange(half_len * n_ctx)
    if n_ctx == 2:
        me = lax.axis_index("ctx")
        block = jnp.where(local < half_len, me, 1 - me)
        return block * half_len + local % half_len
    return local


def tree_sum(values, axes):
    for axis in axes:
        size = lax.axis_size(axis)
        if size & (size - 1):
            values = jax.tree.map(lambda v: lax.psum(v, axis), values)
            continue
        step = 1
        while step < size:
            perm = [(i, i ^ step) for i in range(size)]
            values = jax.tree.map(lambda v: v + lax.ppermute(v, axis, perm), values)
            step *= 2
    return values


def gather_vectors(block, count):
    n_ctx = lax.axis_size("ctx")
    n_dp = lax.axis_size("dp")
    if n_ctx != 2 or n_dp & (n_dp - 1):
        gathered = lax.all_gather(block, ("dp", "ctx"), axis=0, tiled=True)
        return gathered, tree_sum(count, ("tensor", "dp"))
    count = tree_sum(count, ("tensor",))
    other = swap(block, "ctx")
    first = lax.axis_index("ctx") == 0
    blocks = jnp.where(first, jnp.stack([block, other]), jnp.stack([other, block]))
    dp_index = lax.axis_index("dp")
    step = 1
    while step < n_dp:
        perm = [(i, i ^ step) for i in range(n_dp)]
        their_blocks, their_count = lax.ppermute((blocks, count), "dp", perm)
        low = (dp_index // step) % 2 == 0
        blocks = jnp.where(
            low,
            jnp.concatenate([blocks, their_blocks]),
            jnp.concatenate([their_blocks, blocks]),
        )
        count = count + their_count
        step *= 2
    return blocks.reshape(-1, block.shape[1]), count


def on_device_body(
    tokens,
    teacher,
    valid_len,
    ln1_gain,
    ln1_bias,
    w_q,
    b_q,
    w_k,
    w_v,
    b_v,
    w_o,
    b_o,
    ln2_gain,
    ln2_bias,
    w_up,
    b_up,
    w_down,
    b_down,
):
    own_images, half_len, width = tokens.shape
    n_t = lax.axis_size("tensor")
    piece, head_width = w_q.shape
    local_heads = head_width // HD
    hidden_width = w_up.shape[1]
    rows = own_images * half_len
    images = n_t * own_images

    pad_hidden = (-hidden_width) % 128
    pad_out = (-head_width) % 128
    vector_rows = jnp.stack([ln1_gain, ln1_bias, b_o, ln2_gain, ln2_bias, b_down], axis=1)
    vectors, valid_count = gather_vectors(vector_rows, jnp.sum(valid_len.astype(jnp.int32)))
    valid_count = valid_count.astype(F32)
    valid_count, tokens = lax.optimization_barrier((valid_count, tokens))
    attn_pack = jnp.stack([w_q, w_k, w_v, w_o.T])
    attn_full = lax.all_gather(attn_pack, ("dp", "ctx"), axis=1, tiled=True)
    mlp_pack = jnp.pad(jnp.stack([w_up, w_down.T]), ((0, 0), (0, 0), (0, pad_hidden)))
    mlp_full = lax.all_gather(mlp_pack, ("dp", "ctx"), axis=1, tiled=True)
    qkv_w = attn_full[:3].reshape(3, width, local_heads, HD)
    out_wt = attn_full[3]
    vectors = vectors.astype(F32)
    gain_one, shift_one, out_bias, gain_two, shift_two, down_bias = [
        vectors[:, i] for i in range(6)
    ]
    up_w, down_wt = mlp_full[0], mlp_full[1]
    up_b = jnp.pad(b_up.astype(F32), (0, pad_hidden))

    out_per_head = out_wt.reshape(width, local_heads, HD)
    qkv_bias = jnp.stack(
        [b_q.astype(F32), jnp.zeros((head_width,), F32), b_v.astype(F32)]
    ).reshape(3, 1, local_heads, 1, HD)

    inputs = tokens.astype(F32).reshape(rows, width)
    normed, unit_one, inverse_one = norm_forward(inputs, gain_one, shift_one)
    normed_every_row = tensor_gather(normed.astype(BF)).reshape(images, half_len, width)
    qkv_rows = (
        jnp.einsum("pro,tojx->tpjrx", normed_every_row, qkv_w, preferred_element_type=F32)
        + qkv_bias
    ).astype(BF)
    queries, key_rows, value_rows = qkv_rows[0], qkv_rows[1], qkv_rows[2]
    key_all = ctx_gather(key_rows)
    value_all = ctx_gather(value_rows)
    usable = key_positions(half_len) < REAL
    score_scale = HD ** (-0.5)

    raw_scores = jnp.einsum("bhqe,bhke->bhqk", queries, key_all, preferred_element_type=F32)
    scores = jnp.where(usable, raw_scores * score_scale, -1e30)
    summit = jnp.max(scores, axis=-1, keepdims=True)
    exp_total = jnp.sum(jnp.exp(scores - summit), axis=-1, keepdims=True)
    log_totals = summit + jnp.log(exp_total)
    soft_weights = jnp.exp(scores - log_totals).astype(BF)
    mixed_per_head = jnp.einsum(
        "bhqk,bhke->bhqe", soft_weights, value_all, preferred_element_type=F32
    ).astype(BF)

    attn_terms = jnp.einsum(
        "lscm,dsm->lcd", mixed_per_head, out_per_head, preferred_element_type=F32
    )
    attn_sum = tensor_reduce(attn_terms.reshape(n_t, rows, width))
    hidden = inputs + attn_sum + out_bias
    normed_two, unit_two, inverse_two = norm_forward(hidden, gain_two, shift_two)
    normed_two_parts = tensor_gather_parts(normed_two.astype(BF))
    before_parts = [
        jnp.dot(part, up_w, preferred_element_type=F32) + up_b for part in normed_two_parts
    ]
    active_parts = [gelu_tanh(part).astype(BF) for part in before_parts]
    mlp_terms = [
        jnp.einsum("rf,df->rd", part, down_wt, preferred_element_type=F32)
        for part in active_parts
    ]
    result = hidden + tensor_reduce_parts(mlp_terms) + down_bias
    layer_out = result.astype(BF).reshape(own_images, half_len, width)

    position = lax.axis_index("ctx") * half_len + jnp.arange(half_len)
    valid_rows = (position[None, :] < valid_len[:, None]).astype(F32).reshape(rows)
    error_rows = result - teacher.astype(F32).reshape(rows, width)
    partial_value = 0.5 * jnp.sum(valid_rows * jnp.mean(error_rows * error_rows, axis=-1))
    slot_total = own_images * lax.axis_size("dp") * n_t
    factor = slot_total * (half_len * lax.axis_size("ctx")) / valid_count
    grad_out = error_rows * (valid_rows[:, None] * factor)

    grad_rows = grad_out.astype(BF)
    cut = (rows // 2) // 16 * 16
    if n_t == 2 and rows % 16 == 0 and cut > 0:
        chunks = [(grad_rows, active_parts[0], before_parts[0], normed_two_parts[0])]
        owners = [0]
        for lo, hi in ((0, cut), (cut, rows)):
            chunks.append(
                (
                    swap(grad_rows[lo:hi], "tensor"),
                    active_parts[1][lo:hi],
                    before_parts[1][lo:hi],
                    normed_two_parts[1][lo:hi],
                )
            )
            owners.append(1)
    else:
        grad_parts = tensor_gather_parts(grad_rows)
        chunks = list(zip(grad_parts, active_parts, before_parts, normed_two_parts))
        owners = list(range(len(chunks)))
    before_grad_chunks = [
        (
            jnp.einsum("rd,df->rf", g, down_wt, preferred_element_type=F32)
            * gelu_slope(p)
        ).astype(BF)
        for g, _, p, _ in chunks
    ]
    term_chunks = [
        jnp.einsum("rf,df->rd", g, up_w, preferred_element_type=F32)
        for g in before_grad_chunks
    ]
    norm_two_terms = [
        jnp.concatenate([t for t, o in zip(term_chunks, owners) if o == k])
        for k in range(n_t)
    ]
    down_grad_t = None
    up_grad = None
    up_bias_grad = None
    for (g, a_part, _, n_part), p_grad in zip(chunks, before_grad_chunks):
        down_term = jnp.einsum("rd,rf->df", g, a_part, preferred_element_type=F32)
        up_term = jnp.einsum("rd,rf->df", n_part, p_grad, preferred_element_type=F32)
        bias_term = jnp.sum(p_grad[:, :hidden_width], axis=0, dtype=F32)
        down_grad_t = down_term if down_grad_t is None else down_grad_t + down_term
        up_grad = up_term if up_grad is None else up_grad + up_term
        up_bias_grad = bias_term if up_bias_grad is None else up_bias_grad + bias_term
    mlp_grad_pack = jnp.concatenate([up_grad.astype(BF), down_grad_t.astype(BF)], axis=1)
    mlp_grads = lax.psum_scatter(
        mlp_grad_pack, ("dp", "ctx"), scatter_dimension=0, tiled=True
    )
    norm_two_grad = tensor_reduce_parts(norm_two_terms)
    hidden_back, gain_two_grad, shift_two_grad = norm_backward(
        norm_two_grad, unit_two, inverse_two, gain_two
    )
    hidden_grad = grad_out + hidden_back
    down_bias_grad = jnp.sum(grad_out, axis=0)
    out_bias_grad = jnp.sum(hidden_grad, axis=0)
    hidden_token_parts = tensor_gather_parts(hidden_grad.astype(BF))
    out_grad_t = None
    query_parts, key_parts, value_parts = [], [], []
    for i, token_grad in enumerate(hidden_token_parts):
        sl = slice(i * own_images, (i + 1) * own_images)
        token_grad = token_grad.reshape(own_images, half_len, width)
        mixed_i = mixed_per_head[sl]
        out_term = jnp.einsum(
            "lcd,lscm->dsm", token_grad, mixed_i, preferred_element_type=F32
        ).reshape(width, head_width)
        out_grad_t = out_term if out_grad_t is None else out_grad_t + out_term
        mixed_grad = jnp.einsum(
            "lcd,dsm->lscm", token_grad, out_per_head, preferred_element_type=F32
        ).astype(BF)
        value_i = value_all[sl]
        key_i = key_all[sl]
        soft_full = jnp.exp(scores[sl] - log_totals[sl])
        soft_grad = jnp.einsum("bhqe,bhke->bhqk", mixed_grad, value_i, preferred_element_type=F32)
        value_parts.append(
            jnp.einsum(
                "bhqk,bhqe->bhke", soft_full.astype(BF), mixed_grad, preferred_element_type=F32
            )
        )
        inner_sum = jnp.sum(soft_full * soft_grad, axis=-1, keepdims=True)
        score_grad = (soft_full * (soft_grad - inner_sum)).astype(BF)
        query_parts.append(
            jnp.einsum("bhqk,bhke->bhqe", score_grad, key_i, preferred_element_type=F32)
            * score_scale
        )
        key_parts.append(
            jnp.einsum(
                "bhqk,bhqe->bhke", score_grad, queries[sl], preferred_element_type=F32
            )
            * score_scale
        )
    query_grads = jnp.concatenate(query_parts)
    key_grads = jnp.concatenate(key_parts)
    value_grads = jnp.concatenate(value_parts)
    key_reduced_precision = ctx_reduce(key_grads, half_len).astype(BF)
    value_reduced_precision = ctx_reduce(value_grads, half_len).astype(BF)
    query_reduced_precision = query_grads.astype(BF)
    query_bias_grad = jnp.sum(query_reduced_precision, axis=(0, 2), dtype=F32).reshape(head_width)
    value_bias_grad = jnp.sum(value_reduced_precision, axis=(0, 2), dtype=F32).reshape(head_width)
    qkv_grads = jnp.stack(
        [query_reduced_precision, key_reduced_precision, value_reduced_precision]
    )
    qkv_weight_grad = jnp.einsum(
        "okz,toaks->ztas", normed_every_row, qkv_grads, preferred_element_type=F32
    ).reshape(width, 3 * head_width)
    attn_grads = lax.psum_scatter(
        jnp.concatenate(
            [jnp.pad(out_grad_t.astype(BF), ((0, 0), (0, pad_out))), qkv_weight_grad.astype(BF)],
            axis=1,
        ),
        ("dp", "ctx"),
        scatter_dimension=0,
        tiled=True,
    )
    norm_one_terms = jnp.einsum(
        "toaks,tzas->okz", qkv_grads, qkv_w, preferred_element_type=F32
    )
    norm_one_grad = tensor_reduce(norm_one_terms.reshape(n_t, rows, width))
    input_back, gain_one_grad, shift_one_grad = norm_backward(
        norm_one_grad, unit_one, inverse_one, gain_one
    )
    tokens_grad = (hidden_grad + input_back).reshape(own_images, half_len, width)

    row_sums = jnp.concatenate(
        [
            gain_one_grad,
            shift_one_grad,
            out_bias_grad,
            gain_two_grad,
            shift_two_grad,
            down_bias_grad,
            partial_value.reshape(1),
        ]
    )
    head_sums = jnp.concatenate([query_bias_grad, value_bias_grad, up_bias_grad])
    row_sums, head_sums = tree_sum((row_sums, head_sums), ("ctx", "dp"))
    row_sums = tree_sum(row_sums, ("tensor",))
    loss_value = row_sums[6 * width] / valid_count
    piece_start = lax.axis_index(("dp", "ctx")) * piece
    vector_shards = [
        lax.dynamic_slice_in_dim(row_sums, i * width + piece_start, piece) for i in range(6)
    ]
    query_bias_sum = head_sums[:head_width]
    value_bias_sum = head_sums[head_width : 2 * head_width]
    up_bias_sum = head_sums[2 * head_width :]
    attn_grads = attn_grads.astype(F32)
    mlp_grads = mlp_grads.astype(F32)
    out_cols = head_width + pad_out
    attn_grads = [
        attn_grads[:, out_cols + i * head_width : out_cols + (i + 1) * head_width]
        for i in range(3)
    ] + [attn_grads[:, :head_width]]
    hidden_cols = hidden_width + pad_hidden
    mlp_grads = [
        mlp_grads[:, :hidden_width],
        mlp_grads[:, hidden_cols : hidden_cols + hidden_width],
    ]
    return (
        layer_out,
        loss_value,
        tokens_grad,
        vector_shards[0],
        vector_shards[1],
        attn_grads[0],
        query_bias_sum,
        attn_grads[1],
        attn_grads[2],
        value_bias_sum,
        attn_grads[3].T,
        vector_shards[2],
        vector_shards[3],
        vector_shards[4],
        mlp_grads[0],
        up_bias_sum,
        mlp_grads[1].T,
        vector_shards[5],
    )


def solution(mesh):
    return jax.shard_map(
        on_device_body,
        mesh=mesh,
        in_specs=(
            P(("dp", "tensor"), "ctx", None),
            P(("dp", "tensor"), "ctx", None),
            P(("dp", "tensor")),
            P(("dp", "ctx")),
            P(("dp", "ctx")),
            P(("dp", "ctx"), "tensor"),
            P("tensor"),
            P(("dp", "ctx"), "tensor"),
            P(("dp", "ctx"), "tensor"),
            P("tensor"),
            P("tensor", ("dp", "ctx")),
            P(("dp", "ctx")),
            P(("dp", "ctx")),
            P(("dp", "ctx")),
            P(("dp", "ctx"), "tensor"),
            P("tensor"),
            P("tensor", ("dp", "ctx")),
            P(("dp", "ctx")),
        ),
        out_specs=(
            P(("dp", "tensor"), "ctx", None),
            P(),
            P(("dp", "tensor"), "ctx", None),
            P(("dp", "ctx")),
            P(("dp", "ctx")),
            P(("dp", "ctx"), "tensor"),
            P("tensor"),
            P(("dp", "ctx"), "tensor"),
            P(("dp", "ctx"), "tensor"),
            P("tensor"),
            P("tensor", ("dp", "ctx")),
            P(("dp", "ctx")),
            P(("dp", "ctx")),
            P(("dp", "ctx")),
            P(("dp", "ctx"), "tensor"),
            P("tensor"),
            P("tensor", ("dp", "ctx")),
            P(("dp", "ctx")),
        ),
        check_vma=False,
    )
```

```python
import jax
import jax.numpy as jnp
from jax import lax
from jax.sharding import PartitionSpec as P


HD = 72
REAL = 729


EPSILON = 1e-06
GELU_C = 0.7978845608028654
GELU_K = 0.044715
BF = jnp.bfloat16
F32 = jnp.float32


def norm_forward(row_values, gain_vec, shift_vec):
    average = jnp.mean(row_values, axis=-1, keepdims=True)
    centred = row_values - average
    spread = jnp.mean(centred * centred, axis=-1, keepdims=True)
    inverse = lax.rsqrt(spread + EPSILON)
    unit_rows = centred * inverse
    return (unit_rows * gain_vec + shift_vec, unit_rows, inverse)


def norm_backward(upstream, unit_rows, inverse, gain_vec):
    scaled = upstream * gain_vec
    inner_sum = (
        scaled
        - jnp.mean(scaled, axis=-1, keepdims=True)
        - unit_rows * jnp.mean(scaled * unit_rows, axis=-1, keepdims=True)
    )
    return (inner_sum * inverse, jnp.sum(upstream * unit_rows, axis=0), jnp.sum(upstream, axis=0))


def gelu_tanh(values):
    return 0.5 * values * (1.0 + jnp.tanh(GELU_C * (values + GELU_K * values * values * values)))


def gelu_slope(values):
    tanh_part = jnp.tanh(GELU_C * (values + GELU_K * values * values * values))
    return 0.5 * (1.0 + tanh_part) + 0.5 * values * (1.0 - tanh_part * tanh_part) * GELU_C * (
        1.0 + 3.0 * GELU_K * values * values
    )


def swap(values, axis):
    return lax.ppermute(values, axis, [(0, 1), (1, 0)])


def tensor_gather(values):
    if lax.axis_size("tensor") == 2:
        return jnp.stack([values, swap(values, "tensor")])
    return lax.all_gather(values, "tensor", axis=0)


def tensor_reduce(partials):
    if lax.axis_size("tensor") == 2:
        return partials[0] + swap(partials[1].astype(BF), "tensor").astype(F32)
    return lax.psum_scatter(partials.astype(BF), "tensor", scatter_dimension=0).astype(F32)


def tensor_gather_parts(values):
    if lax.axis_size("tensor") == 2:
        return [values, swap(values, "tensor")]
    gathered = lax.all_gather(values, "tensor", axis=0)
    return [gathered[i] for i in range(gathered.shape[0])]


def tensor_reduce_parts(parts):
    if lax.axis_size("tensor") == 2:
        other = swap(parts[1].astype(BF), "tensor")
        return lax.optimization_barrier(parts[0]) + other.astype(F32)
    return lax.psum_scatter(
        jnp.stack(parts).astype(BF), "tensor", scatter_dimension=0
    ).astype(F32)


def ctx_gather(values):
    if lax.axis_size("ctx") == 2:
        return jnp.concatenate([values, swap(values, "ctx")], axis=2)
    return lax.all_gather(values, "ctx", axis=2, tiled=True)


def ctx_reduce(values, half_len):
    if lax.axis_size("ctx") == 2:
        other = swap(values[:, :, half_len:].astype(BF), "ctx")
        return values[:, :, :half_len] + other.astype(F32)
    return lax.psum_scatter(
        values.astype(BF), "ctx", scatter_dimension=2, tiled=True
    ).astype(F32)


def key_positions(half_len):
    n_ctx = lax.axis_size("ctx")
    local = jnp.arange(half_len * n_ctx)
    if n_ctx == 2:
        me = lax.axis_index("ctx")
        block = jnp.where(local < half_len, me, 1 - me)
        return block * half_len + local % half_len
    return local


def tree_sum(values, axes):
    for axis in axes:
        size = lax.axis_size(axis)
        if size & (size - 1):
            values = jax.tree.map(lambda v: lax.psum(v, axis), values)
            continue
        step = 1
        while step < size:
            perm = [(i, i ^ step) for i in range(size)]
            values = jax.tree.map(lambda v: v + lax.ppermute(v, axis, perm), values)
            step *= 2
    return values


def gather_vectors(block, count):
    n_ctx = lax.axis_size("ctx")
    n_dp = lax.axis_size("dp")
    if n_ctx != 2 or n_dp & (n_dp - 1):
        gathered = lax.all_gather(block, ("dp", "ctx"), axis=0, tiled=True)
        return gathered, tree_sum(count, ("tensor", "dp"))
    count = tree_sum(count, ("tensor",))
    other = swap(block, "ctx")
    first = lax.axis_index("ctx") == 0
    blocks = jnp.where(first, jnp.stack([block, other]), jnp.stack([other, block]))
    dp_index = lax.axis_index("dp")
    step = 1
    while step < n_dp:
        perm = [(i, i ^ step) for i in range(n_dp)]
        their_blocks, their_count = lax.ppermute((blocks, count), "dp", perm)
        low = (dp_index // step) % 2 == 0
        blocks = jnp.where(
            low,
            jnp.concatenate([blocks, their_blocks]),
            jnp.concatenate([their_blocks, blocks]),
        )
        count = count + their_count
        step *= 2
    return blocks.reshape(-1, block.shape[1]), count


def on_device_body(
    tokens,
    teacher,
    valid_len,
    ln1_gain,
    ln1_bias,
    w_q,
    b_q,
    w_k,
    w_v,
    b_v,
    w_o,
    b_o,
    ln2_gain,
    ln2_bias,
    w_up,
    b_up,
    w_down,
    b_down,
):
    own_images, half_len, width = tokens.shape
    n_t = lax.axis_size("tensor")
    piece, head_width = w_q.shape
    local_heads = head_width // HD
    hidden_width = w_up.shape[1]
    rows = own_images * half_len
    images = n_t * own_images

    pad_hidden = (-hidden_width) % 128
    pad_out = (-head_width) % 128
    vector_rows = jnp.stack([ln1_gain, ln1_bias, b_o, ln2_gain, ln2_bias, b_down], axis=1)
    vectors, valid_count = gather_vectors(vector_rows, jnp.sum(valid_len.astype(jnp.int32)))
    valid_count = valid_count.astype(F32)
    valid_count, tokens = lax.optimization_barrier((valid_count, tokens))
    attn_pack = jnp.stack([w_q, w_k, w_v, w_o.T])
    attn_full = lax.all_gather(attn_pack, ("dp", "ctx"), axis=1, tiled=True)
    mlp_pack = jnp.pad(jnp.stack([w_up, w_down.T]), ((0, 0), (0, 0), (0, pad_hidden)))
    mlp_full = lax.all_gather(mlp_pack, ("dp", "ctx"), axis=1, tiled=True)
    qkv_w = attn_full[:3].reshape(3, width, local_heads, HD)
    out_wt = attn_full[3]
    vectors = vectors.astype(F32)
    gain_one, shift_one, out_bias, gain_two, shift_two, down_bias = [
        vectors[:, i] for i in range(6)
    ]
    up_w, down_wt = mlp_full[0], mlp_full[1]
    up_b = jnp.pad(b_up.astype(F32), (0, pad_hidden))

    out_per_head = out_wt.reshape(width, local_heads, HD)
    qkv_bias = jnp.stack(
        [b_q.astype(F32), jnp.zeros((head_width,), F32), b_v.astype(F32)]
    ).reshape(3, 1, local_heads, 1, HD)

    inputs = tokens.astype(F32).reshape(rows, width)
    normed, unit_one, inverse_one = norm_forward(inputs, gain_one, shift_one)
    normed_every_row = tensor_gather(normed.astype(BF)).reshape(images, half_len, width)
    qkv_rows = (
        jnp.einsum("pro,tojx->tpjrx", normed_every_row, qkv_w, preferred_element_type=F32)
        + qkv_bias
    ).astype(BF)
    queries, key_rows, value_rows = qkv_rows[0], qkv_rows[1], qkv_rows[2]
    key_all = ctx_gather(key_rows)
    value_all = ctx_gather(value_rows)
    usable = key_positions(half_len) < REAL
    score_scale = HD ** (-0.5)

    raw_scores = jnp.einsum("bhqe,bhke->bhqk", queries, key_all, preferred_element_type=F32)
    scores = jnp.where(usable, raw_scores * score_scale, -1e30)
    summit = jnp.max(scores, axis=-1, keepdims=True)
    exp_total = jnp.sum(jnp.exp(scores - summit), axis=-1, keepdims=True)
    log_totals = summit + jnp.log(exp_total)
    soft_weights = jnp.exp(scores - log_totals).astype(BF)
    mixed_per_head = jnp.einsum(
        "bhqk,bhke->bhqe", soft_weights, value_all, preferred_element_type=F32
    ).astype(BF)

    attn_terms = jnp.einsum(
        "lscm,dsm->lcd", mixed_per_head, out_per_head, preferred_element_type=F32
    )
    attn_sum = tensor_reduce(attn_terms.reshape(n_t, rows, width))
    hidden = inputs + attn_sum + out_bias
    normed_two, unit_two, inverse_two = norm_forward(hidden, gain_two, shift_two)
    normed_two_parts = tensor_gather_parts(normed_two.astype(BF))
    before_parts = [
        jnp.dot(part, up_w, preferred_element_type=F32) + up_b for part in normed_two_parts
    ]
    active_parts = [gelu_tanh(part).astype(BF) for part in before_parts]
    mlp_terms = [
        jnp.einsum("rf,df->rd", part, down_wt, preferred_element_type=F32)
        for part in active_parts
    ]
    result = hidden + tensor_reduce_parts(mlp_terms) + down_bias
    layer_out = result.astype(BF).reshape(own_images, half_len, width)

    position = lax.axis_index("ctx") * half_len + jnp.arange(half_len)
    valid_rows = (position[None, :] < valid_len[:, None]).astype(F32).reshape(rows)
    error_rows = result - teacher.astype(F32).reshape(rows, width)
    partial_value = 0.5 * jnp.sum(valid_rows * jnp.mean(error_rows * error_rows, axis=-1))
    slot_total = own_images * lax.axis_size("dp") * n_t
    factor = slot_total * (half_len * lax.axis_size("ctx")) / valid_count
    grad_out = error_rows * (valid_rows[:, None] * factor)

    grad_parts = tensor_gather_parts(grad_out.astype(BF))
    before_grad_parts = [
        (
            jnp.einsum("rd,df->rf", g, down_wt, preferred_element_type=F32)
            * gelu_slope(p)
        ).astype(BF)
        for g, p in zip(grad_parts, before_parts)
    ]
    norm_two_terms = [
        jnp.einsum("rf,df->rd", g, up_w, preferred_element_type=F32)
        for g in before_grad_parts
    ]
    down_grad_t = None
    up_grad = None
    for g, a_part, n_part, p_grad in zip(
        grad_parts, active_parts, normed_two_parts, before_grad_parts
    ):
        term_type = BF if down_grad_t is None else F32
        down_term = jnp.einsum("rd,rf->df", g, a_part, preferred_element_type=term_type)
        up_term = jnp.einsum("rd,rf->df", n_part, p_grad, preferred_element_type=term_type)
        if down_grad_t is None:
            down_term, up_term = lax.optimization_barrier((down_term, up_term))
        down_grad_t = down_term if down_grad_t is None else down_grad_t + down_term
        up_grad = up_term if up_grad is None else up_grad + up_term
    before_grad = jnp.concatenate(before_grad_parts)
    up_bias_grad = jnp.sum(before_grad[:, :hidden_width], axis=0, dtype=F32)
    mlp_grad_pack = jnp.concatenate([up_grad.astype(BF), down_grad_t.astype(BF)], axis=1)
    mlp_grads = lax.psum_scatter(
        mlp_grad_pack, ("dp", "ctx"), scatter_dimension=0, tiled=True
    )
    norm_two_grad = tensor_reduce_parts(norm_two_terms)
    hidden_back, gain_two_grad, shift_two_grad = norm_backward(
        norm_two_grad, unit_two, inverse_two, gain_two
    )
    hidden_grad = grad_out + hidden_back
    down_bias_grad = jnp.sum(grad_out, axis=0)
    out_bias_grad = jnp.sum(hidden_grad, axis=0)
    hidden_token_parts = tensor_gather_parts(hidden_grad.astype(BF))
    out_grad_t = None
    query_parts, key_parts, value_parts = [], [], []
    for i, token_grad in enumerate(hidden_token_parts):
        if i == 1 and n_t == 2:
            own_done = (out_grad_t, query_parts[0], key_parts[0], value_parts[0])
            own_done, token_grad = lax.optimization_barrier((own_done, token_grad))
            out_grad_t, query_parts[0], key_parts[0], value_parts[0] = own_done
        sl = slice(i * own_images, (i + 1) * own_images)
        token_grad = token_grad.reshape(own_images, half_len, width)
        mixed_i = mixed_per_head[sl]
        out_term = jnp.einsum(
            "lcd,lscm->dsm", token_grad, mixed_i, preferred_element_type=F32
        ).reshape(width, head_width)
        out_grad_t = out_term if out_grad_t is None else out_grad_t + out_term
        mixed_grad = jnp.einsum(
            "lcd,dsm->lscm", token_grad, out_per_head, preferred_element_type=F32
        ).astype(BF)
        value_i = value_all[sl]
        key_i = key_all[sl]
        soft_full = jnp.exp(scores[sl] - log_totals[sl])
        soft_grad = jnp.einsum("bhqe,bhke->bhqk", mixed_grad, value_i, preferred_element_type=F32)
        value_parts.append(
            jnp.einsum(
                "bhqk,bhqe->bhke", soft_full.astype(BF), mixed_grad, preferred_element_type=F32
            )
        )
        inner_sum = jnp.sum(soft_full * soft_grad, axis=-1, keepdims=True)
        score_grad = (soft_full * (soft_grad - inner_sum)).astype(BF)
        query_parts.append(
            jnp.einsum("bhqk,bhke->bhqe", score_grad, key_i, preferred_element_type=F32)
            * score_scale
        )
        key_parts.append(
            jnp.einsum(
                "bhqk,bhqe->bhke", score_grad, queries[sl], preferred_element_type=F32
            )
            * score_scale
        )
    query_grads = jnp.concatenate(query_parts)
    key_grads = jnp.concatenate(key_parts)
    value_grads = jnp.concatenate(value_parts)
    key_reduced_precision = ctx_reduce(key_grads, half_len).astype(BF)
    value_reduced_precision = ctx_reduce(value_grads, half_len).astype(BF)
    query_reduced_precision = query_grads.astype(BF)
    query_bias_grad = jnp.sum(query_reduced_precision, axis=(0, 2), dtype=F32).reshape(head_width)
    value_bias_grad = jnp.sum(value_reduced_precision, axis=(0, 2), dtype=F32).reshape(head_width)
    qkv_grads = jnp.stack(
        [query_reduced_precision, key_reduced_precision, value_reduced_precision]
    )
    qkv_weight_grad = jnp.einsum(
        "okz,toaks->ztas", normed_every_row, qkv_grads, preferred_element_type=F32
    ).reshape(width, 3 * head_width)
    attn_grads = lax.psum_scatter(
        jnp.concatenate(
            [jnp.pad(out_grad_t.astype(BF), ((0, 0), (0, pad_out))), qkv_weight_grad.astype(BF)],
            axis=1,
        ),
        ("dp", "ctx"),
        scatter_dimension=0,
        tiled=True,
    )
    norm_one_terms = jnp.einsum(
        "toaks,tzas->okz", qkv_grads, qkv_w, preferred_element_type=F32
    )
    norm_one_grad = tensor_reduce(norm_one_terms.reshape(n_t, rows, width))
    input_back, gain_one_grad, shift_one_grad = norm_backward(
        norm_one_grad, unit_one, inverse_one, gain_one
    )
    tokens_grad = (hidden_grad + input_back).reshape(own_images, half_len, width)

    row_sums = jnp.concatenate(
        [
            gain_one_grad,
            shift_one_grad,
            out_bias_grad,
            gain_two_grad,
            shift_two_grad,
            down_bias_grad,
            partial_value.reshape(1),
        ]
    )
    head_sums = jnp.concatenate([query_bias_grad, value_bias_grad, up_bias_grad])
    row_sums, head_sums = tree_sum((row_sums, head_sums), ("ctx", "dp"))
    row_sums = tree_sum(row_sums, ("tensor",))
    loss_value = row_sums[6 * width] / valid_count
    piece_start = lax.axis_index(("dp", "ctx")) * piece
    vector_shards = [
        lax.dynamic_slice_in_dim(row_sums, i * width + piece_start, piece) for i in range(6)
    ]
    query_bias_sum = head_sums[:head_width]
    value_bias_sum = head_sums[head_width : 2 * head_width]
    up_bias_sum = head_sums[2 * head_width :]
    attn_grads = attn_grads.astype(F32)
    mlp_grads = mlp_grads.astype(F32)
    out_cols = head_width + pad_out
    attn_grads = [
        attn_grads[:, out_cols + i * head_width : out_cols + (i + 1) * head_width]
        for i in range(3)
    ] + [attn_grads[:, :head_width]]
    hidden_cols = hidden_width + pad_hidden
    mlp_grads = [
        mlp_grads[:, :hidden_width],
        mlp_grads[:, hidden_cols : hidden_cols + hidden_width],
    ]
    return (
        layer_out,
        loss_value,
        tokens_grad,
        vector_shards[0],
        vector_shards[1],
        attn_grads[0],
        query_bias_sum,
        attn_grads[1],
        attn_grads[2],
        value_bias_sum,
        attn_grads[3].T,
        vector_shards[2],
        vector_shards[3],
        vector_shards[4],
        mlp_grads[0],
        up_bias_sum,
        mlp_grads[1].T,
        vector_shards[5],
    )


def solution(mesh):
    return jax.shard_map(
        on_device_body,
        mesh=mesh,
        in_specs=(
            P(("dp", "tensor"), "ctx", None),
            P(("dp", "tensor"), "ctx", None),
            P(("dp", "tensor")),
            P(("dp", "ctx")),
            P(("dp", "ctx")),
            P(("dp", "ctx"), "tensor"),
            P("tensor"),
            P(("dp", "ctx"), "tensor"),
            P(("dp", "ctx"), "tensor"),
            P("tensor"),
            P("tensor", ("dp", "ctx")),
            P(("dp", "ctx")),
            P(("dp", "ctx")),
            P(("dp", "ctx")),
            P(("dp", "ctx"), "tensor"),
            P("tensor"),
            P("tensor", ("dp", "ctx")),
            P(("dp", "ctx")),
        ),
        out_specs=(
            P(("dp", "tensor"), "ctx", None),
            P(),
            P(("dp", "tensor"), "ctx", None),
            P(("dp", "ctx")),
            P(("dp", "ctx")),
            P(("dp", "ctx"), "tensor"),
            P("tensor"),
            P(("dp", "ctx"), "tensor"),
            P(("dp", "ctx"), "tensor"),
            P("tensor"),
            P("tensor", ("dp", "ctx")),
            P(("dp", "ctx")),
            P(("dp", "ctx")),
            P(("dp", "ctx")),
            P(("dp", "ctx"), "tensor"),
            P("tensor"),
            P("tensor", ("dp", "ctx")),
            P(("dp", "ctx")),
        ),
        check_vma=False,
    )
```

```python
import jax
import jax.numpy as jnp
from jax import lax
from jax.sharding import PartitionSpec as P


HD = 72
REAL = 729


EPSILON = 1e-06
GELU_C = 0.7978845608028654
GELU_K = 0.044715
BF = jnp.bfloat16
F32 = jnp.float32


def norm_forward(row_values, gain_vec, shift_vec):
    average = jnp.mean(row_values, axis=-1, keepdims=True)
    centred = row_values - average
    spread = jnp.mean(centred * centred, axis=-1, keepdims=True)
    inverse = lax.rsqrt(spread + EPSILON)
    unit_rows = centred * inverse
    return (unit_rows * gain_vec + shift_vec, unit_rows, inverse)


def norm_backward(upstream, unit_rows, inverse, gain_vec):
    scaled = upstream * gain_vec
    inner_sum = (
        scaled
        - jnp.mean(scaled, axis=-1, keepdims=True)
        - unit_rows * jnp.mean(scaled * unit_rows, axis=-1, keepdims=True)
    )
    return (inner_sum * inverse, jnp.sum(upstream * unit_rows, axis=0), jnp.sum(upstream, axis=0))


def gelu_tanh(values):
    return 0.5 * values * (1.0 + jnp.tanh(GELU_C * (values + GELU_K * values * values * values)))


def gelu_slope(values):
    tanh_part = jnp.tanh(GELU_C * (values + GELU_K * values * values * values))
    return 0.5 * (1.0 + tanh_part) + 0.5 * values * (1.0 - tanh_part * tanh_part) * GELU_C * (
        1.0 + 3.0 * GELU_K * values * values
    )


def swap(values, axis):
    return lax.ppermute(values, axis, [(0, 1), (1, 0)])


def tensor_gather(values):
    if lax.axis_size("tensor") == 2:
        return jnp.stack([values, swap(values, "tensor")])
    return lax.all_gather(values, "tensor", axis=0)


def tensor_reduce(partials):
    if lax.axis_size("tensor") == 2:
        return partials[0] + swap(partials[1].astype(BF), "tensor").astype(F32)
    return lax.psum_scatter(partials.astype(BF), "tensor", scatter_dimension=0).astype(F32)


def tensor_gather_parts(values):
    if lax.axis_size("tensor") == 2:
        return [values, swap(values, "tensor")]
    gathered = lax.all_gather(values, "tensor", axis=0)
    return [gathered[i] for i in range(gathered.shape[0])]


def tensor_reduce_parts(parts):
    if lax.axis_size("tensor") == 2:
        other = swap(parts[1].astype(BF), "tensor")
        return lax.optimization_barrier(parts[0]) + other.astype(F32)
    return lax.psum_scatter(
        jnp.stack(parts).astype(BF), "tensor", scatter_dimension=0
    ).astype(F32)


def ctx_gather(values):
    if lax.axis_size("ctx") == 2:
        return jnp.concatenate([values, swap(values, "ctx")], axis=2)
    return lax.all_gather(values, "ctx", axis=2, tiled=True)


def ctx_reduce(values, half_len):
    if lax.axis_size("ctx") == 2:
        other = swap(values[:, :, half_len:].astype(BF), "ctx")
        return values[:, :, :half_len] + other.astype(F32)
    return lax.psum_scatter(
        values.astype(BF), "ctx", scatter_dimension=2, tiled=True
    ).astype(F32)


def key_positions(half_len):
    n_ctx = lax.axis_size("ctx")
    local = jnp.arange(half_len * n_ctx)
    if n_ctx == 2:
        me = lax.axis_index("ctx")
        block = jnp.where(local < half_len, me, 1 - me)
        return block * half_len + local % half_len
    return local


def tree_sum(values, axes):
    for axis in axes:
        size = lax.axis_size(axis)
        if size & (size - 1):
            values = jax.tree.map(lambda v: lax.psum(v, axis), values)
            continue
        step = 1
        while step < size:
            perm = [(i, i ^ step) for i in range(size)]
            values = jax.tree.map(lambda v: v + lax.ppermute(v, axis, perm), values)
            step *= 2
    return values


def gather_vectors(block, count):
    n_ctx = lax.axis_size("ctx")
    n_dp = lax.axis_size("dp")
    if n_ctx != 2 or n_dp & (n_dp - 1):
        gathered = lax.all_gather(block, ("dp", "ctx"), axis=0, tiled=True)
        return gathered, tree_sum(count, ("tensor", "dp"))
    count = tree_sum(count, ("tensor",))
    other = swap(block, "ctx")
    first = lax.axis_index("ctx") == 0
    blocks = jnp.where(first, jnp.stack([block, other]), jnp.stack([other, block]))
    dp_index = lax.axis_index("dp")
    step = 1
    while step < n_dp:
        perm = [(i, i ^ step) for i in range(n_dp)]
        their_blocks, their_count = lax.ppermute((blocks, count), "dp", perm)
        low = (dp_index // step) % 2 == 0
        blocks = jnp.where(
            low,
            jnp.concatenate([blocks, their_blocks]),
            jnp.concatenate([their_blocks, blocks]),
        )
        count = count + their_count
        step *= 2
    return blocks.reshape(-1, block.shape[1]), count


def on_device_body(
    tokens,
    teacher,
    valid_len,
    ln1_gain,
    ln1_bias,
    w_q,
    b_q,
    w_k,
    w_v,
    b_v,
    w_o,
    b_o,
    ln2_gain,
    ln2_bias,
    w_up,
    b_up,
    w_down,
    b_down,
):
    own_images, half_len, width = tokens.shape
    n_t = lax.axis_size("tensor")
    piece, head_width = w_q.shape
    local_heads = head_width // HD
    hidden_width = w_up.shape[1]
    rows = own_images * half_len
    images = n_t * own_images

    pad_hidden = (-hidden_width) % 128
    vector_rows = jnp.stack([ln1_gain, ln1_bias, b_o, ln2_gain, ln2_bias, b_down], axis=1)
    vectors, valid_count = gather_vectors(vector_rows, jnp.sum(valid_len.astype(jnp.int32)))
    valid_count = valid_count.astype(F32)
    valid_count, tokens = lax.optimization_barrier((valid_count, tokens))
    attn_pack = jnp.stack([w_q, w_k, w_v, w_o.T])
    attn_full = lax.all_gather(attn_pack, ("dp", "ctx"), axis=1, tiled=True)
    mlp_pack = jnp.pad(jnp.stack([w_up, w_down.T]), ((0, 0), (0, 0), (0, pad_hidden)))
    mlp_full = lax.all_gather(mlp_pack, ("dp", "ctx"), axis=1, tiled=True)
    qkv_w = attn_full[:3].reshape(3, width, local_heads, HD)
    out_wt = attn_full[3]
    vectors = vectors.astype(F32)
    gain_one, shift_one, out_bias, gain_two, shift_two, down_bias = [
        vectors[:, i] for i in range(6)
    ]
    up_w, down_wt = mlp_full[0], mlp_full[1]
    up_b = jnp.pad(b_up.astype(F32), (0, pad_hidden))

    out_per_head = out_wt.reshape(width, local_heads, HD)
    qkv_bias = jnp.stack(
        [b_q.astype(F32), jnp.zeros((head_width,), F32), b_v.astype(F32)]
    ).reshape(3, 1, local_heads, 1, HD)

    inputs = tokens.astype(F32).reshape(rows, width)
    normed, unit_one, inverse_one = norm_forward(inputs, gain_one, shift_one)
    normed_every_row = tensor_gather(normed.astype(BF)).reshape(images, half_len, width)
    qkv_rows = (
        jnp.einsum("pro,tojx->tpjrx", normed_every_row, qkv_w, preferred_element_type=F32)
        + qkv_bias
    ).astype(BF)
    queries, key_rows, value_rows = qkv_rows[0], qkv_rows[1], qkv_rows[2]
    key_all = ctx_gather(key_rows)
    value_all = ctx_gather(value_rows)
    usable = key_positions(half_len) < REAL
    score_scale = HD ** (-0.5)

    raw_scores = jnp.einsum("bhqe,bhke->bhqk", queries, key_all, preferred_element_type=F32)
    scores = jnp.where(usable, raw_scores * score_scale, -1e30)
    summit = jnp.max(scores, axis=-1, keepdims=True)
    exp_total = jnp.sum(jnp.exp(scores - summit), axis=-1, keepdims=True)
    log_totals = summit + jnp.log(exp_total)
    soft_weights = jnp.exp(scores - log_totals).astype(BF)
    mixed_per_head = jnp.einsum(
        "bhqk,bhke->bhqe", soft_weights, value_all, preferred_element_type=F32
    ).astype(BF)

    attn_terms = jnp.einsum(
        "lscm,dsm->lcd", mixed_per_head, out_per_head, preferred_element_type=F32
    )
    attn_sum = tensor_reduce(attn_terms.reshape(n_t, rows, width))
    hidden = inputs + attn_sum + out_bias
    normed_two, unit_two, inverse_two = norm_forward(hidden, gain_two, shift_two)
    normed_two_parts = tensor_gather_parts(normed_two.astype(BF))
    before_parts = [
        jnp.dot(part, up_w, preferred_element_type=F32) + up_b for part in normed_two_parts
    ]
    active_parts = [gelu_tanh(part).astype(BF) for part in before_parts]
    mlp_terms = [
        jnp.einsum("rf,df->rd", part, down_wt, preferred_element_type=F32)
        for part in active_parts
    ]
    result = hidden + tensor_reduce_parts(mlp_terms) + down_bias
    layer_out = result.astype(BF).reshape(own_images, half_len, width)

    position = lax.axis_index("ctx") * half_len + jnp.arange(half_len)
    valid_rows = (position[None, :] < valid_len[:, None]).astype(F32).reshape(rows)
    error_rows = result - teacher.astype(F32).reshape(rows, width)
    partial_value = 0.5 * jnp.sum(valid_rows * jnp.mean(error_rows * error_rows, axis=-1))
    slot_total = own_images * lax.axis_size("dp") * n_t
    factor = slot_total * (half_len * lax.axis_size("ctx")) / valid_count
    grad_out = error_rows * (valid_rows[:, None] * factor)

    grad_parts = tensor_gather_parts(grad_out.astype(BF))
    before_grad_parts = [
        (
            jnp.einsum("rd,df->rf", g, down_wt, preferred_element_type=F32)
            * gelu_slope(p)
        ).astype(BF)
        for g, p in zip(grad_parts, before_parts)
    ]
    norm_two_terms = [
        jnp.einsum("rf,df->rd", g, up_w, preferred_element_type=F32)
        for g in before_grad_parts
    ]
    down_grad_t = None
    up_grad = None
    for g, a_part, n_part, p_grad in zip(
        grad_parts, active_parts, normed_two_parts, before_grad_parts
    ):
        term_type = BF if down_grad_t is None else F32
        down_term = jnp.einsum("rd,rf->df", g, a_part, preferred_element_type=term_type)
        up_term = jnp.einsum("rd,rf->df", n_part, p_grad, preferred_element_type=term_type)
        if down_grad_t is None:
            down_term, up_term = lax.optimization_barrier((down_term, up_term))
        down_grad_t = down_term if down_grad_t is None else down_grad_t + down_term
        up_grad = up_term if up_grad is None else up_grad + up_term
    before_grad = jnp.concatenate(before_grad_parts)
    up_bias_grad = jnp.sum(before_grad[:, :hidden_width], axis=0, dtype=F32)
    mlp_grad_pack = jnp.concatenate([up_grad.astype(BF), down_grad_t.astype(BF)], axis=1)
    mlp_grads = lax.psum_scatter(
        mlp_grad_pack, ("dp", "ctx"), scatter_dimension=0, tiled=True
    )
    norm_two_grad = tensor_reduce_parts(norm_two_terms)
    hidden_back, gain_two_grad, shift_two_grad = norm_backward(
        norm_two_grad, unit_two, inverse_two, gain_two
    )
    hidden_grad = grad_out + hidden_back
    down_bias_grad = jnp.sum(grad_out, axis=0)
    out_bias_grad = jnp.sum(hidden_grad, axis=0)
    hidden_token_parts = tensor_gather_parts(hidden_grad.astype(BF))
    out_grad_t = None
    query_parts, key_parts, value_parts = [], [], []
    for i, token_grad in enumerate(hidden_token_parts):
        if i == 1 and n_t == 2:
            own_done = (out_grad_t, query_parts[0], key_parts[0], value_parts[0])
            own_done, token_grad = lax.optimization_barrier((own_done, token_grad))
            out_grad_t, query_parts[0], key_parts[0], value_parts[0] = own_done
        sl = slice(i * own_images, (i + 1) * own_images)
        token_grad = token_grad.reshape(own_images, half_len, width)
        mixed_i = mixed_per_head[sl]
        out_term = jnp.einsum(
            "lcd,lscm->dsm", token_grad, mixed_i, preferred_element_type=F32
        ).reshape(width, head_width)
        out_grad_t = out_term if out_grad_t is None else out_grad_t + out_term
        mixed_grad = jnp.einsum(
            "lcd,dsm->lscm", token_grad, out_per_head, preferred_element_type=F32
        ).astype(BF)
        value_i = value_all[sl]
        key_i = key_all[sl]
        soft_full = jnp.exp(scores[sl] - log_totals[sl])
        soft_grad = jnp.einsum("bhqe,bhke->bhqk", mixed_grad, value_i, preferred_element_type=F32)
        value_parts.append(
            jnp.einsum(
                "bhqk,bhqe->bhke", soft_full.astype(BF), mixed_grad, preferred_element_type=F32
            )
        )
        inner_sum = jnp.sum(soft_full * soft_grad, axis=-1, keepdims=True)
        score_grad = (soft_full * (soft_grad - inner_sum)).astype(BF)
        query_parts.append(
            jnp.einsum("bhqk,bhke->bhqe", score_grad, key_i, preferred_element_type=F32)
            * score_scale
        )
        key_parts.append(
            jnp.einsum(
                "bhqk,bhqe->bhke", score_grad, queries[sl], preferred_element_type=F32
            )
            * score_scale
        )
    query_grads = jnp.concatenate(query_parts)
    key_grads = jnp.concatenate(key_parts)
    value_grads = jnp.concatenate(value_parts)
    key_reduced_precision = ctx_reduce(key_grads, half_len).astype(BF)
    value_reduced_precision = ctx_reduce(value_grads, half_len).astype(BF)
    query_reduced_precision = query_grads.astype(BF)
    query_bias_grad = jnp.sum(query_reduced_precision, axis=(0, 2), dtype=F32).reshape(head_width)
    value_bias_grad = jnp.sum(value_reduced_precision, axis=(0, 2), dtype=F32).reshape(head_width)
    qkv_grads = jnp.stack(
        [query_reduced_precision, key_reduced_precision, value_reduced_precision]
    )
    qkv_weight_grad = jnp.einsum(
        "okz,toaks->ztas", normed_every_row, qkv_grads, preferred_element_type=F32
    ).reshape(width, 3 * head_width)
    attn_grads = lax.psum_scatter(
        jnp.concatenate(
            [qkv_weight_grad.astype(BF), out_grad_t.astype(BF)],
            axis=1,
        ),
        ("dp", "ctx"),
        scatter_dimension=0,
        tiled=True,
    )
    norm_one_terms = jnp.einsum(
        "toaks,tzas->okz", qkv_grads, qkv_w, preferred_element_type=F32
    )
    norm_one_grad = tensor_reduce(norm_one_terms.reshape(n_t, rows, width))
    input_back, gain_one_grad, shift_one_grad = norm_backward(
        norm_one_grad, unit_one, inverse_one, gain_one
    )
    tokens_grad = (hidden_grad + input_back).reshape(own_images, half_len, width)

    row_sums = jnp.concatenate(
        [
            gain_one_grad,
            shift_one_grad,
            out_bias_grad,
            gain_two_grad,
            shift_two_grad,
            down_bias_grad,
            partial_value.reshape(1),
        ]
    )
    head_sums = jnp.concatenate([query_bias_grad, value_bias_grad, up_bias_grad])
    row_sums, head_sums = tree_sum((row_sums, head_sums), ("ctx", "dp"))
    row_sums = tree_sum(row_sums, ("tensor",))
    loss_value = row_sums[6 * width] / valid_count
    piece_start = lax.axis_index(("dp", "ctx")) * piece
    vector_shards = [
        lax.dynamic_slice_in_dim(row_sums, i * width + piece_start, piece) for i in range(6)
    ]
    query_bias_sum = head_sums[:head_width]
    value_bias_sum = head_sums[head_width : 2 * head_width]
    up_bias_sum = head_sums[2 * head_width :]
    attn_grads = attn_grads.astype(F32)
    mlp_grads = mlp_grads.astype(F32)
    attn_grads = [attn_grads[:, i * head_width : (i + 1) * head_width] for i in range(4)]
    hidden_cols = hidden_width + pad_hidden
    mlp_grads = [
        mlp_grads[:, :hidden_width],
        mlp_grads[:, hidden_cols : hidden_cols + hidden_width],
    ]
    return (
        layer_out,
        loss_value,
        tokens_grad,
        vector_shards[0],
        vector_shards[1],
        attn_grads[0],
        query_bias_sum,
        attn_grads[1],
        attn_grads[2],
        value_bias_sum,
        attn_grads[3].T,
        vector_shards[2],
        vector_shards[3],
        vector_shards[4],
        mlp_grads[0],
        up_bias_sum,
        mlp_grads[1].T,
        vector_shards[5],
    )


def solution(mesh):
    return jax.shard_map(
        on_device_body,
        mesh=mesh,
        in_specs=(
            P(("dp", "tensor"), "ctx", None),
            P(("dp", "tensor"), "ctx", None),
            P(("dp", "tensor")),
            P(("dp", "ctx")),
            P(("dp", "ctx")),
            P(("dp", "ctx"), "tensor"),
            P("tensor"),
            P(("dp", "ctx"), "tensor"),
            P(("dp", "ctx"), "tensor"),
            P("tensor"),
            P("tensor", ("dp", "ctx")),
            P(("dp", "ctx")),
            P(("dp", "ctx")),
            P(("dp", "ctx")),
            P(("dp", "ctx"), "tensor"),
            P("tensor"),
            P("tensor", ("dp", "ctx")),
            P(("dp", "ctx")),
        ),
        out_specs=(
            P(("dp", "tensor"), "ctx", None),
            P(),
            P(("dp", "tensor"), "ctx", None),
            P(("dp", "ctx")),
            P(("dp", "ctx")),
            P(("dp", "ctx"), "tensor"),
            P("tensor"),
            P(("dp", "ctx"), "tensor"),
            P(("dp", "ctx"), "tensor"),
            P("tensor"),
            P("tensor", ("dp", "ctx")),
            P(("dp", "ctx")),
            P(("dp", "ctx")),
            P(("dp", "ctx")),
            P(("dp", "ctx"), "tensor"),
            P("tensor"),
            P("tensor", ("dp", "ctx")),
            P(("dp", "ctx")),
        ),
        check_vma=False,
    )
```
